768 devices in a mesh: dom: 64 (over x, y, core), sub: 12 (over z).
Axes of the slice: x: 4, y: 8, z: 12, core: 2. Of those that a mesh axis runs over, the one named last changes fastest.
Arguments:
- displacement: float32 [3, 1036800], P(None, ('dom', 'sub')), may hold values from -0.01 to 0.01
- velocity: float32 [3, 1036800], P(None, ('dom', 'sub')), may hold values from -3 to 3
- energy: float32 [27, 36864], P(None, ('dom', 'sub')), may hold values from 0.5 to 18, as said below
- mass_density: float32 [125, 36864], P(None, ('dom', 'sub')), may hold values from 0.5 to 4
- live_mask: int32 [36864], P(('dom', 'sub')), may hold values from 0 to 1, as said below
- time_step: float32 [], replicated, may hold values from 0.004 to 0.008
Outputs:
- new_velocity: float32 [3, 1036800], P(None, ('dom', 'sub'))
- energy_rate: float32 [27, 36864], P(None, ('dom', 'sub'))
- mesh_velocity: float32 [3, 1036800], P(None, ('dom', 'sub'))
The draws below stay inside these ranges and needn't reach their ends.
Inputs may be any that keep to these rules, and one draw needn't show every extreme that they name: `energy`: internal energies are positive. `live_mask`: at most 36 element slots of one device are live, and some device has exactly 36.
All inputs are finite; a program needn't handle non-finite values.
Results may differ from the reference program's by a relative error of at most 0.0003.
Values sent between devices are 32-bit elements; how exact they have to be, the bound alone decides.
No kernel may reach another device: no remote copies, remote signals or barrier semaphores. Data moves between devices by JAX's collectives and lax.ppermute only.
A program may use at most 32 MiB of HBM per device.

```python
import math
import jax
import jax.numpy as jnp
import numpy as np
from jax import lax

EX = 1
EY = 8
EZ = 6
QUAD_POINTS = 125
CG_ITERS = 2
RELAX_PASSES = 2
GX = 64
GZ = 72
ELEMS = 36864
NODES = 1036800
N_DOM = 64
N_SUB = 12


def draw_energy(key, part):
    devices = N_DOM * N_SUB
    per_device = EX * EY * EZ
    key_base = jax.random.fold_in(key, 11)
    base_values = jnp.exp(jax.random.uniform(key_base, (27, devices, per_device), jnp.float32, math.log(0.5), math.log(2.0)))
    ramp = 1.0 + 2.0 * jnp.arange(devices, dtype=jnp.float32) / max(devices - 1, 1)
    scaled = base_values * ramp[None, :, None]
    return scaled.reshape(27, devices * per_device)


def draw_live_mask(key, part):
    devices = N_DOM * N_SUB
    per_device = EX * EY * EZ
    largest = 3 * per_device // 4
    fewest = max(per_device // 4, 1)
    key_count = jax.random.fold_in(key, 21)
    key_pick = jax.random.fold_in(key, 22)
    key_order = jax.random.fold_in(key, 23)
    counts = jax.random.randint(key_count, (devices,), fewest, largest + 1)
    chosen = jax.random.randint(key_pick, (), 0, devices)
    counts = jnp.where(jnp.arange(devices) == chosen, largest, counts)
    scores = jax.random.randint(key_order, (devices, per_device), 0, 1 << 18)
    scores = scores * per_device + jnp.arange(per_device, dtype=jnp.int32)[None, :]
    ranking = jnp.argsort(jnp.argsort(scores, axis=1, stable=True), axis=1, stable=True)
    live_values = (ranking < counts[:, None]).astype(jnp.int32)
    return live_values.reshape(devices * per_device)


def block_levels(key, dims, split, low, high):
    level = 1.0
    for axis_at, shards_of in split:
        steps = jax.random.uniform(jax.random.fold_in(jax.random.fold_in(key, 6), axis_at), (shards_of,), jnp.float32, low / len(split), high / len(split))
        level = level * jnp.repeat(jnp.exp(steps), dims[axis_at] // shards_of).reshape((-1,) + (1,) * (len(dims) - 1 - axis_at))
    return level


def scatter_about(key, dims, scale, most, cuts=(), kind=jnp.bfloat16):
    gain = block_levels(key, dims, cuts, -0.22, 0.18) if cuts else 1.0
    values = jax.random.normal(key, dims, jnp.float32) * scale * gain
    return jnp.minimum(jnp.maximum(values, -most), most).astype(kind)


def setup_inputs(seed: int = 0) -> dict:
    arg_keys = jax.random.split(jax.random.key(seed), 7)
    return {
        "displacement": jnp.clip(jax.random.uniform(arg_keys[0], (3, NODES), jnp.float32, -0.01, 0.01) * block_levels(arg_keys[0], (3, NODES), ((1, 768),), -0.4, 0.0), -0.01, 0.01),
        "velocity": scatter_about(arg_keys[1], (3, NODES), 0.5, 3.0, ((1, 768),), jnp.float32),
        "energy": draw_energy(jax.random.fold_in(arg_keys[6], 71), 0),
        "mass_density": jnp.clip(jnp.exp(math.log(4.0) - 2.0794415 * jax.random.uniform(arg_keys[3], (QUAD_POINTS, ELEMS), jnp.float32) ** block_levels(arg_keys[3], (QUAD_POINTS, ELEMS), ((1, 768),), -0.2, 0.2)), 0.5, 4.0),
        "live_mask": draw_live_mask(jax.random.fold_in(arg_keys[6], 71), 0),
        "time_step": jnp.clip(jax.random.uniform(arg_keys[5], (), jnp.float32, 0.004, 0.008), 0.004, 0.008),
    }


highest = lax.Precision.HIGHEST
adiabatic = 5.0 / 3.0
viscosity = 0.3
mesh_step = 0.01

def outer_triple(first, second, third):
    product = first[:, None, None, :, None, None] * second[None, :, None, None, :, None] * third[None, None, :, None, None, :]
    return product.reshape(first.shape[0] * second.shape[0] * third.shape[0], first.shape[1] * second.shape[1] * third.shape[1])

def basis_tables():
    root_term = math.sqrt(10.0 / 7.0)
    gauss_roots = np.array([-math.sqrt(5.0 + 2.0 * root_term) / 3.0, -math.sqrt(5.0 - 2.0 * root_term) / 3.0, 0.0, math.sqrt(5.0 - 2.0 * root_term) / 3.0, math.sqrt(5.0 + 2.0 * root_term) / 3.0])
    outer_weight = (322.0 - 13.0 * math.sqrt(70.0)) / 900.0
    middle_weight = (322.0 + 13.0 * math.sqrt(70.0)) / 900.0
    weights = np.array([outer_weight, middle_weight, 128.0 / 225.0, middle_weight, outer_weight]) / 2.0
    points = (1.0 + gauss_roots) / 2.0
    lobatto = [0.0, (1.0 - 1.0 / math.sqrt(5.0)) / 2.0, (1.0 + 1.0 / math.sqrt(5.0)) / 2.0, 1.0]
    values = np.ones((5, 4))
    slopes = np.zeros((5, 4))
    for node_index in range(4):
        for other_index in range(4):
            if other_index != node_index:
                values[:, node_index] *= (points - lobatto[other_index]) / (lobatto[node_index] - lobatto[other_index])
        for other_index in range(4):
            if other_index != node_index:
                factor_term = np.ones(5) / (lobatto[node_index] - lobatto[other_index])
                for third_index in range(4):
                    if third_index != node_index and third_index != other_index:
                        factor_term = factor_term * (points - lobatto[third_index]) / (lobatto[node_index] - lobatto[third_index])
                slopes[:, node_index] += factor_term
    bernstein = np.stack([(1.0 - points) ** 2, 2.0 * points * (1.0 - points), points ** 2], axis=1)
    vel_basis = outer_triple(values, values, values)
    grad_table = np.concatenate([outer_triple(slopes, values, values), outer_triple(values, slopes, values), outer_triple(values, values, slopes)], axis=0)
    energy_basis = outer_triple(bernstein, bernstein, bernstein)
    quad_weight = (weights[:, None, None] * weights[None, :, None] * weights[None, None, :]).reshape(125)
    tables = (jnp.asarray(vel_basis, jnp.float32), jnp.asarray(grad_table, jnp.float32), jnp.asarray(energy_basis, jnp.float32), jnp.asarray(quad_weight, jnp.float32))
    return (tables, lobatto)

def product_dot(left, right):
    return jnp.dot(left, right, precision=highest, preferred_element_type=jnp.float32)

def nodal_gradient(grad_table, nodal_values):
    element_count = nodal_values.shape[1] // 3
    shaped = product_dot(grad_table, nodal_values).reshape(3, 125, 3, element_count)
    return [[shaped[direction, :, component, :] for direction in range(3)] for component in range(3)]

def cofactors(matrix):
    return [[matrix[(row_index + 1) % 3][(col_index + 1) % 3] * matrix[(row_index + 2) % 3][(col_index + 2) % 3] - matrix[(row_index + 1) % 3][(col_index + 2) % 3] * matrix[(row_index + 2) % 3][(col_index + 1) % 3] for col_index in range(3)] for row_index in range(3)]

def project(grad_table, fields):
    element_count = fields[0][0].shape[1]
    stacked = jnp.stack([jnp.stack([fields[component][direction] for component in range(3)], axis=1) for direction in range(3)], axis=0)
    return product_dot(grad_table.T, stacked.reshape(375, 3 * element_count))

def lagrange_rates(coords, speeds, energy, mass_density, live_values, tables):
    vel_basis, grad_table, energy_basis, quad_weight = tables
    jacobian = nodal_gradient(grad_table, coords)
    velocity_grad = nodal_gradient(grad_table, speeds)
    cofactor = cofactors(jacobian)
    volume = jacobian[0][0] * cofactor[0][0] + jacobian[0][1] * cofactor[0][1] + jacobian[0][2] * cofactor[0][2]
    density = mass_density / volume
    pressure = (adiabatic - 1.0) * density * product_dot(energy_basis, energy)
    spatial = [[(velocity_grad[component][0] * cofactor[direction][0] + velocity_grad[component][1] * cofactor[direction][1] + velocity_grad[component][2] * cofactor[direction][2]) / volume for direction in range(3)] for component in range(3)]
    stress = [[viscosity * density * (spatial[component][direction] + spatial[direction][component]) - (pressure if component == direction else 0.0) for direction in range(3)] for component in range(3)]
    weight = quad_weight[:, None] * live_values[None, :]
    flux_terms = [[weight * (stress[component][0] * cofactor[0][direction] + stress[component][1] * cofactor[1][direction] + stress[component][2] * cofactor[2][direction]) for direction in range(3)] for component in range(3)]
    node_force = -project(grad_table, flux_terms)
    power_density = stress[0][0] * spatial[0][0]
    for component in range(3):
        for direction in range(3):
            if component + direction > 0:
                power_density = power_density + stress[component][direction] * spatial[component][direction]
    power_density = weight * volume * power_density
    lumped = product_dot(energy_basis.T, quad_weight[:, None] * mass_density)
    return (node_force, product_dot(energy_basis.T, power_density) / lumped)

def mass_apply(nodal_values, mass_weight, vel_basis):
    element_count = mass_weight.shape[1]
    at_points = product_dot(vel_basis, nodal_values).reshape(125, 3, element_count) * mass_weight[:, None, :]
    return product_dot(vel_basis.T, at_points.reshape(125, 3 * element_count))

def shape_gradient(coords, live_values, tables):
    vel_basis, grad_table, energy_basis, quad_weight = tables
    jacobian = nodal_gradient(grad_table, coords)
    cofactor = cofactors(jacobian)
    volume = jacobian[0][0] * cofactor[0][0] + jacobian[0][1] * cofactor[0][1] + jacobian[0][2] * cofactor[0][2]
    norm_sq = jacobian[0][0] * jacobian[0][0]
    for component in range(3):
        for direction in range(3):
            if component + direction > 0:
                norm_sq = norm_sq + jacobian[component][direction] * jacobian[component][direction]
    ratio_term = norm_sq / volume
    weight = quad_weight[:, None] * live_values[None, :] * volume ** (-2.0 / 3.0)
    fields = [[weight * (2.0 / 3.0 * jacobian[component][direction] - 2.0 / 9.0 * ratio_term * cofactor[component][direction]) for direction in range(3)] for component in range(3)]
    return project(grad_table, fields)

def correlation_take(grid, axis_place):
    rotated = jnp.moveaxis(grid, axis_place, -1)
    block_count = (rotated.shape[-1] - 1) // 3
    main_part = rotated[..., :3 * block_count].reshape(rotated.shape[:-1] + (block_count, 3))
    edge_part = rotated[..., 3::3][..., None]
    return jnp.concatenate([main_part, edge_part], axis=-1)

def correlation_add(pieces):
    block_count = pieces.shape[-2]
    block_width = pieces.shape[-1] - 1
    leading = pieces.shape[:-2]
    main_part = pieces[..., :block_width].reshape(leading + (block_count * block_width,))
    main_part = jnp.pad(main_part, [(0, 0)] * len(leading) + [(0, 1)])
    edge_part = jnp.pad(pieces[..., block_width:], [(0, 0)] * (len(leading) + 1) + [(0, block_width - 1)])
    edge_part = edge_part.reshape(leading + (block_count * block_width,))
    edge_part = jnp.pad(edge_part, [(0, 0)] * len(leading) + [(block_width, 0)])[..., :block_count * block_width + 1]
    return main_part + edge_part

def to_elements(grid):
    pieces = correlation_take(grid, 1)
    pieces = correlation_take(pieces, 1)
    pieces = correlation_take(pieces, 1)
    pieces = pieces.transpose(2, 4, 6, 0, 1, 3, 5)
    return pieces.reshape(64, 3 * EX * EY * EZ)

def to_grid(nodal_values):
    pieces = nodal_values.reshape(4, 4, 4, 3, EX, EY, EZ).transpose(3, 4, 0, 5, 1, 6, 2)
    pieces = correlation_add(pieces)
    pieces = correlation_add(jnp.moveaxis(pieces, (3, 4), (4, 5)))
    pieces = correlation_add(jnp.moveaxis(pieces, (1, 2), (3, 4)))
    return pieces.transpose(0, 3, 2, 1)

def lattice_axis(start_at, extent, lobatto):
    number = start_at + lax.iota(jnp.int32, extent)
    remainder = number % 3
    offset = jnp.where(remainder == 1, lobatto[1], jnp.where(remainder == 2, lobatto[2], 0.0))
    return (number // 3).astype(jnp.float32) + offset

def lattice_grid(start_x, start_z, extent_x, extent_y, extent_z, lobatto):
    along_x = lattice_axis(start_x, extent_x, lobatto)
    along_y = lattice_axis(0, extent_y, lobatto)
    along_z = lattice_axis(start_z, extent_z, lobatto)
    grid_shape = (extent_x, extent_y, extent_z)
    return jnp.stack([jnp.broadcast_to(along_x[:, None, None], grid_shape), jnp.broadcast_to(along_y[None, :, None], grid_shape), jnp.broadcast_to(along_z[None, None, :], grid_shape)])

def full_grid(owned_values):
    channels = owned_values.shape[0]
    blocks = owned_values.reshape(channels, N_DOM, N_SUB, 3 * EX, 3 * EY + 1, 3 * EZ)
    whole = blocks.transpose(0, 1, 3, 4, 2, 5).reshape(channels, 3 * GX, 3 * EY + 1, 3 * GZ)
    return jnp.pad(whole, ((0, 0), (1, 0), (0, 0), (1, 0)))

def device_window(full_values, device):
    dom_place = (device // N_SUB).astype(jnp.int32)
    sub_place = (device % N_SUB).astype(jnp.int32)
    starts = (jnp.int32(0), dom_place * (3 * EX), jnp.int32(0), sub_place * (3 * EZ))
    return lax.dynamic_slice(full_values, starts, (full_values.shape[0], 3 * EX + 1, 3 * EY + 1, 3 * EZ + 1))

def owned_sum(stack):
    channels = stack.shape[1]
    grids = stack.reshape(N_DOM, N_SUB, channels, 3 * EX + 1, 3 * EY + 1, 3 * EZ + 1)
    along_x = correlation_add(grids.transpose(2, 4, 1, 5, 0, 3))
    along_z = correlation_add(along_x.transpose(0, 4, 1, 2, 3))
    interior = along_z[:, 1:, :, 1:]
    blocks = interior.reshape(channels, N_DOM, 3 * EX, 3 * EY + 1, N_SUB, 3 * EZ).transpose(0, 1, 4, 2, 3, 5)
    return blocks.reshape(channels, -1)

def reference(displacement, velocity, energy, mass_density, live_mask, time_step):
    tables, lobatto = basis_tables()
    vel_basis, grad_table, energy_basis, quad_weight = tables
    element_count = EX * EY * EZ
    devices = N_DOM * N_SUB
    device_ids = jnp.arange(devices, dtype=jnp.int32)
    live_values = live_mask.astype(jnp.float32)
    lattice = lattice_grid(0, 0, 3 * GX + 1, 3 * EY + 1, 3 * GZ + 1, lobatto)

    def local_block(element_data, device):
        return lax.dynamic_slice_in_dim(element_data, (device * element_count).astype(jnp.int32), element_count, axis=element_data.ndim - 1)
    full_disp = lattice + full_grid(displacement)
    full_vel = full_grid(velocity)

    def force_block(device):
        coords = to_elements(device_window(full_disp, device))
        speeds = to_elements(device_window(full_vel, device))
        node_force, rate_values = lagrange_rates(coords, speeds, local_block(energy, device), local_block(mass_density, device), local_block(live_values, device), tables)
        return (to_grid(node_force), rate_values)
    forces, rates = lax.map(force_block, device_ids)
    energy_rate = rates.transpose(1, 0, 2).reshape(27, devices * element_count)
    node_force = owned_sum(forces)

    def mass_operator(vector):
        full_values = full_grid(vector)

        def mass_block(device):
            mass_weight = quad_weight[:, None] * local_block(mass_density, device) * local_block(live_values, device)[None, :]
            return to_grid(mass_apply(to_elements(device_window(full_values, device)), mass_weight, vel_basis))
        return owned_sum(lax.map(mass_block, device_ids))
    solution = jnp.zeros_like(node_force)
    residual = node_force
    direction = node_force
    norm_now = jnp.sum(residual * residual)
    for iteration in range(CG_ITERS):
        mass_image = mass_operator(direction)
        step_length = norm_now / jnp.sum(direction * mass_image)
        solution = solution + step_length * direction
        residual = residual - step_length * mass_image
        if iteration + 1 < CG_ITERS:
            norm_next = jnp.sum(residual * residual)
            direction = residual + norm_next / norm_now * direction
            norm_now = norm_next
    new_velocity = velocity + time_step * solution
    moved_disp = displacement + time_step * new_velocity

    def shape_pass(current):
        full_values = lattice + full_grid(current)

        def shape_block(device):
            coords = to_elements(device_window(full_values, device))
            return to_grid(shape_gradient(coords, local_block(live_values, device), tables))
        return owned_sum(lax.map(shape_block, device_ids))
    gradient_sum = jnp.zeros_like(moved_disp)
    for relax_pass in range(RELAX_PASSES):
        gradient = shape_pass(moved_disp)
        gradient_sum = gradient_sum + gradient
        moved_disp = moved_disp - mesh_step * gradient
    mesh_velocity = new_velocity - mesh_step / time_step * gradient_sum
    return (new_velocity, energy_rate, mesh_velocity)
```

```python
import functools
import math

import jax
import jax.numpy as jnp
import numpy as np
from jax import lax
from jax.experimental import pallas as pl
from jax.experimental.pallas import tpu as pltpu
from jax.sharding import PartitionSpec as P

EY = 8
EZ = 6
VISC = 0.3
MESH_STEP = 0.01
BF = jnp.bfloat16
F32 = jnp.float32
ROWS = 40
BELOW = 3
WINDOW = 13
LANE_OWN = 9 * BELOW


def node_row(a, b, c):
    if b == 0 and c > 0:
        return 2 * a + c - 1
    if b > 0 and c == 0:
        return 8 + 2 * a + b - 1
    if b > 0:
        return 16 + 4 * a + 2 * (b - 1) + c - 1
    return 32 + a


def local_row(a, b, c):
    if b < 3 and c < 3:
        return node_row(a, b, c)
    if b == 3 and c < 3:
        return 48 + a if c == 0 else 40 + node_row(a, 0, c)
    if b < 3:
        return 64 + a if b == 0 else 56 + node_row(a, b, 0) - 8
    return 72 + a


def outer_triple(first, second, third):
    product = (
        first[:, None, None, :, None, None]
        * second[None, :, None, None, :, None]
        * third[None, None, :, None, None, :]
    )
    return product.reshape(
        first.shape[0] * second.shape[0] * third.shape[0],
        first.shape[1] * second.shape[1] * third.shape[1],
    )


def basis_tables():
    root_term = math.sqrt(10.0 / 7.0)
    outer = math.sqrt(5.0 + 2.0 * root_term) / 3.0
    inner = math.sqrt(5.0 - 2.0 * root_term) / 3.0
    gauss_roots = np.array([-outer, -inner, 0.0, inner, outer])
    outer_weight = (322.0 - 13.0 * math.sqrt(70.0)) / 900.0
    middle_weight = (322.0 + 13.0 * math.sqrt(70.0)) / 900.0
    weights = (
        np.array([outer_weight, middle_weight, 128.0 / 225.0, middle_weight, outer_weight]) / 2.0
    )
    points = (1.0 + gauss_roots) / 2.0
    lobatto = [0.0, (1.0 - 1.0 / math.sqrt(5.0)) / 2.0, (1.0 + 1.0 / math.sqrt(5.0)) / 2.0, 1.0]
    values = np.ones((5, 4))
    slopes = np.zeros((5, 4))
    for node in range(4):
        for other in range(4):
            if other != node:
                values[:, node] *= (points - lobatto[other]) / (lobatto[node] - lobatto[other])
        for other in range(4):
            if other != node:
                term = np.ones(5) / (lobatto[node] - lobatto[other])
                for third in range(4):
                    if third != node and third != other:
                        term = term * (points - lobatto[third]) / (lobatto[node] - lobatto[third])
                slopes[:, node] += term
    bernstein = np.stack([(1.0 - points) ** 2, 2.0 * points * (1.0 - points), points**2], axis=1)
    quad_weight = (
        weights[:, None, None] * weights[None, :, None] * weights[None, None, :]
    ).reshape(125)
    return (
        outer_triple(values, values, values),
        [
            outer_triple(slopes, values, values),
            outer_triple(values, slopes, values),
            outer_triple(values, values, slopes),
        ],
        outer_triple(bernstein, bernstein, bernstein),
        quad_weight,
    )


def split_table(table):
    high = table.astype(np.float32).astype(jnp.bfloat16)
    low = (table - high.astype(np.float64)).astype(np.float32).astype(jnp.bfloat16)
    return high, low


@functools.cache
def constants():
    vel_basis, grads, energy_basis, quad_weight = basis_tables()
    order = np.zeros(64, np.int64)
    for a in range(4):
        for b in range(4):
            for c in range(4):
                order[16 * a + 4 * b + c] = local_row(a, b, c)

    def spread_columns(table):
        wide = np.zeros((128, 80))
        wide[:125, order] = table
        return wide

    out = {}
    grad = np.concatenate([spread_columns(g) for g in grads], axis=0)
    high, low = split_table(grad)
    out["grad"] = np.concatenate([high, high, low], axis=1)
    high, low = split_table(grad.T)
    out["grad_t"] = np.concatenate([high, low], axis=0)
    phi = spread_columns(vel_basis)
    high, low = split_table(phi)
    out["phi"] = np.concatenate([high, high, low], axis=1)
    high, low = split_table(phi.T)
    out["phi_t"] = np.concatenate([high, low], axis=0)
    psi = np.zeros((128, 32))
    psi[:125, :27] = energy_basis
    high, low = split_table(psi)
    out["psi"] = np.concatenate([high, high, low], axis=1)
    high, low = split_table(psi.T)
    out["psi_t"] = np.concatenate([high, low], axis=0)
    weight = np.zeros((128, 128), np.float32)
    weight[:125] = quad_weight[:, None]
    out["weight"] = weight

    flat = np.arange(1350)
    px, py, pz = flat // 450, (flat // 18) % 25, flat % 18
    lane = 9 * ((pz + 1) // 3) + py // 3
    mask = np.zeros((ROWS, 1350), np.float32)
    mask0 = np.zeros((ROWS, 450), np.float32)
    own = np.zeros((ROWS, 128), np.float32)
    for k in range(1350):
        row = node_row(px[k] + 1, py[k] % 3, (pz[k] + 1) % 3)
        mask[row, k] = 1.0
        own[row, lane[k] + LANE_OWN] = 1.0
    for k in range(450):
        mask0[node_row(0, py[k] % 3, (pz[k] + 1) % 3), k] = 1.0
    out["mask"] = mask
    out["mask0"] = mask0
    out["own"] = own
    pick = np.zeros((1350, 128), np.float32)
    pick[flat, lane] = 1.0
    pick_high = np.zeros((1350, 128), np.float32)
    pick_high[flat, lane + 64] = 1.0
    out["pick"] = pick.astype(jnp.bfloat16)
    out["pick_high"] = pick_high.astype(jnp.bfloat16)
    back = np.zeros((128, 1350), np.float32)
    back[lane + LANE_OWN, flat] = 1.0
    out["back"] = back.astype(jnp.bfloat16)
    element = np.arange(EY * EZ)
    elane = 9 * (element % EZ) + element // EZ
    place = np.zeros((48, 128), np.float32)
    place[element, elane] = 1.0
    place_high = np.zeros((48, 128), np.float32)
    place_high[element, elane + 64] = 1.0
    out["place"] = place.astype(jnp.bfloat16)
    out["place_high"] = place_high.astype(jnp.bfloat16)
    take = np.zeros((128, 48), np.float32)
    take[elane + LANE_OWN, element] = 1.0
    out["take"] = take.astype(jnp.bfloat16)
    own_element = np.zeros((8, 128), np.float32)
    own_element[:, elane + LANE_OWN] = 1.0
    out["own_element"] = own_element
    return out


def dot(left, right):
    return jnp.dot(left, right, preferred_element_type=F32)


def split2(value):
    high = value.astype(BF)
    return high, (value - high.astype(F32)).astype(BF)


def split3(value):
    high = value.astype(BF)
    rest = value - high.astype(F32)
    middle = rest.astype(BF)
    return high, middle, (rest - middle.astype(F32)).astype(BF)


def exact_dot(value, selection):
    high, middle, low = split3(value)
    return dot(high, selection) + (dot(middle, selection) + dot(low, selection))


def stacked(value):
    high, low = split2(value)
    return jnp.concatenate([high, low, high], axis=0)


def rolled(value, by):
    return pltpu.roll(value, by % 128, 1)


def to_local(nodes):
    columns = []
    for comp in range(3):
        block = nodes[ROWS * comp : ROWS * comp + ROWS]
        corner = block[32:40]
        columns.append(
            jnp.concatenate(
                [
                    block,
                    rolled(block[0:8], -1),
                    rolled(corner, -1),
                    rolled(block[8:16], -9),
                    rolled(corner, -9),
                    rolled(corner, -10),
                ],
                axis=0,
            )
        )
    return jnp.concatenate(columns, axis=1)


def from_local(local):
    blocks = []
    for comp in range(3):
        part = local[:, 128 * comp : 128 * comp + 128]
        blocks += [
            part[0:8] + rolled(part[40:48], 1),
            part[8:16] + rolled(part[56:64], 9),
            part[16:32],
            part[32:40]
            + (rolled(part[48:56], 1) + rolled(part[64:72], 9) + rolled(part[72:80], 10)),
        ]
    return jnp.concatenate(blocks, axis=0)


def transposed_dot(table, value):
    high, low = split2(value)
    half = table.shape[0] // 2
    both = dot(table, high)
    return both[:half] + (both[half:] + dot(table[:half], low))


def add_planes(nodes, below, above):
    row = lax.broadcasted_iota(jnp.int32, (8, 128), 0)
    blocks = []
    for comp in range(3):
        at = ROWS * comp
        for group in (0, 8):
            low = pltpu.roll(below[at + group : at + group + 8], 2, 0)
            high = pltpu.roll(above[at + group : at + group + 8], 6, 0)
            blocks.append(
                nodes[at + group : at + group + 8]
                + jnp.where(row < 2, low, jnp.where(row >= 6, high, 0.0))
            )
        low = pltpu.roll(below[at + 24 : at + 32], 4, 0)
        high = pltpu.roll(above[at + 16 : at + 24], 4, 0)
        blocks.append(nodes[at + 16 : at + 24] + jnp.where(row < 4, low, 0.0))
        blocks.append(nodes[at + 24 : at + 32] + jnp.where(row >= 4, high, 0.0))
        low = pltpu.roll(below[at + 32 : at + 40], 5, 0)
        high = pltpu.roll(above[at + 32 : at + 40], 3, 0)
        blocks.append(
            nodes[at + 32 : at + 40] + jnp.where(row == 0, low, jnp.where(row == 3, high, 0.0))
        )
    return jnp.concatenate(blocks, axis=0)


def shared_sum(nodes, even_ref, first_ref, second_ref, wall_ref):
    even = jnp.concatenate([even_ref[...]] * 15, axis=0) > 0.5
    first, second = first_ref[...], second_ref[...]
    total = add_planes(nodes, jnp.where(even, second, first), jnp.where(even, first, second))
    wall = wall_ref[...]
    return total * jnp.concatenate([wall, wall, wall], axis=0)


def cofactors(j):
    return [
        [
            j[(r + 1) % 3][(c + 1) % 3] * j[(r + 2) % 3][(c + 2) % 3]
            - j[(r + 1) % 3][(c + 2) % 3] * j[(r + 2) % 3][(c + 1) % 3]
            for c in range(3)
        ]
        for r in range(3)
    ]


def gradients(ref, chunk, base=0):
    return [
        [
            ref[128 * m + 8 * chunk : 128 * m + 8 * chunk + 8, base + 128 * c : base + 128 * c + 128]
            for m in range(3)
        ]
        for c in range(3)
    ]


def plus_identity(g):
    return [[g[c][m] + 1.0 if c == m else g[c][m] for m in range(3)] for c in range(3)]


def pack_kernel(disp_ref, vel_ref, dens_ref, energy_ref, live_ref, mask_ref, pick_ref, pick_high_ref,
                place_ref, place_high_ref, out_ref):
    mask = mask_ref[...]
    for comp in range(3):
        low = mask * disp_ref[comp : comp + 1, :]
        high = mask * vel_ref[comp : comp + 1, :]
        out_ref[ROWS * comp : ROWS * comp + ROWS, :] = exact_dot(low, pick_ref[...]) + exact_dot(
            high, pick_high_ref[...]
        )
    density = jnp.concatenate([dens_ref[0:120], jnp.pad(dens_ref[120:125], ((0, 3), (0, 0)))], axis=0)
    row = lax.broadcasted_iota(jnp.int32, (8, 48), 0)
    tail = jnp.pad(energy_ref[24:27], ((0, 5), (0, 0)))
    tail = jnp.where(row == 3, live_ref[...].astype(F32), tail)
    energy = jnp.concatenate([energy_ref[0:24], tail], axis=0)
    place, place_high = place_ref[...], place_high_ref[...]
    out_ref[120:184, :] = exact_dot(density[0:64], place) + exact_dot(density[64:128], place_high)
    out_ref[184:200, :] = exact_dot(energy[0:16], place) + exact_dot(energy[16:32], place_high)


def halo_kernel(packed_ref, halo_ref, mask0_ref, pick_ref, pick_high_ref, out_ref):
    mask0 = mask0_ref[...]
    pick, pick_high = pick_ref[0:450, :], pick_high_ref[0:450, :]
    out_ref[120:200, :] = packed_ref[120:200, :]
    for comp in range(3):
        low = mask0 * halo_ref[comp : comp + 1, :]
        high = mask0 * halo_ref[comp + 3 : comp + 4, :]
        at = slice(ROWS * comp, ROWS * comp + ROWS)
        out_ref[at, :] = packed_ref[at, :] + (exact_dot(low, pick) + exact_dot(high, pick_high))


def unpack(own, below, above):
    lane = lax.broadcasted_iota(jnp.int32, own.shape, 1)
    is_own = (lane >= 27) & (lane < 90)
    is_below = lane < 36
    is_above = lane >= 81

    def window(by):
        return (
            jnp.where(is_own, rolled(own, 27 - by), 0.0)
            + jnp.where(is_below, rolled(below, -27 - by), 0.0)
            + jnp.where(is_above, rolled(above, 81 - by), 0.0)
        )

    return window(0), window(64)


def force_kernel(own_ref, below_ref, above_ref, grad_ref, grad_t_ref, psi_ref, weight_ref,
                 force_ref, disp_ref, vel_ref, mass_ref, live_ref, power_ref, wdens_ref,
                 g_ref, flux_ref, point_ref):
    disp, vel = unpack(own_ref[0:120], below_ref[0:120], above_ref[0:120])
    disp_ref[...] = disp
    vel_ref[...] = vel
    dens_low, dens_high = unpack(own_ref[120:184], below_ref[120:184], above_ref[120:184])
    energy_low, energy_high = unpack(own_ref[184:200], below_ref[184:200], above_ref[184:200])
    energy = jnp.concatenate([energy_low, energy_high], axis=0)
    lane = lax.broadcasted_iota(jnp.int32, (1, 128), 1)
    live = jnp.where(lane < 9 * WINDOW, energy[27:28], 0.0)
    live_ref[...] = jnp.broadcast_to(live, (8, 128))
    table = grad_ref[...]
    g_ref[:, 0:384] = dot(table, stacked(to_local(disp)))
    g_ref[:, 384:768] = dot(table, stacked(to_local(vel)))
    point_ref[...] = dot(psi_ref[...], stacked(energy))
    alive = jnp.broadcast_to(live, (8, 128))
    for chunk in range(16):
        at = slice(8 * chunk, 8 * chunk + 8)
        j = plus_identity(gradients(g_ref, chunk))
        g = gradients(g_ref, chunk, 384)
        cof = cofactors(j)
        volume = j[0][0] * cof[0][0] + j[0][1] * cof[0][1] + j[0][2] * cof[0][2]
        volume = jnp.where(alive > 0.5, volume, 1.0)
        inverse = 1.0 / volume
        source = dens_low if chunk < 8 else dens_high
        mass_density = source[8 * (chunk % 8) : 8 * (chunk % 8) + 8]
        density = mass_density * inverse
        pressure = (5.0 / 3.0 - 1.0) * density * point_ref[at, :]
        spatial = [
            [
                (g[c][0] * cof[m][0] + g[c][1] * cof[m][1] + g[c][2] * cof[m][2]) * inverse
                for m in range(3)
            ]
            for c in range(3)
        ]
        drag = VISC * density
        stress = [[None] * 3 for _ in range(3)]
        for c in range(3):
            for m in range(c, 3):
                value = drag * (spatial[c][m] + spatial[m][c])
                stress[c][m] = stress[m][c] = value - pressure if c == m else value
        weight = weight_ref[at, :]
        live_weight = weight * alive
        for c in range(3):
            for m in range(3):
                flux_ref[128 * m + 8 * chunk : 128 * m + 8 * chunk + 8, 128 * c : 128 * c + 128] = (
                    -live_weight
                ) * (stress[c][0] * cof[0][m] + stress[c][1] * cof[1][m] + stress[c][2] * cof[2][m])
        power = stress[0][0] * spatial[0][0]
        for c in range(3):
            for m in range(3):
                if c + m > 0:
                    power = power + stress[c][m] * spatial[c][m]
        power_ref[at, :] = live_weight * volume * power
        wdens = weight * mass_density
        wdens_ref[at, :] = wdens
        mass_ref[at, :] = wdens * alive
    force_ref[...] = from_local(transposed_dot(grad_t_ref[...], flux_ref[...]))


def energy_kernel(power_ref, wdens_ref, psi_t_ref, take_ref, out_ref):
    table = psi_t_ref[...]
    lumped = transposed_dot(table, wdens_ref[...])
    lumped = jnp.where(lumped > 0.0, lumped, 1.0)
    rate = transposed_dot(table, power_ref[...]) / lumped
    out_ref[...] = exact_dot(rate, take_ref[...])[0:27]


def total_of(value):
    return jnp.sum(jnp.sum(value, axis=0, keepdims=True), axis=1, keepdims=True)


def mass_points(nodes, phi_ref, mass_ref):
    return dot(phi_ref[...], stacked(to_local(nodes)))


def point_energy(points, mass, own_element):
    square = (
        points[:, 0:128] * points[:, 0:128]
        + points[:, 128:256] * points[:, 128:256]
        + points[:, 256:384] * points[:, 256:384]
    )
    return total_of(jnp.sum(square * mass, axis=0, keepdims=True) * own_element)


def norm_of(nodes, own):
    return total_of(nodes * nodes * jnp.concatenate([own, own, own], axis=0))


def mass_kernel(part_ref, first_ref, second_ref, even_ref, wall_ref, mass_ref, phi_ref, phi_t_ref,
                own_ref, own_element_ref, resid_ref, image_ref, sums_ref):
    resid = shared_sum(part_ref[...], even_ref, first_ref, second_ref, wall_ref)
    resid_ref[...] = resid
    points = mass_points(resid, phi_ref, mass_ref)
    mass = mass_ref[...]
    image_ref[...] = from_local(
        transposed_dot(phi_t_ref[...], points * jnp.concatenate([mass, mass, mass], axis=1))
    )
    norm = norm_of(resid, own_ref[...])
    energy = point_energy(points, mass, own_element_ref[0:1])
    lane = lax.broadcasted_iota(jnp.int32, (8, 128), 1)
    sums_ref[...] = jnp.where(lane == 0, norm, jnp.where(lane == 1, energy, 0.0))


def moment_kernel(part_ref, first_ref, second_ref, even_ref, wall_ref, mass_ref, phi_ref, own_ref,
                  own_element_ref, sums_ref, image_ref, out_ref):
    image = shared_sum(part_ref[...], even_ref, first_ref, second_ref, wall_ref)
    image_ref[...] = image
    points = mass_points(image, phi_ref, mass_ref)
    norm = norm_of(image, own_ref[...])
    energy = point_energy(points, mass_ref[...], own_element_ref[0:1])
    lane = lax.broadcasted_iota(jnp.int32, (1, 128), 1)
    row = sums_ref[0:1] + jnp.where(lane == 2, norm, jnp.where(lane == 3, energy, 0.0))
    out_ref[...] = jnp.broadcast_to(row, out_ref.shape)


def shape_forces(u, live, grad_ref, grad_t_ref, weight_ref, g_ref, flux_ref):
    g_ref[...] = dot(grad_ref[...], stacked(to_local(u)))
    for chunk in range(16):
        at = slice(8 * chunk, 8 * chunk + 8)
        j = plus_identity(gradients(g_ref, chunk))
        cof = cofactors(j)
        volume = j[0][0] * cof[0][0] + j[0][1] * cof[0][1] + j[0][2] * cof[0][2]
        volume = jnp.where(live > 0.5, volume, 1.0)
        norm = j[0][0] * j[0][0]
        for c in range(3):
            for m in range(3):
                if c + m > 0:
                    norm = norm + j[c][m] * j[c][m]
        weight = weight_ref[at, :] * live * jnp.exp(jnp.log(volume) * (-2.0 / 3.0))
        first = weight * (2.0 / 3.0)
        second = weight * (-2.0 / 9.0) * (norm / volume)
        for c in range(3):
            for m in range(3):
                flux_ref[128 * m + 8 * chunk : 128 * m + 8 * chunk + 8, 128 * c : 128 * c + 128] = (
                    first * j[c][m] + second * cof[c][m]
                )
    return from_local(transposed_dot(grad_t_ref[...], flux_ref[...]))


def first_shape_kernel(moments_ref, disp_ref, vel_ref, resid_ref, image_ref, live_ref, step_ref,
                       grad_ref, grad_t_ref, weight_ref, newvel_ref, moved_ref, part_ref,
                       g_ref, flux_ref):
    moments = jnp.sum(moments_ref[...], axis=0, keepdims=True)
    mu0, mu1, mu2, mu3 = (moments[:, i : i + 1] for i in range(4))
    alpha = mu0 / mu1
    rest = alpha * alpha * mu2 - mu0
    beta = rest / mu0
    gain = 1.0 + beta
    second = rest / (gain * gain * mu1 - 2.0 * gain * alpha * mu2 + alpha * alpha * mu3)
    step = step_ref[0:1, 0:1]
    newvel = vel_ref[...] + step * (
        (alpha + second * gain) * resid_ref[...] - (alpha * second) * image_ref[...]
    )
    newvel_ref[...] = newvel
    moved = disp_ref[...] + step * newvel
    moved_ref[...] = moved
    part_ref[...] = shape_forces(
        moved, live_ref[...], grad_ref, grad_t_ref, weight_ref, g_ref, flux_ref
    )


def second_shape_kernel(part_ref, first_ref, second_ref, even_ref, wall_ref, newvel_ref, moved_ref,
                        live_ref, step_ref, grad_ref, grad_t_ref, weight_ref, base_ref, next_ref,
                        g_ref, flux_ref):
    gradient = shared_sum(part_ref[...], even_ref, first_ref, second_ref, wall_ref)
    u = moved_ref[...] - MESH_STEP * gradient
    part = shape_forces(u, live_ref[...], grad_ref, grad_t_ref, weight_ref, g_ref, flux_ref)
    next_ref[...] = part
    base_ref[...] = newvel_ref[...] - (MESH_STEP / step_ref[0:1, 0:1]) * (gradient + part)


def write_nodes(nodes, mask_ref, back_ref, out_ref):
    mask = mask_ref[...]
    back = back_ref[...]
    for comp in range(3):
        wide = exact_dot(nodes[ROWS * comp : ROWS * comp + ROWS], back)
        out_ref[comp : comp + 1, :] = jnp.sum(wide * mask, axis=0, keepdims=True)


def velocity_kernel(nodes_ref, mask_ref, back_ref, out_ref):
    write_nodes(nodes_ref[...], mask_ref, back_ref, out_ref)


def mesh_kernel(base_ref, above_ref, step_ref, mask_ref, back_ref, out_ref):
    zero = jnp.zeros((120, 128), F32)
    extra = add_planes(zero, zero, above_ref[...])
    nodes = base_ref[...] - (MESH_STEP / step_ref[0:1, 0:1]) * extra
    write_nodes(nodes, mask_ref, back_ref, out_ref)


def call(kernel, name, outs, scratch=(), flops=1_000_000):
    spec = pl.BlockSpec(memory_space=pltpu.VMEM)

    def run(*args):
        return pl.pallas_call(
            kernel,
            out_shape=[jax.ShapeDtypeStruct(shape, F32) for shape in outs],
            in_specs=[spec] * len(args),
            out_specs=[spec] * len(outs),
            scratch_shapes=[pltpu.VMEM(shape, F32) for shape in scratch],
            name=name,
            cost_estimate=pl.CostEstimate(flops=flops, bytes_accessed=400_000, transcendentals=0),
        )(*args)

    return run


NODES = (120, 128)
POINTS = (128, 128)


def body(displacement, velocity, energy, mass_density, live_mask, time_step):
    table = {name: jnp.asarray(value) for name, value in constants().items()}
    n_dom, n_sub = lax.axis_size("dom"), lax.axis_size("sub")
    dom, sub = lax.axis_index("dom"), lax.axis_index("sub")
    up = [(i, i + 1) for i in range(n_dom - 1)]
    down = [(i + 1, i) for i in range(n_dom - 1)]
    pairs_first = [p for i in range(0, n_dom - 1, 2) for p in ((i, i + 1), (i + 1, i))]
    pairs_second = [p for i in range(1, n_dom - 1, 2) for p in ((i, i + 1), (i + 1, i))]
    z_up = [(i, i + 1) for i in range(n_sub - 1)]
    z_down = [(i + 1, i) for i in range(n_sub - 1)]

    step = jnp.broadcast_to(time_step.reshape(1, 1), (8, 128))
    even = jnp.broadcast_to((1 - dom % 2).astype(F32).reshape(1, 1), (8, 128))
    rows = np.arange(ROWS)
    row_a = np.select([rows < 8, rows < 16, rows < 32, rows < 36],
                      [rows // 2, (rows - 8) // 2, (rows - 16) // 4, rows - 32], 9)
    row_c = np.select([rows < 8, rows < 16, rows < 32], [rows % 2 + 1, 0 * rows, rows % 2 + 1], 0)
    node_z = 3 * (np.arange(128) // 9 - BELOW)[None, :] + row_c[:, None]
    on_x = jnp.asarray(np.broadcast_to((row_a == 0)[:, None], (ROWS, 128)))
    on_z = jnp.asarray(node_z <= 0)
    wall = jnp.where((on_x & (dom == 0)) | (on_z & (sub == 0)), 0.0, 1.0).astype(F32)

    last = jnp.concatenate([displacement[:, 900:], velocity[:, 900:]], axis=0)
    halo = lax.ppermute(last, "dom", up)
    (packed,) = call(pack_kernel, "pack", [(200, 128)])(
        displacement, velocity, mass_density, energy, live_mask.reshape(1, 48), table["mask"],
        table["pick"], table["pick_high"], table["place"], table["place_high"],
    )
    (own,) = call(halo_kernel, "halo", [(200, 128)])(
        packed, halo, table["mask0"], table["pick"], table["pick_high"]
    )
    below = lax.ppermute(own, "sub", z_up)
    above = lax.ppermute(own, "sub", z_down)
    force, disp, vel, mass, live, power, wdens = call(
        force_kernel, "force",
        [NODES, NODES, NODES, POINTS, (8, 128), POINTS, POINTS],
        [(384, 768), (384, 384), POINTS],
    )(own, below, above, table["grad"], table["grad_t"], table["psi"], table["weight"])

    def swap(part):
        return lax.ppermute(part, "dom", pairs_first), lax.ppermute(part, "dom", pairs_second)

    first, second = swap(force)
    (energy_rate,) = call(energy_kernel, "energy", [(27, 48)])(
        power, wdens, table["psi_t"], table["take"]
    )
    resid, image_part, sums = call(mass_kernel, "mass", [NODES, NODES, (8, 128)])(
        force, first, second, even, wall, mass, table["phi"], table["phi_t"], table["own"],
        table["own_element"],
    )
    first, second = swap(image_part)
    image, local = call(moment_kernel, "moment", [NODES, (n_dom, 128)])(
        image_part, first, second, even, wall, mass, table["phi"], table["own"],
        table["own_element"], sums,
    )
    slab = jnp.sum(lax.all_to_all(local, "dom", 0, 0, tiled=True), axis=0, keepdims=True)
    moments = lax.all_to_all(jnp.broadcast_to(slab, (n_sub, 128)), "sub", 0, 0, tiled=True)
    newvel, moved, part = call(
        first_shape_kernel, "shape1", [NODES, NODES, NODES], [(384, 384), (384, 384)]
    )(moments, disp, vel, resid, image, live, step, table["grad"], table["grad_t"], table["weight"])
    first, second = swap(part)
    (new_velocity,) = call(velocity_kernel, "newvel", [(3, 1350)])(
        newvel, table["mask"], table["back"]
    )
    base, part = call(
        second_shape_kernel, "shape2", [NODES, NODES], [(384, 384), (384, 384)]
    )(part, first, second, even, wall, newvel, moved, live, step, table["grad"], table["grad_t"],
      table["weight"])
    from_above = lax.ppermute(part, "dom", down)
    (mesh_velocity,) = call(mesh_kernel, "mesh", [(3, 1350)])(
        base, from_above, step, table["mask"], table["back"]
    )
    return new_velocity, energy_rate, mesh_velocity


def solution(mesh):
    both = ("dom", "sub")
    return jax.shard_map(
        body,
        mesh=mesh,
        in_specs=(P(None, both), P(None, both), P(None, both), P(None, both), P(both), P()),
        out_specs=(P(None, both), P(None, both), P(None, both)),
        check_vma=False,
    )
```

```python
import functools
import math

import jax
import jax.numpy as jnp
import numpy as np
from jax import lax
from jax.experimental import pallas as pl
from jax.experimental.pallas import tpu as pltpu
from jax.sharding import PartitionSpec as P

EY = 8
EZ = 6
VISC = 0.3
MESH_STEP = 0.01
BF = jnp.bfloat16
F32 = jnp.float32
ROWS = 40
BELOW = 3
WINDOW = 13
LANE_OWN = 9 * BELOW


def node_row(a, b, c):
    if b == 0 and c > 0:
        return 2 * a + c - 1
    if b > 0 and c == 0:
        return 8 + 2 * a + b - 1
    if b > 0:
        return 16 + 4 * a + 2 * (b - 1) + c - 1
    return 32 + a


def face_row(b, c):
    if b == 0 and c > 0:
        return c - 1
    if b > 0 and c == 0:
        return 2 + b - 1
    if b > 0:
        return 4 + 2 * (b - 1) + c - 1
    return 8


def local_row(a, b, c):
    if b < 3 and c < 3:
        return node_row(a, b, c)
    if b == 3 and c < 3:
        return 48 + a if c == 0 else 40 + node_row(a, 0, c)
    if b < 3:
        return 64 + a if b == 0 else 56 + node_row(a, b, 0) - 8
    return 72 + a


def outer_triple(first, second, third):
    product = (
        first[:, None, None, :, None, None]
        * second[None, :, None, None, :, None]
        * third[None, None, :, None, None, :]
    )
    return product.reshape(
        first.shape[0] * second.shape[0] * third.shape[0],
        first.shape[1] * second.shape[1] * third.shape[1],
    )


def basis_tables():
    root_term = math.sqrt(10.0 / 7.0)
    outer = math.sqrt(5.0 + 2.0 * root_term) / 3.0
    inner = math.sqrt(5.0 - 2.0 * root_term) / 3.0
    gauss_roots = np.array([-outer, -inner, 0.0, inner, outer])
    outer_weight = (322.0 - 13.0 * math.sqrt(70.0)) / 900.0
    middle_weight = (322.0 + 13.0 * math.sqrt(70.0)) / 900.0
    weights = (
        np.array([outer_weight, middle_weight, 128.0 / 225.0, middle_weight, outer_weight]) / 2.0
    )
    points = (1.0 + gauss_roots) / 2.0
    lobatto = [0.0, (1.0 - 1.0 / math.sqrt(5.0)) / 2.0, (1.0 + 1.0 / math.sqrt(5.0)) / 2.0, 1.0]
    values = np.ones((5, 4))
    slopes = np.zeros((5, 4))
    for node in range(4):
        for other in range(4):
            if other != node:
                values[:, node] *= (points - lobatto[other]) / (lobatto[node] - lobatto[other])
        for other in range(4):
            if other != node:
                term = np.ones(5) / (lobatto[node] - lobatto[other])
                for third in range(4):
                    if third != node and third != other:
                        term = term * (points - lobatto[third]) / (lobatto[node] - lobatto[third])
                slopes[:, node] += term
    bernstein = np.stack([(1.0 - points) ** 2, 2.0 * points * (1.0 - points), points**2], axis=1)
    quad_weight = (
        weights[:, None, None] * weights[None, :, None] * weights[None, None, :]
    ).reshape(125)
    return (
        outer_triple(values, values, values),
        [
            outer_triple(slopes, values, values),
            outer_triple(values, slopes, values),
            outer_triple(values, values, slopes),
        ],
        outer_triple(bernstein, bernstein, bernstein),
        quad_weight,
    )


def split_table(table):
    high = table.astype(np.float32).astype(jnp.bfloat16)
    low = (table - high.astype(np.float64)).astype(np.float32).astype(jnp.bfloat16)
    return high, low


@functools.cache
def constants():
    vel_basis, grads, energy_basis, quad_weight = basis_tables()
    order = np.zeros(64, np.int64)
    for a in range(4):
        for b in range(4):
            for c in range(4):
                order[16 * a + 4 * b + c] = local_row(a, b, c)

    def spread_columns(table):
        wide = np.zeros((128, 80))
        wide[:125, order] = table
        return wide

    out = {}
    grad = np.concatenate([spread_columns(g) for g in grads], axis=0)
    high, low = split_table(grad)
    out["grad"] = np.concatenate([high, high, low], axis=1)
    high, low = split_table(grad.T)
    out["grad_t"] = np.concatenate([high, low], axis=0)
    phi = spread_columns(vel_basis)
    high, low = split_table(phi)
    out["phi"] = np.concatenate([high, high, low], axis=1)
    high, low = split_table(phi.T)
    out["phi_t"] = np.concatenate([high, low], axis=0)
    psi = np.zeros((128, 32))
    psi[:125, :27] = energy_basis
    high, low = split_table(psi)
    out["psi"] = np.concatenate([high, high, low], axis=1)
    high, low = split_table(psi.T)
    out["psi_t"] = np.concatenate([high, low], axis=0)
    weight = np.zeros((128, 128), np.float32)
    weight[:125] = quad_weight[:, None]
    out["weight"] = weight

    flat = np.arange(450)
    py, pz = flat // 18, flat % 18
    lane = 9 * ((pz + 1) // 3) + py // 3
    mask = np.zeros((4, ROWS, 450), np.float32)
    own = np.zeros((ROWS, 128), np.float32)
    face_mask = np.zeros((16, 454), np.float32)
    for a in range(4):
        for k in range(450):
            b, c = py[k] % 3, (pz[k] + 1) % 3
            row = node_row(a, b, c)
            mask[a, row, k] = 1.0
            if a > 0:
                own[row, lane[k] + LANE_OWN] = 1.0
            else:
                face_mask[face_row(b, c), k + 4] = 1.0
    out["mask"] = mask.reshape(4 * ROWS, 450)
    out["own"] = own
    out["face_mask"] = face_mask
    pick = np.zeros((450, 128), np.float32)
    pick[flat, lane] = 1.0
    out["pick"] = pick.astype(jnp.bfloat16)
    back = np.zeros((128, 450), np.float32)
    back[lane + LANE_OWN, flat] = 1.0
    out["back"] = back.astype(jnp.bfloat16)
    face_back = np.zeros((128, 454), np.float32)
    face_back[lane + LANE_OWN, flat + 4] = 1.0
    out["face_back"] = face_back.astype(jnp.bfloat16)
    off_x = np.ones((ROWS, 128), np.float32)
    off_z = np.ones((ROWS, 128), np.float32)
    for b in range(3):
        for c in range(3):
            for a in range(4):
                if a == 0:
                    off_x[node_row(a, b, c)] = 0.0
                off_z[node_row(a, b, c), 3 * (np.arange(128) // 9 - BELOW) + c <= 0] = 0.0
    out["off_x"] = off_x
    out["off_z"] = off_z
    element = np.arange(EY * EZ)
    elane = 9 * (element % EZ) + element // EZ
    place = np.zeros((48, 128), np.float32)
    place[element, elane] = 1.0
    out["place"] = place.astype(jnp.bfloat16)
    take = np.zeros((128, 48), np.float32)
    take[elane + LANE_OWN, element] = 1.0
    out["take"] = take.astype(jnp.bfloat16)
    own_element = np.zeros((8, 128), np.float32)
    own_element[:, elane + LANE_OWN] = 1.0
    out["own_element"] = own_element
    return out


def dot(left, right):
    return jnp.dot(left, right, preferred_element_type=F32)


def split2(value):
    high = value.astype(BF)
    return high, (value - high.astype(F32)).astype(BF)


def split3(value):
    high = value.astype(BF)
    rest = value - high.astype(F32)
    middle = rest.astype(BF)
    return high, middle, (rest - middle.astype(F32)).astype(BF)


def exact_dot(value, selection):
    high, middle, low = (part.astype(F32) for part in split3(value))
    rows = value.shape[0]
    wide = dot(jnp.concatenate([high, middle, low], axis=0).astype(BF), selection)
    return wide[:rows] + (wide[rows : 2 * rows] + wide[2 * rows :])


def stacked(value):
    high, low = split2(value)
    return jnp.concatenate([high, low, high], axis=0)


def rolled(value, by):
    return pltpu.roll(value, by % 128, 1)


def to_local(nodes):
    columns = []
    for comp in range(3):
        block = nodes[ROWS * comp : ROWS * comp + ROWS]
        corner = block[32:40]
        columns.append(
            jnp.concatenate(
                [
                    block,
                    rolled(block[0:8], -1),
                    rolled(corner, -1),
                    rolled(block[8:16], -9),
                    rolled(corner, -9),
                    rolled(corner, -10),
                ],
                axis=0,
            )
        )
    return jnp.concatenate(columns, axis=1)


def from_local(local):
    blocks = []
    for comp in range(3):
        part = local[:, 128 * comp : 128 * comp + 128]
        blocks += [
            part[0:8] + rolled(part[40:48], 1),
            part[8:16] + rolled(part[56:64], 9),
            part[16:32],
            part[32:40]
            + (rolled(part[48:56], 1) + rolled(part[64:72], 9) + rolled(part[72:80], 10)),
        ]
    return jnp.concatenate(blocks, axis=0)


def transposed_dot(table, value):
    high, low = split2(value)
    half = table.shape[0] // 2
    both = dot(table, high)
    return both[:half] + (both[half:] + dot(table[:half], low))


def turned(value, by):
    return value if by % 8 == 0 else pltpu.roll(value, by % 8, 0)


def row_index():
    return lax.broadcasted_iota(jnp.int32, (8, 128), 0)


def face_of(nodes, plane):
    row = row_index()
    by = (0, 2, 4) if plane == 0 else (2, 4, 0)
    inner = 16 if plane == 0 else 24
    blocks = []
    corners = jnp.zeros((8, 128), F32)
    for comp in range(3):
        at = ROWS * comp
        first = turned(nodes[at : at + 8], by[0])
        second = turned(nodes[at + 8 : at + 16], by[1])
        third = turned(nodes[at + inner : at + inner + 8], by[2])
        blocks.append(jnp.where(row < 2, first, jnp.where(row < 4, second, third)))
        corners = jnp.where(row == comp, turned(nodes[at + 32 : at + 40], comp - plane), corners)
    return jnp.concatenate(blocks + [corners], axis=0)


def add_faces(nodes, below, above):
    row = row_index()
    blocks = []
    for comp in range(3):
        at = ROWS * comp
        low, high = below[8 * comp : 8 * comp + 8], above[8 * comp : 8 * comp + 8]
        blocks.append(
            nodes[at : at + 8] + jnp.where(row < 2, low, jnp.where(row >= 6, turned(high, 6), 0.0))
        )
        blocks.append(
            nodes[at + 8 : at + 16]
            + jnp.where(row < 2, turned(low, 6), jnp.where(row >= 6, turned(high, 4), 0.0))
        )
        blocks.append(nodes[at + 16 : at + 24] + jnp.where(row < 4, turned(low, 4), 0.0))
        blocks.append(nodes[at + 24 : at + 32] + jnp.where(row >= 4, high, 0.0))
        low, high = turned(below[24:32], -comp), turned(above[24:32], 3 - comp)
        blocks.append(
            nodes[at + 32 : at + 40] + jnp.where(row == 0, low, jnp.where(row == 3, high, 0.0))
        )
    return jnp.concatenate(blocks, axis=0)


def flag(flags_ref, row):
    return flags_ref[row : row + 1, 0:1]


def is_even(flags_ref):
    return jnp.broadcast_to(flag(flags_ref, 0), (32, 128)) > 0.5


def send_faces(nodes, flags_ref, first_ref, second_ref):
    even = is_even(flags_ref)
    low, high = face_of(nodes, 0), face_of(nodes, 3)
    first_ref[...] = jnp.where(even, high, low)
    second_ref[...] = jnp.where(even, low, high)


def shared_sum(nodes, flags_ref, first_ref, second_ref, off_x_ref, off_z_ref):
    even = is_even(flags_ref)
    first, second = first_ref[...], second_ref[...]
    total = add_faces(nodes, jnp.where(even, second, first), jnp.where(even, first, second))
    wall = jnp.maximum(off_x_ref[...], flag(flags_ref, 1)) * jnp.maximum(
        off_z_ref[...], flag(flags_ref, 2)
    )
    return total * jnp.concatenate([wall, wall, wall], axis=0)


def cofactors(j):
    return [
        [
            j[(r + 1) % 3][(c + 1) % 3] * j[(r + 2) % 3][(c + 2) % 3]
            - j[(r + 1) % 3][(c + 2) % 3] * j[(r + 2) % 3][(c + 1) % 3]
            for c in range(3)
        ]
        for r in range(3)
    ]


def gradients(ref, chunk, base=0):
    return [
        [
            ref[128 * m + 8 * chunk : 128 * m + 8 * chunk + 8, base + 128 * c : base + 128 * c + 128]
            for m in range(3)
        ]
        for c in range(3)
    ]


def plus_identity(g):
    return [[g[c][m] + 1.0 if c == m else g[c][m] for m in range(3)] for c in range(3)]


def last_kernel(disp_ref, vel_ref, out_ref):
    out_ref[0:3, :] = disp_ref[:, 900:1350]
    out_ref[3:6, :] = vel_ref[:, 900:1350]


def add_packed(value, out_ref, at):
    half = value.shape[0] // 2
    out_ref[at : at + half, :] = value[:half] + rolled(value[half:], 64)


def pack_kernel(disp_ref, vel_ref, dens_ref, energy_ref, live_ref, mask_ref, pick_ref, place_ref,
                out_ref):
    masks = [mask_ref[ROWS * a : ROWS * a + ROWS] for a in range(1, 4)]
    blocks = []
    for ref in (disp_ref, vel_ref):
        planes = [ref[:, 450 * x : 450 * x + 450] for x in range(3)]
        for comp in range(3):
            blocks.append(
                sum(masks[x] * planes[x][comp : comp + 1, :] for x in range(3))
            )
    add_packed(exact_dot(jnp.concatenate(blocks, axis=0), pick_ref[...]), out_ref, 0)
    row = lax.broadcasted_iota(jnp.int32, (8, 48), 0)
    tail = jnp.pad(energy_ref[24:27], ((0, 5), (0, 0)))
    tail = jnp.where(row == 3, live_ref[...].astype(F32), tail)
    values = jnp.concatenate(
        [dens_ref[0:120], jnp.pad(dens_ref[120:125], ((0, 3), (0, 0))), energy_ref[0:24], tail], axis=0
    )
    placed = exact_dot(values, place_ref[...])
    add_packed(placed[0:128], out_ref, 120)
    add_packed(placed[128:160], out_ref, 184)


def halo_kernel(packed_ref, halo_ref, mask_ref, pick_ref, out_ref):
    mask = mask_ref[0:ROWS]
    blocks = [mask * halo_ref[comp : comp + 1, :] for comp in range(6)]
    nodes = exact_dot(jnp.concatenate(blocks, axis=0), pick_ref[...])
    out_ref[0:120, :] = packed_ref[0:120, :] + (nodes[:120] + rolled(nodes[120:], 64))
    out_ref[120:200, :] = packed_ref[120:200, :]


def unpack(own, below, above):
    lane = lax.broadcasted_iota(jnp.int32, own.shape, 1)
    is_own = (lane >= 27) & (lane < 90)
    is_below = lane < 36
    is_above = lane >= 81

    def window(by):
        return (
            jnp.where(is_own, rolled(own, 27 - by), 0.0)
            + jnp.where(is_below, rolled(below, -27 - by), 0.0)
            + jnp.where(is_above, rolled(above, 81 - by), 0.0)
        )

    return window(0), window(64)


def force_kernel(own_ref, below_ref, above_ref, grad_ref, grad_t_ref, psi_ref, weight_ref,
                 flags_ref, force_ref, face1_ref, face2_ref, disp_ref, vel_ref, mass_ref, live_ref,
                 power_ref, wdens_ref, g_ref, flux_ref, point_ref):
    disp, vel = unpack(own_ref[0:120], below_ref[0:120], above_ref[0:120])
    disp_ref[...] = disp
    vel_ref[...] = vel
    dens_low, dens_high = unpack(own_ref[120:184], below_ref[120:184], above_ref[120:184])
    energy_low, energy_high = unpack(own_ref[184:200], below_ref[184:200], above_ref[184:200])
    energy = jnp.concatenate([energy_low, energy_high], axis=0)
    lane = lax.broadcasted_iota(jnp.int32, (1, 128), 1)
    live = jnp.where(lane < 9 * WINDOW, energy[27:28], 0.0)
    live_ref[...] = jnp.broadcast_to(live, (8, 128))
    table = grad_ref[...]
    g_ref[:, 0:384] = dot(table, stacked(to_local(disp)))
    g_ref[:, 384:768] = dot(table, stacked(to_local(vel)))
    point_ref[...] = dot(psi_ref[...], stacked(energy))
    alive = jnp.broadcast_to(live, (8, 128))
    for chunk in range(16):
        at = slice(8 * chunk, 8 * chunk + 8)
        j = plus_identity(gradients(g_ref, chunk))
        g = gradients(g_ref, chunk, 384)
        cof = cofactors(j)
        volume = j[0][0] * cof[0][0] + j[0][1] * cof[0][1] + j[0][2] * cof[0][2]
        volume = jnp.where(alive > 0.5, volume, 1.0)
        inverse = 1.0 / volume
        source = dens_low if chunk < 8 else dens_high
        mass_density = source[8 * (chunk % 8) : 8 * (chunk % 8) + 8]
        density = mass_density * inverse
        pressure = (5.0 / 3.0 - 1.0) * density * point_ref[at, :]
        spatial = [
            [
                (g[c][0] * cof[m][0] + g[c][1] * cof[m][1] + g[c][2] * cof[m][2]) * inverse
                for m in range(3)
            ]
            for c in range(3)
        ]
        drag = VISC * density
        stress = [[None] * 3 for _ in range(3)]
        for c in range(3):
            for m in range(c, 3):
                value = drag * (spatial[c][m] + spatial[m][c])
                stress[c][m] = stress[m][c] = value - pressure if c == m else value
        weight = weight_ref[at, :]
        live_weight = weight * alive
        for c in range(3):
            for m in range(3):
                flux_ref[128 * m + 8 * chunk : 128 * m + 8 * chunk + 8, 128 * c : 128 * c + 128] = (
                    -live_weight
                ) * (stress[c][0] * cof[0][m] + stress[c][1] * cof[1][m] + stress[c][2] * cof[2][m])
        power = stress[0][0] * spatial[0][0]
        for c in range(3):
            for m in range(3):
                if c + m > 0:
                    power = power + stress[c][m] * spatial[c][m]
        power_ref[at, :] = live_weight * volume * power
        wdens = weight * mass_density
        wdens_ref[at, :] = wdens
        mass_ref[at, :] = wdens * alive
    force = from_local(transposed_dot(grad_t_ref[...], flux_ref[...]))
    force_ref[...] = force
    send_faces(force, flags_ref, face1_ref, face2_ref)


def energy_kernel(power_ref, wdens_ref, psi_t_ref, take_ref, out_ref):
    table = psi_t_ref[...]
    lumped = transposed_dot(table, wdens_ref[...])
    lumped = jnp.where(lumped > 0.0, lumped, 1.0)
    rate = transposed_dot(table, power_ref[...]) / lumped
    out_ref[...] = exact_dot(rate, take_ref[...])[0:27]


def total_of(value):
    return jnp.sum(jnp.sum(value, axis=0, keepdims=True), axis=1, keepdims=True)


def mass_points(nodes, phi_ref):
    return dot(phi_ref[...], stacked(to_local(nodes)))


def point_energy(points, mass, own_element):
    square = (
        points[:, 0:128] * points[:, 0:128]
        + points[:, 128:256] * points[:, 128:256]
        + points[:, 256:384] * points[:, 256:384]
    )
    return total_of(jnp.sum(square * mass, axis=0, keepdims=True) * own_element)


def norm_of(nodes, own):
    return total_of(nodes * nodes * jnp.concatenate([own, own, own], axis=0))


def mass_kernel(part_ref, first_ref, second_ref, flags_ref, off_x_ref, off_z_ref, mass_ref, phi_ref,
                phi_t_ref, own_ref, own_element_ref, resid_ref, image_ref, face1_ref, face2_ref,
                sums_ref):
    resid = shared_sum(part_ref[...], flags_ref, first_ref, second_ref, off_x_ref, off_z_ref)
    resid_ref[...] = resid
    points = mass_points(resid, phi_ref)
    mass = mass_ref[...]
    image = from_local(
        transposed_dot(phi_t_ref[...], points * jnp.concatenate([mass, mass, mass], axis=1))
    )
    image_ref[...] = image
    send_faces(image, flags_ref, face1_ref, face2_ref)
    norm = norm_of(resid, own_ref[...])
    energy = point_energy(points, mass, own_element_ref[0:1])
    lane = lax.broadcasted_iota(jnp.int32, (8, 128), 1)
    sums_ref[...] = jnp.where(lane == 0, norm, jnp.where(lane == 1, energy, 0.0))


def moment_kernel(part_ref, first_ref, second_ref, flags_ref, off_x_ref, off_z_ref, mass_ref, phi_ref,
                  own_ref, own_element_ref, sums_ref, image_ref, out_ref):
    image = shared_sum(part_ref[...], flags_ref, first_ref, second_ref, off_x_ref, off_z_ref)
    image_ref[...] = image
    points = mass_points(image, phi_ref)
    norm = norm_of(image, own_ref[...])
    energy = point_energy(points, mass_ref[...], own_element_ref[0:1])
    lane = lax.broadcasted_iota(jnp.int32, (1, 128), 1)
    row = sums_ref[0:1] + jnp.where(lane == 2, norm, jnp.where(lane == 3, energy, 0.0))
    out_ref[...] = jnp.broadcast_to(row, out_ref.shape)


def shape_forces(u, live, grad_ref, grad_t_ref, weight_ref, g_ref, flux_ref):
    g_ref[...] = dot(grad_ref[...], stacked(to_local(u)))
    for chunk in range(16):
        at = slice(8 * chunk, 8 * chunk + 8)
        j = plus_identity(gradients(g_ref, chunk))
        cof = cofactors(j)
        volume = j[0][0] * cof[0][0] + j[0][1] * cof[0][1] + j[0][2] * cof[0][2]
        volume = jnp.where(live > 0.5, volume, 1.0)
        norm = j[0][0] * j[0][0]
        for c in range(3):
            for m in range(3):
                if c + m > 0:
                    norm = norm + j[c][m] * j[c][m]
        weight = weight_ref[at, :] * live * jnp.exp(jnp.log(volume) * (-2.0 / 3.0))
        first = weight * (2.0 / 3.0)
        second = weight * (-2.0 / 9.0) * (norm / volume)
        for c in range(3):
            for m in range(3):
                flux_ref[128 * m + 8 * chunk : 128 * m + 8 * chunk + 8, 128 * c : 128 * c + 128] = (
                    first * j[c][m] + second * cof[c][m]
                )
    return from_local(transposed_dot(grad_t_ref[...], flux_ref[...]))


def first_shape_kernel(moments_ref, disp_ref, vel_ref, resid_ref, image_ref, live_ref, flags_ref,
                       grad_ref, grad_t_ref, weight_ref, newvel_ref, moved_ref, part_ref, face1_ref,
                       face2_ref, g_ref, flux_ref):
    moments = jnp.sum(moments_ref[...], axis=0, keepdims=True)
    mu0, mu1, mu2, mu3 = (moments[:, i : i + 1] for i in range(4))
    alpha = mu0 / mu1
    rest = alpha * alpha * mu2 - mu0
    beta = rest / mu0
    gain = 1.0 + beta
    second = rest / (gain * gain * mu1 - 2.0 * gain * alpha * mu2 + alpha * alpha * mu3)
    step = flag(flags_ref, 3)
    newvel = vel_ref[...] + step * (
        (alpha + second * gain) * resid_ref[...] - (alpha * second) * image_ref[...]
    )
    newvel_ref[...] = newvel
    moved = disp_ref[...] + step * newvel
    moved_ref[...] = moved
    part = shape_forces(moved, live_ref[...], grad_ref, grad_t_ref, weight_ref, g_ref, flux_ref)
    part_ref[...] = part
    send_faces(part, flags_ref, face1_ref, face2_ref)


def second_shape_kernel(part_ref, first_ref, second_ref, flags_ref, off_x_ref, off_z_ref, newvel_ref,
                        moved_ref, live_ref, grad_ref, grad_t_ref, weight_ref, base_ref, face_ref,
                        g_ref, flux_ref):
    gradient = shared_sum(part_ref[...], flags_ref, first_ref, second_ref, off_x_ref, off_z_ref)
    u = moved_ref[...] - MESH_STEP * gradient
    part = shape_forces(u, live_ref[...], grad_ref, grad_t_ref, weight_ref, g_ref, flux_ref)
    face_ref[...] = face_of(part, 0)
    base_ref[...] = newvel_ref[...] - (MESH_STEP / flag(flags_ref, 3)) * (gradient + part)


def write_kernel(nodes_ref, mask_ref, back_ref, out_ref):
    wide = exact_dot(nodes_ref[...], back_ref[...])
    for comp in range(3):
        part = wide[ROWS * comp : ROWS * comp + ROWS]
        planes = [
            jnp.sum(part * mask_ref[ROWS * a : ROWS * a + ROWS], axis=0, keepdims=True)
            for a in range(1, 4)
        ]
        out_ref[comp : comp + 1, :] = jnp.concatenate(planes, axis=1)


def mesh_kernel(base_ref, face_ref, flags_ref, face_mask_ref, face_back_ref, out_ref):
    scale = -MESH_STEP / flag(flags_ref, 3)
    wide = exact_dot(face_ref[...], face_back_ref[...])
    mask = face_mask_ref[0:8]
    corner = face_mask_ref[8:9]
    out_ref[:, 0:896] = base_ref[:, 0:896]
    for comp in range(3):
        extra = jnp.sum(wide[8 * comp : 8 * comp + 8] * mask, axis=0, keepdims=True)
        extra = extra + wide[24 + comp : 25 + comp] * corner
        out_ref[comp : comp + 1, 896:1350] = base_ref[comp : comp + 1, 896:1350] + scale * extra


def call(kernel, name, outs, scratch=(), flops=1_000_000):
    spec = pl.BlockSpec(memory_space=pltpu.VMEM)

    def run(*args):
        return pl.pallas_call(
            kernel,
            out_shape=[jax.ShapeDtypeStruct(shape, F32) for shape in outs],
            in_specs=[spec] * len(args),
            out_specs=[spec] * len(outs),
            scratch_shapes=[pltpu.VMEM(shape, F32) for shape in scratch],
            name=name,
            compiler_params=pltpu.CompilerParams(vmem_limit_bytes=16 * 1024 * 1024),
            cost_estimate=pl.CostEstimate(flops=flops, bytes_accessed=400_000, transcendentals=0),
        )(*args)

    return run


NODES = (120, 128)
POINTS = (128, 128)
FACE = (32, 128)


def body(displacement, velocity, energy, mass_density, live_mask, time_step):
    table = {name: jnp.asarray(value) for name, value in constants().items()}
    n_dom, n_sub = lax.axis_size("dom"), lax.axis_size("sub")
    dom, sub = lax.axis_index("dom"), lax.axis_index("sub")
    up = [(i, i + 1) for i in range(n_dom - 1)]
    down = [(i + 1, i) for i in range(n_dom - 1)]
    pairs_first = [p for i in range(0, n_dom - 1, 2) for p in ((i, i + 1), (i + 1, i))]
    pairs_second = [p for i in range(1, n_dom - 1, 2) for p in ((i, i + 1), (i + 1, i))]
    z_up = [(i, i + 1) for i in range(n_sub - 1)]
    z_down = [(i + 1, i) for i in range(n_sub - 1)]

    row = lax.broadcasted_iota(jnp.int32, (8, 128), 0)
    flags = jnp.where(
        row == 0,
        (1 - dom % 2).astype(F32),
        jnp.where(
            row == 1,
            jnp.minimum(dom, 1).astype(F32),
            jnp.where(row == 2, jnp.minimum(sub, 1).astype(F32), time_step),
        ),
    )
    walls = (table["off_x"], table["off_z"])

    (last,) = call(last_kernel, "last", [(6, 450)])(displacement, velocity)
    halo = lax.ppermute(last, "dom", up)
    (packed,) = call(pack_kernel, "pack", [(200, 128)])(
        displacement, velocity, mass_density, energy, live_mask.reshape(1, 48), table["mask"],
        table["pick"], table["place"],
    )
    (own,) = call(halo_kernel, "halo", [(200, 128)])(packed, halo, table["mask"], table["pick"])
    below = lax.ppermute(own, "sub", z_up)
    above = lax.ppermute(own, "sub", z_down)
    force, face1, face2, disp, vel, mass, live, power, wdens = call(
        force_kernel, "force",
        [NODES, FACE, FACE, NODES, NODES, POINTS, (8, 128), POINTS, POINTS],
        [(384, 768), (384, 384), POINTS],
    )(own, below, above, table["grad"], table["grad_t"], table["psi"], table["weight"], flags)

    def swap(face1, face2):
        return lax.ppermute(face1, "dom", pairs_first), lax.ppermute(face2, "dom", pairs_second)

    first, second = swap(face1, face2)
    (energy_rate,) = call(energy_kernel, "energy", [(27, 48)])(
        power, wdens, table["psi_t"], table["take"]
    )
    force, energy_rate = lax.optimization_barrier((force, energy_rate))
    resid, image_part, face1, face2, sums = call(
        mass_kernel, "mass", [NODES, NODES, FACE, FACE, (8, 128)]
    )(force, first, second, flags, *walls, mass, table["phi"], table["phi_t"], table["own"],
      table["own_element"])
    first, second = swap(face1, face2)
    image, local = call(moment_kernel, "moment", [NODES, (n_dom, 128)])(
        image_part, first, second, flags, *walls, mass, table["phi"], table["own"],
        table["own_element"], sums,
    )
    slab = jnp.sum(lax.all_to_all(local, "dom", 0, 0, tiled=True), axis=0, keepdims=True)
    moments = lax.all_to_all(jnp.broadcast_to(slab, (n_sub, 128)), "sub", 0, 0, tiled=True)
    newvel, moved, part, face1, face2 = call(
        first_shape_kernel, "shape1", [NODES, NODES, NODES, FACE, FACE], [(384, 384), (384, 384)]
    )(moments, disp, vel, resid, image, live, flags, table["grad"], table["grad_t"], table["weight"])
    first, second = swap(face1, face2)
    (new_velocity,) = call(write_kernel, "newvel", [(3, 1350)])(newvel, table["mask"], table["back"])
    part, new_velocity = lax.optimization_barrier((part, new_velocity))
    base, face = call(
        second_shape_kernel, "shape2", [NODES, FACE], [(384, 384), (384, 384)]
    )(part, first, second, flags, *walls, newvel, moved, live, table["grad"], table["grad_t"],
      table["weight"])
    from_above = lax.ppermute(face, "dom", down)
    (mesh_base,) = call(write_kernel, "base", [(3, 1350)])(base, table["mask"], table["back"])
    (mesh_velocity,) = call(mesh_kernel, "mesh", [(3, 1350)])(
        mesh_base, from_above, flags, table["face_mask"], table["face_back"]
    )
    return new_velocity, energy_rate, mesh_velocity


def solution(mesh):
    both = ("dom", "sub")
    return jax.shard_map(
        body,
        mesh=mesh,
        in_specs=(P(None, both), P(None, both), P(None, both), P(None, both), P(both), P()),
        out_specs=(P(None, both), P(None, both), P(None, both)),
        check_vma=False,
    )
```

```python
import functools
import math

import jax
import jax.numpy as jnp
import numpy as np
from jax import lax
from jax.experimental import pallas as pl
from jax.experimental.pallas import tpu as pltpu
from jax.sharding import PartitionSpec as P


EY = 8
EZ = 6
VISC = 0.3
MESH_STEP = 0.01
BF = jnp.bfloat16
F32 = jnp.float32
ROWS = 40
BELOW = 3
WINDOW = 13
LANE_OWN = 9 * BELOW


def node_row(a, b, c):
    if b == 0 and c > 0:
        return 2 * a + c - 1
    if b > 0 and c == 0:
        return 8 + 2 * a + b - 1
    if b > 0:
        return 16 + 4 * a + 2 * (b - 1) + c - 1
    return 32 + a


def face_row(b, c):
    if b == 0 and c > 0:
        return c - 1
    if b > 0 and c == 0:
        return 2 + b - 1
    if b > 0:
        return 4 + 2 * (b - 1) + c - 1
    return 8


def local_row(a, b, c):
    if b < 3 and c < 3:
        return node_row(a, b, c)
    if b == 3 and c < 3:
        return 48 + a if c == 0 else 40 + node_row(a, 0, c)
    if b < 3:
        return 64 + a if b == 0 else 56 + node_row(a, b, 0) - 8
    return 72 + a


def outer_triple(first, second, third):
    product = (
        first[:, None, None, :, None, None]
        * second[None, :, None, None, :, None]
        * third[None, None, :, None, None, :]
    )
    return product.reshape(
        first.shape[0] * second.shape[0] * third.shape[0],
        first.shape[1] * second.shape[1] * third.shape[1],
    )


def basis_tables():
    root_term = math.sqrt(10.0 / 7.0)
    outer = math.sqrt(5.0 + 2.0 * root_term) / 3.0
    inner = math.sqrt(5.0 - 2.0 * root_term) / 3.0
    gauss_roots = np.array([-outer, -inner, 0.0, inner, outer])
    outer_weight = (322.0 - 13.0 * math.sqrt(70.0)) / 900.0
    middle_weight = (322.0 + 13.0 * math.sqrt(70.0)) / 900.0
    weights = (
        np.array([outer_weight, middle_weight, 128.0 / 225.0, middle_weight, outer_weight]) / 2.0
    )
    points = (1.0 + gauss_roots) / 2.0
    lobatto = [0.0, (1.0 - 1.0 / math.sqrt(5.0)) / 2.0, (1.0 + 1.0 / math.sqrt(5.0)) / 2.0, 1.0]
    values = np.ones((5, 4))
    slopes = np.zeros((5, 4))
    for node in range(4):
        for other in range(4):
            if other != node:
                values[:, node] *= (points - lobatto[other]) / (lobatto[node] - lobatto[other])
        for other in range(4):
            if other != node:
                term = np.ones(5) / (lobatto[node] - lobatto[other])
                for third in range(4):
                    if third != node and third != other:
                        term = term * (points - lobatto[third]) / (lobatto[node] - lobatto[third])
                slopes[:, node] += term
    bernstein = np.stack([(1.0 - points) ** 2, 2.0 * points * (1.0 - points), points**2], axis=1)
    quad_weight = (
        weights[:, None, None] * weights[None, :, None] * weights[None, None, :]
    ).reshape(125)
    return (
        outer_triple(values, values, values),
        [
            outer_triple(slopes, values, values),
            outer_triple(values, slopes, values),
            outer_triple(values, values, slopes),
        ],
        outer_triple(bernstein, bernstein, bernstein),
        quad_weight,
    )


def split_table(table):
    high = table.astype(np.float32).astype(jnp.bfloat16)
    low = (table - high.astype(np.float64)).astype(np.float32).astype(jnp.bfloat16)
    return high, low


@functools.cache
def constants():
    vel_basis, grads, energy_basis, quad_weight = basis_tables()
    order = np.zeros(64, np.int64)
    for a in range(4):
        for b in range(4):
            for c in range(4):
                order[16 * a + 4 * b + c] = local_row(a, b, c)

    def spread_columns(table):
        wide = np.zeros((128, 80))
        wide[:125, order] = table
        return wide

    out = {}
    grad = np.concatenate([spread_columns(g) for g in grads], axis=0)
    high, low = split_table(grad)
    out["grad"] = np.concatenate([high, high, low], axis=1)
    high, low = split_table(grad.T)
    out["grad_t"] = np.concatenate([high, low], axis=0)
    phi = spread_columns(vel_basis)
    high, low = split_table(phi)
    out["phi"] = np.concatenate([high, high, low], axis=1)
    high, low = split_table(phi.T)
    out["phi_t"] = np.concatenate([high, low], axis=0)
    psi = np.zeros((128, 32))
    psi[:125, :27] = energy_basis
    high, low = split_table(psi)
    out["psi"] = np.concatenate([high, high, low], axis=1)
    high, low = split_table(psi.T)
    out["psi_t"] = np.concatenate([high, low], axis=0)
    weight = np.zeros((128, 128), np.float32)
    weight[:125] = quad_weight[:, None]
    out["weight"] = weight

    flat = np.arange(450)
    py, pz = flat // 18, flat % 18
    lane = 9 * ((pz + 1) // 3) + py // 3
    own = np.zeros((ROWS, 128), np.float32)
    face_mask = np.zeros((16, 454), np.float32)
    for a in range(4):
        for k in range(450):
            b, c = py[k] % 3, (pz[k] + 1) % 3
            row = node_row(a, b, c)
            if a > 0:
                own[row, lane[k] + LANE_OWN] = 1.0
            else:
                face_mask[face_row(b, c), k + 4] = 1.0
    out["own"] = own
    out["face_mask"] = face_mask
    pick = np.zeros((450, 128), np.float32)
    pick[flat, lane] = 1.0
    out["pick"] = pick.astype(jnp.bfloat16)
    back = np.zeros((128, 450), np.float32)
    back[lane + LANE_OWN, flat] = 1.0
    out["back"] = back.astype(jnp.bfloat16)
    face_back = np.zeros((128, 454), np.float32)
    face_back[lane + LANE_OWN, flat + 4] = 1.0
    out["face_back"] = face_back.astype(jnp.bfloat16)
    off_x = np.ones((ROWS, 128), np.float32)
    off_z = np.ones((ROWS, 128), np.float32)
    for b in range(3):
        for c in range(3):
            for a in range(4):
                if a == 0:
                    off_x[node_row(a, b, c)] = 0.0
                off_z[node_row(a, b, c), 3 * (np.arange(128) // 9 - BELOW) + c <= 0] = 0.0
    out["off_x"] = off_x
    out["off_z"] = off_z
    element = np.arange(EY * EZ)
    elane = 9 * (element % EZ) + element // EZ
    place = np.zeros((48, 128), np.float32)
    place[element, elane] = 1.0
    out["place"] = place.astype(jnp.bfloat16)
    take = np.zeros((128, 48), np.float32)
    take[elane + LANE_OWN, element] = 1.0
    out["take"] = take.astype(jnp.bfloat16)
    own_element = np.zeros((8, 128), np.float32)
    own_element[:, elane + LANE_OWN] = 1.0
    out["own_element"] = own_element
    return out


def dot(left, right):
    return jnp.dot(left, right, preferred_element_type=F32)


def split2(value):
    high = value.astype(BF)
    return high, (value - high.astype(F32)).astype(BF)


def split3(value):
    high = value.astype(BF)
    rest = value - high.astype(F32)
    middle = rest.astype(BF)
    return high, middle, (rest - middle.astype(F32)).astype(BF)


def exact_dot(value, selection):
    high, middle, low = (part.astype(F32) for part in split3(value))
    rows = value.shape[0]
    wide = dot(jnp.concatenate([high, middle, low], axis=0).astype(BF), selection)
    return wide[:rows] + (wide[rows : 2 * rows] + wide[2 * rows :])


def stacked(value):
    high, low = split2(value)
    return jnp.concatenate([high, low, high], axis=0)


def rolled(value, by):
    return pltpu.roll(value, by % 128, 1)


def to_local(nodes):
    columns = []
    for comp in range(3):
        block = nodes[ROWS * comp : ROWS * comp + ROWS]
        corner = block[32:40]
        columns.append(
            jnp.concatenate(
                [
                    block,
                    rolled(block[0:8], -1),
                    rolled(corner, -1),
                    rolled(block[8:16], -9),
                    rolled(corner, -9),
                    rolled(corner, -10),
                ],
                axis=0,
            )
        )
    return jnp.concatenate(columns, axis=1)


def from_local(local):
    blocks = []
    for comp in range(3):
        part = local[:, 128 * comp : 128 * comp + 128]
        blocks += [
            part[0:8] + rolled(part[40:48], 1),
            part[8:16] + rolled(part[56:64], 9),
            part[16:32],
            part[32:40]
            + (rolled(part[48:56], 1) + rolled(part[64:72], 9) + rolled(part[72:80], 10)),
        ]
    return jnp.concatenate(blocks, axis=0)


def transposed_dot(table, value):
    high, low = split2(value)
    half = table.shape[0] // 2
    both = dot(table, high)
    return both[:half] + (both[half:] + dot(table[:half], low))


def turned(value, by):
    return value if by % 8 == 0 else pltpu.roll(value, by % 8, 0)


def row_index():
    return lax.broadcasted_iota(jnp.int32, (8, 128), 0)


def face_of(nodes, plane):
    row = row_index()
    by = (0, 2, 4) if plane == 0 else (2, 4, 0)
    inner = 16 if plane == 0 else 24
    blocks = []
    corners = jnp.zeros((8, 128), F32)
    for comp in range(3):
        at = ROWS * comp
        first = turned(nodes[at : at + 8], by[0])
        second = turned(nodes[at + 8 : at + 16], by[1])
        third = turned(nodes[at + inner : at + inner + 8], by[2])
        blocks.append(jnp.where(row < 2, first, jnp.where(row < 4, second, third)))
        corners = jnp.where(row == comp, turned(nodes[at + 32 : at + 40], comp - plane), corners)
    return jnp.concatenate(blocks + [corners], axis=0)


def add_faces(nodes, below, above):
    row = row_index()
    blocks = []
    for comp in range(3):
        at = ROWS * comp
        low, high = below[8 * comp : 8 * comp + 8], above[8 * comp : 8 * comp + 8]
        blocks.append(
            nodes[at : at + 8] + jnp.where(row < 2, low, jnp.where(row >= 6, turned(high, 6), 0.0))
        )
        blocks.append(
            nodes[at + 8 : at + 16]
            + jnp.where(row < 2, turned(low, 6), jnp.where(row >= 6, turned(high, 4), 0.0))
        )
        blocks.append(nodes[at + 16 : at + 24] + jnp.where(row < 4, turned(low, 4), 0.0))
        blocks.append(nodes[at + 24 : at + 32] + jnp.where(row >= 4, high, 0.0))
        low, high = turned(below[24:32], -comp), turned(above[24:32], 3 - comp)
        blocks.append(
            nodes[at + 32 : at + 40] + jnp.where(row == 0, low, jnp.where(row == 3, high, 0.0))
        )
    return jnp.concatenate(blocks, axis=0)


def flag(flags_ref, row):
    return flags_ref[row : row + 1, 0:1]


def is_even(flags_ref, row, shape):
    place = flag(flags_ref, row)
    rest = place - 2.0 * jnp.floor(place * 0.5)
    return jnp.broadcast_to(rest, shape) < 0.5


def send_faces(nodes, flags_ref, first_ref, second_ref):
    even = is_even(flags_ref, 0, (32, 128))
    low, high = face_of(nodes, 0), face_of(nodes, 3)
    first_ref[...] = jnp.where(even, high, low)
    second_ref[...] = jnp.where(even, low, high)


def shared_sum(nodes, flags_ref, first_ref, second_ref, off_x_ref, off_z_ref):
    even = is_even(flags_ref, 0, (32, 128))
    first, second = first_ref[...], second_ref[...]
    total = add_faces(nodes, jnp.where(even, second, first), jnp.where(even, first, second))
    wall = jnp.minimum(off_x_ref[...] + flag(flags_ref, 0), 1.0) * jnp.minimum(
        off_z_ref[...] + flag(flags_ref, 1), 1.0
    )
    return total * jnp.concatenate([wall, wall, wall], axis=0)


def cofactors(j):
    return [
        [
            j[(r + 1) % 3][(c + 1) % 3] * j[(r + 2) % 3][(c + 2) % 3]
            - j[(r + 1) % 3][(c + 2) % 3] * j[(r + 2) % 3][(c + 1) % 3]
            for c in range(3)
        ]
        for r in range(3)
    ]


def gradients(ref, chunk, base=0):
    return [
        [
            ref[128 * m + 8 * chunk : 128 * m + 8 * chunk + 8, base + 128 * c : base + 128 * c + 128]
            for m in range(3)
        ]
        for c in range(3)
    ]


def plus_identity(g):
    return [[g[c][m] + 1.0 if c == m else g[c][m] for m in range(3)] for c in range(3)]


def add_packed(value, out_ref, at):
    half = value.shape[0] // 2
    out_ref[at : at + half, :] = value[:half] + rolled(value[half:], 64)


def plane_index(width):
    row = lax.broadcasted_iota(jnp.int32, (ROWS, width), 0)
    return jnp.where(
        row < 8,
        row // 2,
        jnp.where(
            row < 16,
            (row - 8) // 2,
            jnp.where(row < 32, (row - 16) // 4, jnp.where(row < 36, row - 32, 9)),
        ),
    )


def node_mask():
    row = lax.broadcasted_iota(jnp.int32, (ROWS, 450), 0)
    odd = row & 1
    row_code = jnp.where(
        row < 8,
        odd + 1,
        jnp.where(
            row < 16,
            3 * odd + 3,
            jnp.where(row < 32, 3 * ((row >> 1) & 1) + odd + 4, jnp.where(row < 36, 0, 99)),
        ),
    )
    flat = lax.broadcasted_iota(jnp.int32, (ROWS, 450), 1)
    y = (flat * 3641) >> 16
    z = flat - 18 * y + 1
    code = 3 * (y - 3 * ((y * 86) >> 8)) + z - 3 * ((z * 86) >> 8)
    return row_code == code


def last_kernel(disp_ref, vel_ref, out_ref):
    out_ref[0:3, :] = disp_ref[:, 900:1350]
    out_ref[3:6, :] = vel_ref[:, 900:1350]


def pack_kernel(disp_ref, vel_ref, dens_ref, energy_ref, live_ref, pick_ref, place_ref, out_ref):
    plane = plane_index(450)
    mask = node_mask() & (plane >= 1)
    blocks = []
    for ref in (disp_ref, vel_ref):
        planes = [ref[:, 450 * x : 450 * x + 450] for x in range(3)]
        for comp in range(3):
            first, second, third = (jnp.broadcast_to(p[comp : comp + 1], (ROWS, 450)) for p in planes)
            blocks.append(
                jnp.where(
                    mask, jnp.where(plane == 1, first, jnp.where(plane == 2, second, third)), 0.0
                )
            )
    add_packed(exact_dot(jnp.concatenate(blocks, axis=0), pick_ref[...]), out_ref, 0)
    row = lax.broadcasted_iota(jnp.int32, (8, 48), 0)
    tail = jnp.pad(energy_ref[24:27], ((0, 5), (0, 0)))
    tail = jnp.where(row == 3, live_ref[...].astype(F32), tail)
    density = jnp.pad(dens_ref[...], ((0, 0), (0, 3))).T
    placed = exact_dot(
        jnp.concatenate([density, energy_ref[0:24], tail], axis=0), place_ref[...]
    )
    add_packed(placed[0:128], out_ref, 120)
    add_packed(placed[128:160], out_ref, 184)


def halo_kernel(packed_ref, halo_ref, pick_ref, out_ref):
    mask = node_mask() & (plane_index(450) == 0)
    blocks = [
        jnp.where(mask, jnp.broadcast_to(halo_ref[comp : comp + 1, :], (ROWS, 450)), 0.0)
        for comp in range(6)
    ]
    nodes = exact_dot(jnp.concatenate(blocks, axis=0), pick_ref[...])
    out_ref[0:120, :] = packed_ref[0:120, :] + (nodes[:120] + rolled(nodes[120:], 64))
    out_ref[120:200, :] = packed_ref[120:200, :]


def unpack(own, below, above):
    lane = lax.broadcasted_iota(jnp.int32, own.shape, 1)
    is_own = (lane >= 27) & (lane < 90)
    is_below = lane < 36
    is_above = lane >= 81

    def window(by):
        return (
            jnp.where(is_own, rolled(own, 27 - by), 0.0)
            + jnp.where(is_below, rolled(below, -27 - by), 0.0)
            + jnp.where(is_above, rolled(above, 81 - by), 0.0)
        )

    return window(0), window(64)


def force_kernel(own_ref, first_ref, second_ref, grad_ref, grad_t_ref, psi_ref, weight_ref,
                 flags_ref, force_ref, face1_ref, face2_ref, disp_ref, vel_ref, mass_ref, live_ref,
                 power_ref, wdens_ref, g_ref, flux_ref, point_ref):
    even = is_even(flags_ref, 1, (200, 128))
    first, second = first_ref[...], second_ref[...]
    below = jnp.where(even, second, first)
    above = jnp.where(even, first, second)
    disp, vel = unpack(own_ref[0:120], below[0:120], above[0:120])
    disp_ref[...] = disp
    vel_ref[...] = vel
    dens_low, dens_high = unpack(own_ref[120:184], below[120:184], above[120:184])
    energy_low, energy_high = unpack(own_ref[184:200], below[184:200], above[184:200])
    energy = jnp.concatenate([energy_low, energy_high], axis=0)
    lane = lax.broadcasted_iota(jnp.int32, (1, 128), 1)
    live = jnp.where(lane < 9 * WINDOW, energy[27:28], 0.0)
    live_ref[...] = jnp.broadcast_to(live, (8, 128))
    table = grad_ref[...]
    g_ref[:, 0:384] = dot(table, stacked(to_local(disp)))
    g_ref[:, 384:768] = dot(table, stacked(to_local(vel)))
    point_ref[...] = dot(psi_ref[...], stacked(energy))
    alive = jnp.broadcast_to(live, (8, 128))
    for chunk in range(16):
        at = slice(8 * chunk, 8 * chunk + 8)
        j = plus_identity(gradients(g_ref, chunk))
        g = gradients(g_ref, chunk, 384)
        cof = cofactors(j)
        volume = j[0][0] * cof[0][0] + j[0][1] * cof[0][1] + j[0][2] * cof[0][2]
        volume = jnp.where(alive > 0.5, volume, 1.0)
        inverse = 1.0 / volume
        source = dens_low if chunk < 8 else dens_high
        mass_density = source[8 * (chunk % 8) : 8 * (chunk % 8) + 8]
        density = mass_density * inverse
        pressure = (5.0 / 3.0 - 1.0) * density * point_ref[at, :]
        spatial = [
            [
                (g[c][0] * cof[m][0] + g[c][1] * cof[m][1] + g[c][2] * cof[m][2]) * inverse
                for m in range(3)
            ]
            for c in range(3)
        ]
        drag = VISC * density
        stress = [[None] * 3 for _ in range(3)]
        for c in range(3):
            for m in range(c, 3):
                value = drag * (spatial[c][m] + spatial[m][c])
                stress[c][m] = stress[m][c] = value - pressure if c == m else value
        weight = weight_ref[at, :]
        live_weight = weight * alive
        for c in range(3):
            for m in range(3):
                flux_ref[128 * m + 8 * chunk : 128 * m + 8 * chunk + 8, 128 * c : 128 * c + 128] = (
                    -live_weight
                ) * (stress[c][0] * cof[0][m] + stress[c][1] * cof[1][m] + stress[c][2] * cof[2][m])
        power = stress[0][0] * spatial[0][0]
        for c in range(3):
            for m in range(3):
                if c + m > 0:
                    power = power + stress[c][m] * spatial[c][m]
        power_ref[at, :] = live_weight * volume * power
        wdens = weight * mass_density
        wdens_ref[at, :] = wdens
        mass_ref[at, :] = wdens * alive
    force = from_local(transposed_dot(grad_t_ref[...], flux_ref[...]))
    force_ref[...] = force
    send_faces(force, flags_ref, face1_ref, face2_ref)


def energy_kernel(power_ref, wdens_ref, psi_t_ref, take_ref, out_ref):
    table = psi_t_ref[...]
    lumped = transposed_dot(table, wdens_ref[...])
    lumped = jnp.where(lumped > 0.0, lumped, 1.0)
    rate = transposed_dot(table, power_ref[...]) / lumped
    out_ref[...] = exact_dot(rate, take_ref[...])[0:27]


def total_of(value):
    return jnp.sum(jnp.sum(value, axis=0, keepdims=True), axis=1, keepdims=True)


def mass_points(nodes, phi_ref):
    return dot(phi_ref[...], stacked(to_local(nodes)))


def point_energy(points, mass, own_element):
    square = (
        points[:, 0:128] * points[:, 0:128]
        + points[:, 128:256] * points[:, 128:256]
        + points[:, 256:384] * points[:, 256:384]
    )
    return total_of(jnp.sum(square * mass, axis=0, keepdims=True) * own_element)


def norm_of(nodes, own):
    return total_of(nodes * nodes * jnp.concatenate([own, own, own], axis=0))


def mass_kernel(part_ref, first_ref, second_ref, flags_ref, off_x_ref, off_z_ref, mass_ref, phi_ref,
                phi_t_ref, own_ref, own_element_ref, resid_ref, image_ref, face1_ref, face2_ref,
                sums_ref):
    resid = shared_sum(part_ref[...], flags_ref, first_ref, second_ref, off_x_ref, off_z_ref)
    resid_ref[...] = resid
    points = mass_points(resid, phi_ref)
    mass = mass_ref[...]
    image = from_local(
        transposed_dot(phi_t_ref[...], points * jnp.concatenate([mass, mass, mass], axis=1))
    )
    image_ref[...] = image
    send_faces(image, flags_ref, face1_ref, face2_ref)
    norm = norm_of(resid, own_ref[...])
    energy = point_energy(points, mass, own_element_ref[0:1])
    lane = lax.broadcasted_iota(jnp.int32, (8, 128), 1)
    sums_ref[...] = jnp.where(lane == 0, norm, jnp.where(lane == 1, energy, 0.0))


def moment_kernel(part_ref, first_ref, second_ref, flags_ref, off_x_ref, off_z_ref, mass_ref, phi_ref,
                  own_ref, own_element_ref, sums_ref, image_ref, out_ref):
    image = shared_sum(part_ref[...], flags_ref, first_ref, second_ref, off_x_ref, off_z_ref)
    image_ref[...] = image
    points = mass_points(image, phi_ref)
    norm = norm_of(image, own_ref[...])
    energy = point_energy(points, mass_ref[...], own_element_ref[0:1])
    lane = lax.broadcasted_iota(jnp.int32, (1, 128), 1)
    row = sums_ref[0:1] + jnp.where(lane == 2, norm, jnp.where(lane == 3, energy, 0.0))
    out_ref[...] = jnp.broadcast_to(row, out_ref.shape)


def shape_forces(u, live, grad_ref, grad_t_ref, weight_ref, g_ref, flux_ref):
    g_ref[...] = dot(grad_ref[...], stacked(to_local(u)))
    for chunk in range(16):
        at = slice(8 * chunk, 8 * chunk + 8)
        j = plus_identity(gradients(g_ref, chunk))
        cof = cofactors(j)
        volume = j[0][0] * cof[0][0] + j[0][1] * cof[0][1] + j[0][2] * cof[0][2]
        volume = jnp.where(live > 0.5, volume, 1.0)
        norm = j[0][0] * j[0][0]
        for c in range(3):
            for m in range(3):
                if c + m > 0:
                    norm = norm + j[c][m] * j[c][m]
        weight = weight_ref[at, :] * live * jnp.exp(jnp.log(volume) * (-2.0 / 3.0))
        first = weight * (2.0 / 3.0)
        second = weight * (-2.0 / 9.0) * (norm / volume)
        for c in range(3):
            for m in range(3):
                flux_ref[128 * m + 8 * chunk : 128 * m + 8 * chunk + 8, 128 * c : 128 * c + 128] = (
                    first * j[c][m] + second * cof[c][m]
                )
    return from_local(transposed_dot(grad_t_ref[...], flux_ref[...]))


def first_shape_kernel(moments_ref, disp_ref, vel_ref, resid_ref, image_ref, live_ref, flags_ref,
                       grad_ref, grad_t_ref, weight_ref, newvel_ref, moved_ref, part_ref, face1_ref,
                       face2_ref, g_ref, flux_ref):
    moments = jnp.sum(moments_ref[...], axis=0, keepdims=True)
    mu0, mu1, mu2, mu3 = (moments[:, i : i + 1] for i in range(4))
    alpha = mu0 / mu1
    rest = alpha * alpha * mu2 - mu0
    beta = rest / mu0
    gain = 1.0 + beta
    second = rest / (gain * gain * mu1 - 2.0 * gain * alpha * mu2 + alpha * alpha * mu3)
    step = flag(flags_ref, 2)
    newvel = vel_ref[...] + step * (
        (alpha + second * gain) * resid_ref[...] - (alpha * second) * image_ref[...]
    )
    newvel_ref[...] = newvel
    moved = disp_ref[...] + step * newvel
    moved_ref[...] = moved
    part = shape_forces(moved, live_ref[...], grad_ref, grad_t_ref, weight_ref, g_ref, flux_ref)
    part_ref[...] = part
    send_faces(part, flags_ref, face1_ref, face2_ref)


def second_shape_kernel(part_ref, first_ref, second_ref, flags_ref, off_x_ref, off_z_ref, newvel_ref,
                        moved_ref, live_ref, grad_ref, grad_t_ref, weight_ref, base_ref, face_ref,
                        g_ref, flux_ref):
    gradient = shared_sum(part_ref[...], flags_ref, first_ref, second_ref, off_x_ref, off_z_ref)
    u = moved_ref[...] - MESH_STEP * gradient
    part = shape_forces(u, live_ref[...], grad_ref, grad_t_ref, weight_ref, g_ref, flux_ref)
    face_ref[...] = face_of(part, 0)
    base_ref[...] = newvel_ref[...] - (MESH_STEP / flag(flags_ref, 2)) * (gradient + part)


def write_kernel(nodes_ref, back_ref, out_ref):
    wide = exact_dot(nodes_ref[...], back_ref[...])
    plane = plane_index(450)
    masks = [node_mask() & (plane == a) for a in range(1, 4)]
    for comp in range(3):
        part = wide[ROWS * comp : ROWS * comp + ROWS]
        planes = [jnp.sum(jnp.where(mask, part, 0.0), axis=0, keepdims=True) for mask in masks]
        out_ref[comp : comp + 1, :] = jnp.concatenate(planes, axis=1)


def mesh_kernel(base_ref, face_ref, flags_ref, face_mask_ref, face_back_ref, out_ref):
    scale = -MESH_STEP / flag(flags_ref, 2)
    wide = exact_dot(face_ref[...], face_back_ref[...])
    mask = face_mask_ref[0:8]
    corner = face_mask_ref[8:9]
    out_ref[:, 0:896] = base_ref[:, 0:896]
    for comp in range(3):
        extra = jnp.sum(wide[8 * comp : 8 * comp + 8] * mask, axis=0, keepdims=True)
        extra = extra + wide[24 + comp : 25 + comp] * corner
        out_ref[comp : comp + 1, 896:1350] = base_ref[comp : comp + 1, 896:1350] + scale * extra


def copying(kernel, count):
    def run(*refs):
        sources, outs = refs[:count], refs[count : -count - 1]
        copies, sems = refs[-count - 1 : -1], refs[-1]
        moves = [
            pltpu.make_async_copy(source, target, sems.at[i])
            for i, (source, target) in enumerate(zip(sources, copies))
        ]
        for move in moves:
            move.start()
        for move in moves:
            move.wait()
        kernel(*copies, *outs)

    return run


def call(kernel, outs, scratch=(), flops=1_000_000, copied=False):
    spec = pl.BlockSpec(memory_space=pltpu.VMEM)

    def run(*args):
        given, body_of = spec, kernel
        extra = [pltpu.VMEM(shape, F32) for shape in scratch]
        if copied:
            given, body_of = pl.BlockSpec(memory_space=pltpu.HBM), copying(kernel, len(args))
            extra = [pltpu.VMEM(arg.shape, arg.dtype) for arg in args]
            extra.append(pltpu.SemaphoreType.DMA((len(args),)))
            args = [pltpu.with_memory_space_constraint(arg, pltpu.HBM) for arg in args]
        return pl.pallas_call(
            body_of,
            out_shape=[jax.ShapeDtypeStruct(shape, F32) for shape in outs],
            in_specs=[given] * len(args),
            out_specs=[spec] * len(outs),
            scratch_shapes=extra,
            compiler_params=pltpu.CompilerParams(vmem_limit_bytes=16 * 1024 * 1024),
            cost_estimate=pl.CostEstimate(flops=flops, bytes_accessed=400_000, transcendentals=0),
        )(*args)

    return run


NODES = (120, 128)
POINTS = (128, 128)
FACE = (32, 128)


def body(displacement, velocity, energy, mass_density, live_mask, time_step):
    table = {name: jnp.asarray(value) for name, value in constants().items()}
    n_dom, n_sub = lax.axis_size("dom"), lax.axis_size("sub")
    dom, sub = lax.axis_index("dom"), lax.axis_index("sub")
    up = [(i, i + 1) for i in range(n_dom - 1)]
    down = [(i + 1, i) for i in range(n_dom - 1)]

    def pairs(start, size):
        return [p for i in range(start, size - 1, 2) for p in ((i, i + 1), (i + 1, i))]

    row = lax.broadcasted_iota(jnp.int32, (8, 128), 0)
    flags = jnp.where(
        row == 0, dom.astype(F32), jnp.where(row == 1, sub.astype(F32), time_step)
    )
    walls = (table["off_x"], table["off_z"])

    (last,) = call(last_kernel, [(6, 450)], copied=True)(displacement, velocity)
    halo = lax.ppermute(last, "dom", up)
    (packed,) = call(pack_kernel, [(200, 128)], copied=True)(
        displacement, velocity, mass_density.T, energy, live_mask.reshape(1, 48), table["pick"],
        table["place"],
    )
    (own,) = call(halo_kernel, [(200, 128)])(packed, halo, table["pick"])
    below = lax.ppermute(own, "sub", pairs(0, n_sub))
    above = lax.ppermute(own, "sub", pairs(1, n_sub))
    force, face1, face2, disp, vel, mass, live, power, wdens = call(
        force_kernel,
        [NODES, FACE, FACE, NODES, NODES, POINTS, (8, 128), POINTS, POINTS],
        [(384, 768), (384, 384), POINTS],
    )(own, below, above, table["grad"], table["grad_t"], table["psi"], table["weight"], flags)

    def swap(face1, face2):
        second = lax.ppermute(face2, "dom", pairs(1, n_dom))
        return lax.ppermute(face1, "dom", pairs(0, n_dom)), second

    first, second = swap(face1, face2)
    (energy_rate,) = call(energy_kernel, [(27, 48)])(power, wdens, table["psi_t"], table["take"])
    force, energy_rate = lax.optimization_barrier((force, energy_rate))
    resid, image_part, face1, face2, sums = call(
        mass_kernel, [NODES, NODES, FACE, FACE, (8, 128)]
    )(force, first, second, flags, *walls, mass, table["phi"], table["phi_t"], table["own"],
      table["own_element"])
    first, second = swap(face1, face2)
    image, local = call(moment_kernel, [NODES, (n_dom, 128)])(
        image_part, first, second, flags, *walls, mass, table["phi"], table["own"],
        table["own_element"], sums,
    )
    slab = jnp.sum(lax.all_to_all(local, "dom", 0, 0, tiled=True), axis=0, keepdims=True)
    moments = lax.all_to_all(jnp.broadcast_to(slab, (n_sub, 128)), "sub", 0, 0, tiled=True)
    newvel, moved, part, face1, face2 = call(
        first_shape_kernel, [NODES, NODES, NODES, FACE, FACE], [(384, 384), (384, 384)]
    )(moments, disp, vel, resid, image, live, flags, table["grad"], table["grad_t"], table["weight"])
    first, second = swap(face1, face2)
    (new_velocity,) = call(write_kernel, [(3, 1350)])(newvel, table["back"])
    part, new_velocity = lax.optimization_barrier((part, new_velocity))
    base, face = call(
        second_shape_kernel, [NODES, FACE], [(384, 384), (384, 384)]
    )(part, first, second, flags, *walls, newvel, moved, live, table["grad"], table["grad_t"],
      table["weight"])
    from_above = lax.ppermute(face, "dom", down)
    (mesh_base,) = call(write_kernel, [(3, 1350)])(base, table["back"])
    (mesh_velocity,) = call(mesh_kernel, [(3, 1350)])(
        mesh_base, from_above, flags, table["face_mask"], table["face_back"]
    )
    return new_velocity, energy_rate, mesh_velocity


def solution(mesh):
    both = ("dom", "sub")

    return jax.shard_map(
        body,
        mesh=mesh,
        in_specs=(P(None, both), P(None, both), P(None, both), P(None, both), P(both), P()),
        out_specs=(P(None, both), P(None, both), P(None, both)),
        check_vma=False,
    )
```

```python
import functools
import math

import jax
import jax.numpy as jnp
import numpy as np
from jax import lax
from jax.experimental import pallas as pl
from jax.experimental.pallas import tpu as pltpu
from jax.sharding import PartitionSpec as P


EY = 8
EZ = 6
VISC = 0.3
MESH_STEP = 0.01
BF = jnp.bfloat16
F32 = jnp.float32
ROWS = 40
BELOW = 3
WINDOW = 13
LANE_OWN = 9 * BELOW
BLOCK = 136


def node_row(a, b, c):
    if b == 0 and c > 0:
        return 2 * a + c - 1
    if b > 0 and c == 0:
        return 8 + 2 * a + b - 1
    if b > 0:
        return 16 + 4 * a + 2 * (b - 1) + c - 1
    return 32 + a


def face_row(b, c):
    if b == 0 and c > 0:
        return c - 1
    if b > 0 and c == 0:
        return 2 + b - 1
    if b > 0:
        return 4 + 2 * (b - 1) + c - 1
    return 8


def local_row(a, b, c):
    if b < 3 and c < 3:
        return node_row(a, b, c)
    if b == 3 and c < 3:
        return 48 + a if c == 0 else 40 + node_row(a, 0, c)
    if b < 3:
        return 64 + a if b == 0 else 56 + node_row(a, b, 0) - 8
    return 72 + a


def outer_triple(first, second, third):
    product = (
        first[:, None, None, :, None, None]
        * second[None, :, None, None, :, None]
        * third[None, None, :, None, None, :]
    )
    return product.reshape(
        first.shape[0] * second.shape[0] * third.shape[0],
        first.shape[1] * second.shape[1] * third.shape[1],
    )


def basis_tables():
    root_term = math.sqrt(10.0 / 7.0)
    outer = math.sqrt(5.0 + 2.0 * root_term) / 3.0
    inner = math.sqrt(5.0 - 2.0 * root_term) / 3.0
    gauss_roots = np.array([-outer, -inner, 0.0, inner, outer])
    outer_weight = (322.0 - 13.0 * math.sqrt(70.0)) / 900.0
    middle_weight = (322.0 + 13.0 * math.sqrt(70.0)) / 900.0
    weights = (
        np.array([outer_weight, middle_weight, 128.0 / 225.0, middle_weight, outer_weight]) / 2.0
    )
    points = (1.0 + gauss_roots) / 2.0
    lobatto = [0.0, (1.0 - 1.0 / math.sqrt(5.0)) / 2.0, (1.0 + 1.0 / math.sqrt(5.0)) / 2.0, 1.0]
    values = np.ones((5, 4))
    slopes = np.zeros((5, 4))
    for node in range(4):
        for other in range(4):
            if other != node:
                values[:, node] *= (points - lobatto[other]) / (lobatto[node] - lobatto[other])
        for other in range(4):
            if other != node:
                term = np.ones(5) / (lobatto[node] - lobatto[other])
                for third in range(4):
                    if third != node and third != other:
                        term = term * (points - lobatto[third]) / (lobatto[node] - lobatto[third])
                slopes[:, node] += term
    bernstein = np.stack([(1.0 - points) ** 2, 2.0 * points * (1.0 - points), points**2], axis=1)
    quad_weight = (
        weights[:, None, None] * weights[None, :, None] * weights[None, None, :]
    ).reshape(125)
    return (
        outer_triple(values, values, values),
        [
            outer_triple(slopes, values, values),
            outer_triple(values, slopes, values),
            outer_triple(values, values, slopes),
        ],
        outer_triple(bernstein, bernstein, bernstein),
        quad_weight,
    )


def split_table(table):
    high = table.astype(np.float32).astype(jnp.bfloat16)
    low = (table - high.astype(np.float64)).astype(np.float32).astype(jnp.bfloat16)
    return high, low


@functools.cache
def constants():
    vel_basis, grads, energy_basis, quad_weight = basis_tables()
    order = np.zeros(64, np.int64)
    for a in range(4):
        for b in range(4):
            for c in range(4):
                order[16 * a + 4 * b + c] = local_row(a, b, c)

    def spread_columns(table):
        wide = np.zeros((128, 80))
        wide[:125, order] = table
        return wide

    out = {}
    grad = np.concatenate([spread_columns(g) for g in grads], axis=0)
    high, low = split_table(grad)
    out["grad"] = np.concatenate([high, high, low], axis=1)
    high, low = split_table(grad.T)
    out["grad_t"] = np.concatenate([high, low], axis=0)
    phi = spread_columns(vel_basis)
    high, low = split_table(phi)
    out["phi"] = np.concatenate([high, high, low], axis=1)
    high, low = split_table(phi.T)
    out["phi_t"] = np.concatenate([high, low], axis=0)
    psi = np.zeros((128, 32))
    psi[:125, :27] = energy_basis
    high, low = split_table(psi)
    out["psi"] = np.concatenate([high, high, low], axis=1)
    high, low = split_table(psi.T)
    out["psi_t"] = np.concatenate([high, low], axis=0)
    weight = np.zeros((128, 128), np.float32)
    weight[:125] = quad_weight[:, None]
    out["weight"] = weight

    flat = np.arange(450)
    py, pz = flat // 18, flat % 18
    lane = 9 * ((pz + 1) // 3) + py // 3
    frame = lane - 9 * (pz % 3 == 2)
    own = np.zeros((ROWS, 128), np.float32)
    face_mask = np.zeros((16, 454), np.float32)
    for a in range(4):
        for k in range(450):
            b, c = py[k] % 3, (pz[k] + 1) % 3
            row = node_row(a, b, c)
            if a > 0:
                own[row, lane[k] + LANE_OWN] = 1.0
            else:
                face_mask[face_row(b, c), k + 4] = 1.0
    out["own"] = own
    out["face_mask"] = face_mask
    pick = np.zeros((450, 128), np.float32)
    pick[flat, frame] = 1.0
    out["pick"] = pick.astype(jnp.bfloat16)
    back = np.zeros((128, 450), np.float32)
    back[lane + LANE_OWN, flat] = 1.0
    out["back"] = back.astype(jnp.bfloat16)
    face_back = np.zeros((128, 454), np.float32)
    face_back[lane + LANE_OWN, flat + 4] = 1.0
    out["face_back"] = face_back.astype(jnp.bfloat16)
    off_x = np.ones((ROWS, 128), np.float32)
    off_z = np.ones((ROWS, 128), np.float32)
    for b in range(3):
        for c in range(3):
            for a in range(4):
                if a == 0:
                    off_x[node_row(a, b, c)] = 0.0
                off_z[node_row(a, b, c), 3 * (np.arange(128) // 9 - BELOW) + c <= 0] = 0.0
    out["off_x"] = off_x
    out["off_z"] = off_z
    element = np.arange(EY * EZ)
    elane = 9 * (element % EZ) + element // EZ
    place = np.zeros((48, 128), np.float32)
    place[element, elane] = 1.0
    out["place"] = place.astype(jnp.bfloat16)
    take = np.zeros((128, 48), np.float32)
    take[elane + LANE_OWN, element] = 1.0
    out["take"] = take.astype(jnp.bfloat16)
    own_element = np.zeros((8, 128), np.float32)
    own_element[:, elane + LANE_OWN] = 1.0
    out["own_element"] = own_element
    return out


def dot(left, right):
    return jnp.dot(left, right, preferred_element_type=F32)


def split2(value):
    high = value.astype(BF)
    return high, (value - high.astype(F32)).astype(BF)


def split3(value):
    high = value.astype(BF)
    rest = value - high.astype(F32)
    middle = rest.astype(BF)
    return high, middle, (rest - middle.astype(F32)).astype(BF)


def exact_dot(value, selection):
    high, middle, low = (part.astype(F32) for part in split3(value))
    rows = value.shape[0]
    wide = dot(jnp.concatenate([high, middle, low], axis=0).astype(BF), selection)
    return wide[:rows] + (wide[rows : 2 * rows] + wide[2 * rows :])


def stacked(value):
    high, low = split2(value)
    return jnp.concatenate([high, low, high], axis=0)


def rolled(value, by):
    return pltpu.roll(value, by % 128, 1)


def to_local(nodes):
    columns = []
    for comp in range(3):
        block = nodes[ROWS * comp : ROWS * comp + ROWS]
        corner = block[32:40]
        columns.append(
            jnp.concatenate(
                [
                    block,
                    rolled(block[0:8], -1),
                    rolled(corner, -1),
                    rolled(block[8:16], -9),
                    rolled(corner, -9),
                    rolled(corner, -10),
                ],
                axis=0,
            )
        )
    return jnp.concatenate(columns, axis=1)


def from_local(local):
    blocks = []
    for comp in range(3):
        part = local[:, 128 * comp : 128 * comp + 128]
        blocks += [
            part[0:8] + rolled(part[40:48], 1),
            part[8:16] + rolled(part[56:64], 9),
            part[16:32],
            part[32:40]
            + (rolled(part[48:56], 1) + rolled(part[64:72], 9) + rolled(part[72:80], 10)),
        ]
    return jnp.concatenate(blocks, axis=0)


def transposed_dot(table, value):
    high, low = split2(value)
    half = table.shape[0] // 2
    both = dot(table, high)
    return both[:half] + (both[half:] + dot(table[:half], low))


def turned(value, by):
    return value if by % 8 == 0 else pltpu.roll(value, by % 8, 0)


def row_index():
    return lax.broadcasted_iota(jnp.int32, (8, 128), 0)


def face_of(nodes, plane):
    row = row_index()
    by = (0, 2, 4) if plane == 0 else (2, 4, 0)
    inner = 16 if plane == 0 else 24
    blocks = []
    corners = jnp.zeros((8, 128), F32)
    for comp in range(3):
        at = ROWS * comp
        first = turned(nodes[at : at + 8], by[0])
        second = turned(nodes[at + 8 : at + 16], by[1])
        third = turned(nodes[at + inner : at + inner + 8], by[2])
        blocks.append(jnp.where(row < 2, first, jnp.where(row < 4, second, third)))
        corners = jnp.where(row == comp, turned(nodes[at + 32 : at + 40], comp - plane), corners)
    return jnp.concatenate(blocks + [corners], axis=0)


def add_faces(nodes, below, above):
    row = row_index()
    blocks = []
    for comp in range(3):
        at = ROWS * comp
        low, high = below[8 * comp : 8 * comp + 8], above[8 * comp : 8 * comp + 8]
        blocks.append(
            nodes[at : at + 8] + jnp.where(row < 2, low, jnp.where(row >= 6, turned(high, 6), 0.0))
        )
        blocks.append(
            nodes[at + 8 : at + 16]
            + jnp.where(row < 2, turned(low, 6), jnp.where(row >= 6, turned(high, 4), 0.0))
        )
        blocks.append(nodes[at + 16 : at + 24] + jnp.where(row < 4, turned(low, 4), 0.0))
        blocks.append(nodes[at + 24 : at + 32] + jnp.where(row >= 4, high, 0.0))
        low, high = turned(below[24:32], -comp), turned(above[24:32], 3 - comp)
        blocks.append(
            nodes[at + 32 : at + 40] + jnp.where(row == 0, low, jnp.where(row == 3, high, 0.0))
        )
    return jnp.concatenate(blocks, axis=0)


def flag(flags_ref, row):
    return flags_ref[row : row + 1, 0:1]


def is_even(flags_ref, row, shape):
    place = flag(flags_ref, row)
    rest = place - 2.0 * jnp.floor(place * 0.5)
    return jnp.broadcast_to(rest, shape) < 0.5


def send_faces(nodes, flags_ref, first_ref, second_ref):
    even = is_even(flags_ref, 0, (32, 128))
    low, high = face_of(nodes, 0), face_of(nodes, 3)
    first_ref[...] = jnp.where(even, high, low)
    second_ref[...] = jnp.where(even, low, high)


def shared_sum(nodes, flags_ref, first_ref, second_ref, off_x_ref, off_z_ref):
    even = is_even(flags_ref, 0, (32, 128))
    first, second = first_ref[...], second_ref[...]
    total = add_faces(nodes, jnp.where(even, second, first), jnp.where(even, first, second))
    wall = jnp.minimum(off_x_ref[...] + flag(flags_ref, 0), 1.0) * jnp.minimum(
        off_z_ref[...] + flag(flags_ref, 1), 1.0
    )
    return total * jnp.concatenate([wall, wall, wall], axis=0)


def cofactors(j):
    return [
        [
            j[(r + 1) % 3][(c + 1) % 3] * j[(r + 2) % 3][(c + 2) % 3]
            - j[(r + 1) % 3][(c + 2) % 3] * j[(r + 2) % 3][(c + 1) % 3]
            for c in range(3)
        ]
        for r in range(3)
    ]


def gradients(ref, chunk, base=0):
    return [
        [
            ref[128 * m + 8 * chunk : 128 * m + 8 * chunk + 8, base + 128 * c : base + 128 * c + 128]
            for m in range(3)
        ]
        for c in range(3)
    ]


def plus_identity(g):
    return [[g[c][m] + 1.0 if c == m else g[c][m] for m in range(3)] for c in range(3)]


def plane_index(width):
    row = lax.broadcasted_iota(jnp.int32, (ROWS, width), 0)
    return jnp.where(
        row < 8,
        row // 2,
        jnp.where(
            row < 16,
            (row - 8) // 2,
            jnp.where(row < 32, (row - 16) // 4, jnp.where(row < 36, row - 32, 9)),
        ),
    )


def node_mask():
    row = lax.broadcasted_iota(jnp.int32, (ROWS, 450), 0)
    odd = row & 1
    row_code = jnp.where(
        row < 8,
        odd + 1,
        jnp.where(
            row < 16,
            3 * odd + 3,
            jnp.where(row < 32, 3 * ((row >> 1) & 1) + odd + 4, jnp.where(row < 36, 0, 99)),
        ),
    )
    flat = lax.broadcasted_iota(jnp.int32, (ROWS, 450), 1)
    y = (flat * 3641) >> 16
    z = flat - 18 * y + 1
    code = 3 * (y - 3 * ((y * 86) >> 8)) + z - 3 * ((z * 86) >> 8)
    return row_code == code


def last_kernel(disp_ref, vel_ref, out_ref):
    out_ref[0:3, :] = disp_ref[:, 900:1350]
    out_ref[3:6, :] = vel_ref[:, 900:1350]


def pack_kernel(disp_ref, vel_ref, dens_ref, energy_ref, live_ref, pick_ref, place_ref, out_ref,
                where_ref):
    dom, sub = lax.axis_index("dom"), lax.axis_index("sub")
    where_ref[...] = jnp.where(row_index() == 0, dom.astype(F32), sub.astype(F32))
    plane = plane_index(450)
    mask = node_mask() & (plane >= 1)
    blocks = []
    for ref in (disp_ref, vel_ref):
        planes = [ref[:, 450 * x : 450 * x + 450] for x in range(3)]
        for comp in range(3):
            first, second, third = (jnp.broadcast_to(p[comp : comp + 1], (ROWS, 450)) for p in planes)
            blocks.append(
                jnp.where(
                    mask, jnp.where(plane == 1, first, jnp.where(plane == 2, second, third)), 0.0
                )
            )
    out_ref[0:240, :] = exact_dot(jnp.concatenate(blocks, axis=0), pick_ref[...])
    row = lax.broadcasted_iota(jnp.int32, (8, 48), 0)
    tail = jnp.pad(energy_ref[24:27], ((0, 5), (0, 0)))
    tail = jnp.where(row == 3, live_ref[...].astype(F32), tail)
    density = jnp.pad(dens_ref[...], ((0, 0), (0, 3))).T
    out_ref[240:400, :] = exact_dot(
        jnp.concatenate([density, energy_ref[0:24], tail], axis=0), place_ref[...]
    )


def send_columns(value, start):
    lane = lax.broadcasted_iota(jnp.int32, (BLOCK, 128), 1)
    value = jnp.concatenate([value, jnp.zeros((3 * BLOCK - 400, 128), F32)], axis=0)
    parts = [rolled(value[BLOCK * i : BLOCK * i + BLOCK], 36 * i - start) for i in range(3)]
    return jnp.where(lane < 36, parts[0], jnp.where(lane < 72, parts[1], parts[2]))


def halo_kernel(packed_ref, halo_ref, pick_ref, where_ref, own_ref, first_ref, second_ref):
    mask = node_mask() & (plane_index(450) == 0)
    blocks = [
        jnp.where(mask, jnp.broadcast_to(halo_ref[comp : comp + 1, :], (ROWS, 450)), 0.0)
        for comp in range(6)
    ]
    nodes = exact_dot(jnp.concatenate(blocks, axis=0), pick_ref[...])
    own = jnp.concatenate([packed_ref[0:240] + nodes, packed_ref[240:400]], axis=0)
    own_ref[...] = own
    up, down = send_columns(own, 18), send_columns(own, 0)
    even = is_even(where_ref, 1, (BLOCK, 128))
    first_ref[...] = jnp.where(even, up, down)
    second_ref[...] = jnp.where(even, down, up)


def unpack(own, below, above):
    lane = lax.broadcasted_iota(jnp.int32, (8, 128), 1)
    rows = []
    for at in range(0, 400, 8):
        block, inner = at // BLOCK, at % BLOCK
        on_vertex = 9 if at < 240 and at % ROWS in (8, 32) else 0
        base = 36 * block
        mine = rolled(own[at : at + 8], 27 + on_vertex)
        low = rolled(below[inner : inner + 8], on_vertex - 9 - base)
        high = rolled(above[inner : inner + 8], 81 + on_vertex - base)
        rows.append(
            jnp.where(
                lane < 27 + on_vertex, low, jnp.where(lane < 81 + on_vertex, mine, high)
            )
        )
    return jnp.concatenate(rows, axis=0)


def force_kernel(own_ref, first_ref, second_ref, grad_ref, grad_t_ref, psi_ref, weight_ref,
                 flags_ref, force_ref, face1_ref, face2_ref, disp_ref, vel_ref, mass_ref, live_ref,
                 power_ref, wdens_ref, g_ref, flux_ref, point_ref):
    even = is_even(flags_ref, 1, (BLOCK, 128))
    first, second = first_ref[...], second_ref[...]
    window = unpack(own_ref[...], jnp.where(even, second, first), jnp.where(even, first, second))
    disp, vel, energy = window[0:120], window[120:240], window[368:400]
    disp_ref[...] = disp
    vel_ref[...] = vel
    lane = lax.broadcasted_iota(jnp.int32, (1, 128), 1)
    live = jnp.where(lane < 9 * WINDOW, energy[27:28], 0.0)
    live_ref[...] = jnp.broadcast_to(live, (8, 128))
    table = grad_ref[...]
    g_ref[:, 0:384] = dot(table, stacked(to_local(disp)))
    g_ref[:, 384:768] = dot(table, stacked(to_local(vel)))
    point_ref[...] = dot(psi_ref[...], stacked(energy))
    alive = jnp.broadcast_to(live, (8, 128))
    for chunk in range(16):
        at = slice(8 * chunk, 8 * chunk + 8)
        j = plus_identity(gradients(g_ref, chunk))
        g = gradients(g_ref, chunk, 384)
        cof = cofactors(j)
        volume = j[0][0] * cof[0][0] + j[0][1] * cof[0][1] + j[0][2] * cof[0][2]
        volume = jnp.where(alive > 0.5, volume, 1.0)
        inverse = 1.0 / volume
        mass_density = window[240 + 8 * chunk : 248 + 8 * chunk]
        density = mass_density * inverse
        pressure = (5.0 / 3.0 - 1.0) * density * point_ref[at, :]
        spatial = [
            [
                (g[c][0] * cof[m][0] + g[c][1] * cof[m][1] + g[c][2] * cof[m][2]) * inverse
                for m in range(3)
            ]
            for c in range(3)
        ]
        drag = VISC * density
        stress = [[None] * 3 for _ in range(3)]
        for c in range(3):
            for m in range(c, 3):
                value = drag * (spatial[c][m] + spatial[m][c])
                stress[c][m] = stress[m][c] = value - pressure if c == m else value
        weight = weight_ref[at, :]
        live_weight = weight * alive
        for c in range(3):
            for m in range(3):
                flux_ref[128 * m + 8 * chunk : 128 * m + 8 * chunk + 8, 128 * c : 128 * c + 128] = (
                    -live_weight
                ) * (stress[c][0] * cof[0][m] + stress[c][1] * cof[1][m] + stress[c][2] * cof[2][m])
        power = stress[0][0] * spatial[0][0]
        for c in range(3):
            for m in range(3):
                if c + m > 0:
                    power = power + stress[c][m] * spatial[c][m]
        power_ref[at, :] = live_weight * volume * power
        wdens = weight * mass_density
        wdens_ref[at, :] = wdens
        mass_ref[at, :] = wdens * alive
    force = from_local(transposed_dot(grad_t_ref[...], flux_ref[...]))
    force_ref[...] = force
    send_faces(force, flags_ref, face1_ref, face2_ref)


def energy_kernel(power_ref, wdens_ref, psi_t_ref, take_ref, out_ref):
    table = psi_t_ref[...]
    lumped = transposed_dot(table, wdens_ref[...])
    lumped = jnp.where(lumped > 0.0, lumped, 1.0)
    rate = transposed_dot(table, power_ref[...]) / lumped
    out_ref[...] = exact_dot(rate, take_ref[...])[0:27]


def total_of(value):
    return jnp.sum(jnp.sum(value, axis=0, keepdims=True), axis=1, keepdims=True)


def mass_points(nodes, phi_ref):
    return dot(phi_ref[...], stacked(to_local(nodes)))


def point_energy(points, mass, own_element):
    square = (
        points[:, 0:128] * points[:, 0:128]
        + points[:, 128:256] * points[:, 128:256]
        + points[:, 256:384] * points[:, 256:384]
    )
    return total_of(jnp.sum(square * mass, axis=0, keepdims=True) * own_element)


def norm_of(nodes, own):
    return total_of(nodes * nodes * jnp.concatenate([own, own, own], axis=0))


def mass_kernel(part_ref, first_ref, second_ref, flags_ref, off_x_ref, off_z_ref, mass_ref, phi_ref,
                phi_t_ref, own_ref, own_element_ref, resid_ref, image_ref, face1_ref, face2_ref,
                sums_ref):
    resid = shared_sum(part_ref[...], flags_ref, first_ref, second_ref, off_x_ref, off_z_ref)
    resid_ref[...] = resid
    points = mass_points(resid, phi_ref)
    mass = mass_ref[...]
    image = from_local(
        transposed_dot(phi_t_ref[...], points * jnp.concatenate([mass, mass, mass], axis=1))
    )
    image_ref[...] = image
    send_faces(image, flags_ref, face1_ref, face2_ref)
    norm = norm_of(resid, own_ref[...])
    energy = point_energy(points, mass, own_element_ref[0:1])
    lane = lax.broadcasted_iota(jnp.int32, (8, 128), 1)
    sums_ref[...] = jnp.where(lane == 0, norm, jnp.where(lane == 1, energy, 0.0))


def moment_kernel(part_ref, first_ref, second_ref, flags_ref, off_x_ref, off_z_ref, mass_ref, phi_ref,
                  own_ref, own_element_ref, sums_ref, image_ref, out_ref):
    image = shared_sum(part_ref[...], flags_ref, first_ref, second_ref, off_x_ref, off_z_ref)
    image_ref[...] = image
    points = mass_points(image, phi_ref)
    norm = norm_of(image, own_ref[...])
    energy = point_energy(points, mass_ref[...], own_element_ref[0:1])
    lane = lax.broadcasted_iota(jnp.int32, (1, 128), 1)
    row = sums_ref[0:1] + jnp.where(lane == 2, norm, jnp.where(lane == 3, energy, 0.0))
    out_ref[...] = jnp.broadcast_to(row, out_ref.shape)


def shape_forces(u, live, grad_ref, grad_t_ref, weight_ref, g_ref, flux_ref):
    g_ref[...] = dot(grad_ref[...], stacked(to_local(u)))
    for chunk in range(16):
        at = slice(8 * chunk, 8 * chunk + 8)
        j = plus_identity(gradients(g_ref, chunk))
        cof = cofactors(j)
        volume = j[0][0] * cof[0][0] + j[0][1] * cof[0][1] + j[0][2] * cof[0][2]
        volume = jnp.where(live > 0.5, volume, 1.0)
        norm = j[0][0] * j[0][0]
        for c in range(3):
            for m in range(3):
                if c + m > 0:
                    norm = norm + j[c][m] * j[c][m]
        weight = weight_ref[at, :] * live * jnp.exp(jnp.log(volume) * (-2.0 / 3.0))
        first = weight * (2.0 / 3.0)
        second = weight * (-2.0 / 9.0) * (norm / volume)
        for c in range(3):
            for m in range(3):
                flux_ref[128 * m + 8 * chunk : 128 * m + 8 * chunk + 8, 128 * c : 128 * c + 128] = (
                    first * j[c][m] + second * cof[c][m]
                )
    return from_local(transposed_dot(grad_t_ref[...], flux_ref[...]))


def first_shape_kernel(moments_ref, disp_ref, vel_ref, resid_ref, image_ref, live_ref, flags_ref,
                       grad_ref, grad_t_ref, weight_ref, newvel_ref, moved_ref, part_ref, face1_ref,
                       face2_ref, g_ref, flux_ref):
    moments = jnp.sum(moments_ref[...], axis=0, keepdims=True)
    mu0, mu1, mu2, mu3 = (moments[:, i : i + 1] for i in range(4))
    alpha = mu0 / mu1
    rest = alpha * alpha * mu2 - mu0
    beta = rest / mu0
    gain = 1.0 + beta
    second = rest / (gain * gain * mu1 - 2.0 * gain * alpha * mu2 + alpha * alpha * mu3)
    step = flag(flags_ref, 2)
    newvel = vel_ref[...] + step * (
        (alpha + second * gain) * resid_ref[...] - (alpha * second) * image_ref[...]
    )
    newvel_ref[...] = newvel
    moved = disp_ref[...] + step * newvel
    moved_ref[...] = moved
    part = shape_forces(moved, live_ref[...], grad_ref, grad_t_ref, weight_ref, g_ref, flux_ref)
    part_ref[...] = part
    send_faces(part, flags_ref, face1_ref, face2_ref)


def second_shape_kernel(part_ref, first_ref, second_ref, flags_ref, off_x_ref, off_z_ref, newvel_ref,
                        moved_ref, live_ref, grad_ref, grad_t_ref, weight_ref, base_ref, face_ref,
                        g_ref, flux_ref):
    gradient = shared_sum(part_ref[...], flags_ref, first_ref, second_ref, off_x_ref, off_z_ref)
    u = moved_ref[...] - MESH_STEP * gradient
    part = shape_forces(u, live_ref[...], grad_ref, grad_t_ref, weight_ref, g_ref, flux_ref)
    face_ref[...] = face_of(part, 0)
    base_ref[...] = newvel_ref[...] - (MESH_STEP / flag(flags_ref, 2)) * (gradient + part)


def write_kernel(nodes_ref, back_ref, out_ref):
    wide = exact_dot(nodes_ref[...], back_ref[...])
    plane = plane_index(450)
    masks = [node_mask() & (plane == a) for a in range(1, 4)]
    for comp in range(3):
        part = wide[ROWS * comp : ROWS * comp + ROWS]
        planes = [jnp.sum(jnp.where(mask, part, 0.0), axis=0, keepdims=True) for mask in masks]
        out_ref[comp : comp + 1, :] = jnp.concatenate(planes, axis=1)


def mesh_kernel(base_ref, face_ref, flags_ref, face_mask_ref, face_back_ref, out_ref):
    scale = -MESH_STEP / flag(flags_ref, 2)
    wide = exact_dot(face_ref[...], face_back_ref[...])
    mask = face_mask_ref[0:8]
    corner = face_mask_ref[8:9]
    out_ref[:, 0:896] = base_ref[:, 0:896]
    for comp in range(3):
        extra = jnp.sum(wide[8 * comp : 8 * comp + 8] * mask, axis=0, keepdims=True)
        extra = extra + wide[24 + comp : 25 + comp] * corner
        out_ref[comp : comp + 1, 896:1350] = base_ref[comp : comp + 1, 896:1350] + scale * extra


def copying(kernel, count):
    def run(*refs):
        sources, outs = refs[:count], refs[count : -count - 1]
        copies, sems = refs[-count - 1 : -1], refs[-1]
        moves = [
            pltpu.make_async_copy(source, target, sems.at[i])
            for i, (source, target) in enumerate(zip(sources, copies))
        ]
        for move in moves:
            move.start()
        for move in moves:
            move.wait()
        kernel(*copies, *outs)

    return run


def call(kernel, outs, scratch=(), flops=1_000_000, copied=False):
    spec = pl.BlockSpec(memory_space=pltpu.VMEM)

    def run(*args):
        given, body_of = spec, kernel
        extra = [pltpu.VMEM(shape, F32) for shape in scratch]
        if copied:
            given, body_of = pl.BlockSpec(memory_space=pltpu.HBM), copying(kernel, len(args))
            extra = [pltpu.VMEM(arg.shape, arg.dtype) for arg in args]
            extra.append(pltpu.SemaphoreType.DMA((len(args),)))
            args = [pltpu.with_memory_space_constraint(arg, pltpu.HBM) for arg in args]
        return pl.pallas_call(
            body_of,
            out_shape=[jax.ShapeDtypeStruct(shape, F32) for shape in outs],
            in_specs=[given] * len(args),
            out_specs=[spec] * len(outs),
            scratch_shapes=extra,
            compiler_params=pltpu.CompilerParams(vmem_limit_bytes=16 * 1024 * 1024),
            cost_estimate=pl.CostEstimate(flops=flops, bytes_accessed=400_000, transcendentals=0),
        )(*args)

    return run


NODES = (120, 128)
POINTS = (128, 128)
FACE = (32, 128)


def body(displacement, velocity, energy, mass_density, live_mask, time_step):
    table = {name: jnp.asarray(value) for name, value in constants().items()}
    n_dom, n_sub = lax.axis_size("dom"), lax.axis_size("sub")
    up = [(i, i + 1) for i in range(n_dom - 1)]
    down = [(i + 1, i) for i in range(n_dom - 1)]

    def pairs(start, size):
        return [p for i in range(start, size - 1, 2) for p in ((i, i + 1), (i + 1, i))]

    walls = (table["off_x"], table["off_z"])

    (last,) = call(last_kernel, [(6, 450)], copied=True)(displacement, velocity)
    halo = lax.ppermute(last, "dom", up)
    packed, where = call(pack_kernel, [(400, 128), (8, 128)], copied=True)(
        displacement, velocity, mass_density.T, energy, live_mask.reshape(1, 48), table["pick"],
        table["place"],
    )
    row = lax.broadcasted_iota(jnp.int32, (8, 128), 0)
    own, z_first, z_second = call(
        halo_kernel, [(400, 128), (BLOCK, 128), (BLOCK, 128)]
    )(packed, halo, table["pick"], where)
    flags = jnp.where(row < 2, where, time_step)
    first = lax.ppermute(z_first, "sub", pairs(0, n_sub))
    second = lax.ppermute(z_second, "sub", pairs(1, n_sub))
    force, face1, face2, disp, vel, mass, live, power, wdens = call(
        force_kernel,
        [NODES, FACE, FACE, NODES, NODES, POINTS, (8, 128), POINTS, POINTS],
        [(384, 768), (384, 384), POINTS],
    )(own, first, second, table["grad"], table["grad_t"], table["psi"], table["weight"], flags)

    def swap(face1, face2):
        second = lax.ppermute(face2, "dom", pairs(1, n_dom))
        return lax.ppermute(face1, "dom", pairs(0, n_dom)), second

    first, second = swap(face1, face2)
    (energy_rate,) = call(energy_kernel, [(27, 48)])(power, wdens, table["psi_t"], table["take"])
    force, energy_rate = lax.optimization_barrier((force, energy_rate))
    resid, image_part, face1, face2, sums = call(
        mass_kernel, [NODES, NODES, FACE, FACE, (8, 128)]
    )(force, first, second, flags, *walls, mass, table["phi"], table["phi_t"], table["own"],
      table["own_element"])
    first, second = swap(face1, face2)
    image, local = call(moment_kernel, [NODES, (n_dom, 128)])(
        image_part, first, second, flags, *walls, mass, table["phi"], table["own"],
        table["own_element"], sums,
    )
    slab = jnp.sum(lax.all_to_all(local, "dom", 0, 0, tiled=True), axis=0, keepdims=True)
    moments = lax.all_to_all(jnp.broadcast_to(slab, (n_sub, 128)), "sub", 0, 0, tiled=True)
    newvel, moved, part, face1, face2 = call(
        first_shape_kernel, [NODES, NODES, NODES, FACE, FACE], [(384, 384), (384, 384)]
    )(moments, disp, vel, resid, image, live, flags, table["grad"], table["grad_t"], table["weight"])
    first, second = swap(face1, face2)
    (new_velocity,) = call(write_kernel, [(3, 1350)])(newvel, table["back"])
    part, new_velocity = lax.optimization_barrier((part, new_velocity))
    base, face = call(
        second_shape_kernel, [NODES, FACE], [(384, 384), (384, 384)]
    )(part, first, second, flags, *walls, newvel, moved, live, table["grad"], table["grad_t"],
      table["weight"])
    from_above = lax.ppermute(face, "dom", down)
    (mesh_base,) = call(write_kernel, [(3, 1350)])(base, table["back"])
    (mesh_velocity,) = call(mesh_kernel, [(3, 1350)])(
        mesh_base, from_above, flags, table["face_mask"], table["face_back"]
    )
    return new_velocity, energy_rate, mesh_velocity


def solution(mesh):
    both = ("dom", "sub")

    return jax.shard_map(
        body,
        mesh=mesh,
        in_specs=(P(None, both), P(None, both), P(None, both), P(None, both), P(both), P()),
        out_specs=(P(None, both), P(None, both), P(None, both)),
        check_vma=False,
    )
```

```python
import functools
import math

import jax
import jax.numpy as jnp
import numpy as np
from jax import lax
from jax.experimental import pallas as pl
from jax.experimental.pallas import tpu as pltpu
from jax.sharding import PartitionSpec as P


EY = 8
EZ = 6
VISC = 0.3
MESH_STEP = 0.01
BF = jnp.bfloat16
F32 = jnp.float32
ROWS = 40
BELOW = 3
WINDOW = 13
LANE_OWN = 9 * BELOW
BLOCK = 136


def node_row(a, b, c):
    if b == 0 and c > 0:
        return 2 * a + c - 1
    if b > 0 and c == 0:
        return 8 + 2 * a + b - 1
    if b > 0:
        return 16 + 4 * a + 2 * (b - 1) + c - 1
    return 32 + a


def local_row(a, b, c):
    if b < 3 and c < 3:
        return node_row(a, b, c)
    if b == 3 and c < 3:
        return 48 + a if c == 0 else 40 + node_row(a, 0, c)
    if b < 3:
        return 64 + a if b == 0 else 56 + node_row(a, b, 0) - 8
    return 72 + a


def outer_triple(first, second, third):
    product = (
        first[:, None, None, :, None, None]
        * second[None, :, None, None, :, None]
        * third[None, None, :, None, None, :]
    )
    return product.reshape(
        first.shape[0] * second.shape[0] * third.shape[0],
        first.shape[1] * second.shape[1] * third.shape[1],
    )


def basis_tables():
    root_term = math.sqrt(10.0 / 7.0)
    outer = math.sqrt(5.0 + 2.0 * root_term) / 3.0
    inner = math.sqrt(5.0 - 2.0 * root_term) / 3.0
    gauss_roots = np.array([-outer, -inner, 0.0, inner, outer])
    outer_weight = (322.0 - 13.0 * math.sqrt(70.0)) / 900.0
    middle_weight = (322.0 + 13.0 * math.sqrt(70.0)) / 900.0
    weights = (
        np.array([outer_weight, middle_weight, 128.0 / 225.0, middle_weight, outer_weight]) / 2.0
    )
    points = (1.0 + gauss_roots) / 2.0
    lobatto = [0.0, (1.0 - 1.0 / math.sqrt(5.0)) / 2.0, (1.0 + 1.0 / math.sqrt(5.0)) / 2.0, 1.0]
    values = np.ones((5, 4))
    slopes = np.zeros((5, 4))
    for node in range(4):
        for other in range(4):
            if other != node:
                values[:, node] *= (points - lobatto[other]) / (lobatto[node] - lobatto[other])
        for other in range(4):
            if other != node:
                term = np.ones(5) / (lobatto[node] - lobatto[other])
                for third in range(4):
                    if third != node and third != other:
                        term = term * (points - lobatto[third]) / (lobatto[node] - lobatto[third])
                slopes[:, node] += term
    bernstein = np.stack([(1.0 - points) ** 2, 2.0 * points * (1.0 - points), points**2], axis=1)
    quad_weight = (
        weights[:, None, None] * weights[None, :, None] * weights[None, None, :]
    ).reshape(125)
    return (
        outer_triple(values, values, values),
        [
            outer_triple(slopes, values, values),
            outer_triple(values, slopes, values),
            outer_triple(values, values, slopes),
        ],
        outer_triple(bernstein, bernstein, bernstein),
        quad_weight,
    )


def split_table(table):
    high = table.astype(np.float32).astype(jnp.bfloat16)
    low = (table - high.astype(np.float64)).astype(np.float32).astype(jnp.bfloat16)
    return high, low


@functools.cache
def constants():
    vel_basis, grads, energy_basis, quad_weight = basis_tables()
    order = np.zeros(64, np.int64)
    for a in range(4):
        for b in range(4):
            for c in range(4):
                order[16 * a + 4 * b + c] = local_row(a, b, c)

    def spread_columns(table):
        wide = np.zeros((128, 80))
        wide[:125, order] = table
        return wide

    out = {}
    grad = np.concatenate([spread_columns(g) for g in grads], axis=0)
    high, low = split_table(grad)
    out["grad"] = np.concatenate([high, high, low], axis=1)
    high, low = split_table(grad.T)
    out["grad_t"] = np.concatenate([high, low], axis=0)
    phi = spread_columns(vel_basis)
    high, low = split_table(phi)
    out["phi"] = np.concatenate([high, high, low], axis=1)
    high, low = split_table(phi.T)
    out["phi_t"] = np.concatenate([high, low], axis=0)
    psi = np.zeros((128, 32))
    psi[:125, :27] = energy_basis
    high, low = split_table(psi)
    out["psi"] = np.concatenate([high, high, low], axis=1)
    high, low = split_table(psi.T)
    out["psi_t"] = np.concatenate([high, low], axis=0)
    weight = np.zeros((128, 128), np.float32)
    weight[:125] = quad_weight[:, None]
    out["weight"] = weight

    flat = np.arange(450)
    py, pz = flat // 18, flat % 18
    lane = 9 * ((pz + 1) // 3) + py // 3
    frame = lane - 9 * (pz % 3 == 2)
    own = np.zeros((ROWS, 128), np.float32)
    for a in range(4):
        for k in range(450):
            b, c = py[k] % 3, (pz[k] + 1) % 3
            row = node_row(a, b, c)
            if a > 0:
                own[row, lane[k] + LANE_OWN] = 1.0
    out["own"] = own
    pick = np.zeros((450, 128), np.float32)
    pick[flat, frame] = 1.0
    out["pick"] = pick.astype(jnp.bfloat16)
    back = np.zeros((128, 450), np.float32)
    back[lane + LANE_OWN, flat] = 1.0
    out["back"] = back.astype(jnp.bfloat16)
    off_x = np.ones((ROWS, 128), np.float32)
    off_z = np.ones((ROWS, 128), np.float32)
    for b in range(3):
        for c in range(3):
            for a in range(4):
                if a == 0:
                    off_x[node_row(a, b, c)] = 0.0
                off_z[node_row(a, b, c), 3 * (np.arange(128) // 9 - BELOW) + c <= 0] = 0.0
    out["off_x"] = off_x
    out["off_z"] = off_z
    element = np.arange(EY * EZ)
    elane = 9 * (element % EZ) + element // EZ
    place = np.zeros((48, 128), np.float32)
    place[element, elane] = 1.0
    out["place"] = place.astype(jnp.bfloat16)
    take = np.zeros((128, 48), np.float32)
    take[elane + LANE_OWN, element] = 1.0
    out["take"] = take.astype(jnp.bfloat16)
    own_element = np.zeros((8, 128), np.float32)
    own_element[:, elane + LANE_OWN] = 1.0
    out["own_element"] = own_element
    return out


def dot(left, right):
    return jnp.dot(left, right, preferred_element_type=F32)


def split2(value):
    high = value.astype(BF)
    return high, (value - high.astype(F32)).astype(BF)


def split3(value):
    high = value.astype(BF)
    rest = value - high.astype(F32)
    middle = rest.astype(BF)
    return high, middle, (rest - middle.astype(F32)).astype(BF)


def exact_dot(value, selection):
    high, middle, low = (part.astype(F32) for part in split3(value))
    rows = value.shape[0]
    wide = dot(jnp.concatenate([high, middle, low], axis=0).astype(BF), selection)
    return wide[:rows] + (wide[rows : 2 * rows] + wide[2 * rows :])


def stacked(value):
    high, low = split2(value)
    return jnp.concatenate([high, low, high], axis=0)


def rolled(value, by):
    return pltpu.roll(value, by % 128, 1)


def to_local(nodes):
    columns = []
    for comp in range(3):
        block = nodes[ROWS * comp : ROWS * comp + ROWS]
        corner = block[32:40]
        columns.append(
            jnp.concatenate(
                [
                    block,
                    rolled(block[0:8], -1),
                    rolled(corner, -1),
                    rolled(block[8:16], -9),
                    rolled(corner, -9),
                    rolled(corner, -10),
                ],
                axis=0,
            )
        )
    return jnp.concatenate(columns, axis=1)


def from_local(local):
    blocks = []
    for comp in range(3):
        part = local[:, 128 * comp : 128 * comp + 128]
        blocks += [
            part[0:8] + rolled(part[40:48], 1),
            part[8:16] + rolled(part[56:64], 9),
            part[16:32],
            part[32:40]
            + (rolled(part[48:56], 1) + rolled(part[64:72], 9) + rolled(part[72:80], 10)),
        ]
    return jnp.concatenate(blocks, axis=0)


def transposed_dot(table, value):
    high, low = split2(value)
    half = table.shape[0] // 2
    both = dot(table, high)
    return both[:half] + (both[half:] + dot(table[:half], low))


def turned(value, by):
    return value if by % 8 == 0 else pltpu.roll(value, by % 8, 0)


def row_index():
    return lax.broadcasted_iota(jnp.int32, (8, 128), 0)


def face_of(nodes, plane):
    row = row_index()
    by = (0, 2, 4) if plane == 0 else (2, 4, 0)
    inner = 16 if plane == 0 else 24
    blocks = []
    corners = jnp.zeros((8, 128), F32)
    for comp in range(3):
        at = ROWS * comp
        first = turned(nodes[at : at + 8], by[0])
        second = turned(nodes[at + 8 : at + 16], by[1])
        third = turned(nodes[at + inner : at + inner + 8], by[2])
        blocks.append(jnp.where(row < 2, first, jnp.where(row < 4, second, third)))
        corners = jnp.where(row == comp, turned(nodes[at + 32 : at + 40], comp - plane), corners)
    return jnp.concatenate(blocks + [corners], axis=0)


def add_faces(nodes, below, above):
    row = row_index()
    blocks = []
    for comp in range(3):
        at = ROWS * comp
        low, high = below[8 * comp : 8 * comp + 8], above[8 * comp : 8 * comp + 8]
        blocks.append(
            nodes[at : at + 8] + jnp.where(row < 2, low, jnp.where(row >= 6, turned(high, 6), 0.0))
        )
        blocks.append(
            nodes[at + 8 : at + 16]
            + jnp.where(row < 2, turned(low, 6), jnp.where(row >= 6, turned(high, 4), 0.0))
        )
        blocks.append(nodes[at + 16 : at + 24] + jnp.where(row < 4, turned(low, 4), 0.0))
        blocks.append(nodes[at + 24 : at + 32] + jnp.where(row >= 4, high, 0.0))
        low, high = turned(below[24:32], -comp), turned(above[24:32], 3 - comp)
        blocks.append(
            nodes[at + 32 : at + 40] + jnp.where(row == 0, low, jnp.where(row == 3, high, 0.0))
        )
    return jnp.concatenate(blocks, axis=0)


def flag(flags_ref, row):
    return flags_ref[row : row + 1, 0:1]


def is_even(flags_ref, row, shape):
    place = flag(flags_ref, row)
    rest = place - 2.0 * jnp.floor(place * 0.5)
    return jnp.broadcast_to(rest, shape) < 0.5


def send_faces(nodes, flags_ref, first_ref, second_ref):
    even = is_even(flags_ref, 0, (32, 128))
    low, high = face_of(nodes, 0), face_of(nodes, 3)
    first_ref[...] = jnp.where(even, high, low)
    second_ref[...] = jnp.where(even, low, high)


def z_wall(flags_ref, off_z_ref):
    wall = jnp.minimum(off_z_ref[...] + flag(flags_ref, 1), 1.0)
    return jnp.concatenate([wall, wall, wall], axis=0)


def shared_sum(nodes, flags_ref, first_ref, second_ref, off_x_ref, off_z_ref):
    even = is_even(flags_ref, 0, (32, 128))
    first, second = first_ref[...], second_ref[...]
    total = add_faces(nodes, jnp.where(even, second, first), jnp.where(even, first, second))
    wall = jnp.minimum(off_x_ref[...] + flag(flags_ref, 0), 1.0) * jnp.minimum(
        off_z_ref[...] + flag(flags_ref, 1), 1.0
    )
    return total * jnp.concatenate([wall, wall, wall], axis=0)


def cofactors(j):
    return [
        [
            j[(r + 1) % 3][(c + 1) % 3] * j[(r + 2) % 3][(c + 2) % 3]
            - j[(r + 1) % 3][(c + 2) % 3] * j[(r + 2) % 3][(c + 1) % 3]
            for c in range(3)
        ]
        for r in range(3)
    ]


def gradients(ref, chunk, base=0):
    return [
        [
            ref[128 * m + 8 * chunk : 128 * m + 8 * chunk + 8, base + 128 * c : base + 128 * c + 128]
            for m in range(3)
        ]
        for c in range(3)
    ]


def plus_identity(g):
    return [[g[c][m] + 1.0 if c == m else g[c][m] for m in range(3)] for c in range(3)]


def plane_index(width):
    row = lax.broadcasted_iota(jnp.int32, (ROWS, width), 0)
    return jnp.where(
        row < 8,
        row // 2,
        jnp.where(
            row < 16,
            (row - 8) // 2,
            jnp.where(row < 32, (row - 16) // 4, jnp.where(row < 36, row - 32, 9)),
        ),
    )


def node_mask():
    row = lax.broadcasted_iota(jnp.int32, (ROWS, 450), 0)
    odd = row & 1
    row_code = jnp.where(
        row < 8,
        odd + 1,
        jnp.where(
            row < 16,
            3 * odd + 3,
            jnp.where(row < 32, 3 * ((row >> 1) & 1) + odd + 4, jnp.where(row < 36, 0, 99)),
        ),
    )
    flat = lax.broadcasted_iota(jnp.int32, (ROWS, 450), 1)
    y = (flat * 3641) >> 16
    z = flat - 18 * y + 1
    code = 3 * (y - 3 * ((y * 86) >> 8)) + z - 3 * ((z * 86) >> 8)
    return row_code == code


def last_kernel(disp_ref, vel_ref, out_ref):
    out_ref[0:3, :] = disp_ref[:, 900:1350]
    out_ref[3:6, :] = vel_ref[:, 900:1350]


def pack_kernel(disp_ref, vel_ref, dens_ref, energy_ref, live_ref, pick_ref, place_ref, out_ref,
                where_ref):
    dom, sub = lax.axis_index("dom"), lax.axis_index("sub")
    where_ref[...] = jnp.where(row_index() == 0, dom.astype(F32), sub.astype(F32))
    plane = plane_index(450)
    mask = node_mask() & (plane >= 1)
    blocks = []
    for ref in (disp_ref, vel_ref):
        planes = [ref[:, 450 * x : 450 * x + 450] for x in range(3)]
        for comp in range(3):
            first, second, third = (jnp.broadcast_to(p[comp : comp + 1], (ROWS, 450)) for p in planes)
            blocks.append(
                jnp.where(
                    mask, jnp.where(plane == 1, first, jnp.where(plane == 2, second, third)), 0.0
                )
            )
    out_ref[0:240, :] = exact_dot(jnp.concatenate(blocks, axis=0), pick_ref[...])
    row = lax.broadcasted_iota(jnp.int32, (8, 48), 0)
    tail = jnp.pad(energy_ref[24:27], ((0, 5), (0, 0)))
    tail = jnp.where(row == 3, live_ref[...].astype(F32), tail)
    density = jnp.pad(dens_ref[...], ((0, 0), (0, 3))).T
    out_ref[240:400, :] = exact_dot(
        jnp.concatenate([density, energy_ref[0:24], tail], axis=0), place_ref[...]
    )


def send_columns(value, start):
    lane = lax.broadcasted_iota(jnp.int32, (BLOCK, 128), 1)
    value = jnp.concatenate([value, jnp.zeros((3 * BLOCK - 400, 128), F32)], axis=0)
    parts = [rolled(value[BLOCK * i : BLOCK * i + BLOCK], 36 * i - start) for i in range(3)]
    return jnp.where(lane < 36, parts[0], jnp.where(lane < 72, parts[1], parts[2]))


def halo_kernel(packed_ref, halo_ref, pick_ref, where_ref, own_ref, first_ref, second_ref):
    mask = node_mask() & (plane_index(450) == 0)
    blocks = [
        jnp.where(mask, jnp.broadcast_to(halo_ref[comp : comp + 1, :], (ROWS, 450)), 0.0)
        for comp in range(6)
    ]
    nodes = exact_dot(jnp.concatenate(blocks, axis=0), pick_ref[...])
    own = jnp.concatenate([packed_ref[0:240] + nodes, packed_ref[240:400]], axis=0)
    own_ref[...] = own
    up, down = send_columns(own, 18), send_columns(own, 0)
    even = is_even(where_ref, 1, (BLOCK, 128))
    first_ref[...] = jnp.where(even, up, down)
    second_ref[...] = jnp.where(even, down, up)


def unpack(own, below, above):
    lane = lax.broadcasted_iota(jnp.int32, (8, 128), 1)
    rows = []
    for at in range(0, 400, 8):
        block, inner = at // BLOCK, at % BLOCK
        on_vertex = 9 if at < 240 and at % ROWS in (8, 32) else 0
        base = 36 * block
        mine = rolled(own[at : at + 8], 27 + on_vertex)
        low = rolled(below[inner : inner + 8], on_vertex - 9 - base)
        high = rolled(above[inner : inner + 8], 81 + on_vertex - base)
        rows.append(
            jnp.where(
                lane < 27 + on_vertex, low, jnp.where(lane < 81 + on_vertex, mine, high)
            )
        )
    return jnp.concatenate(rows, axis=0)


def force_kernel(own_ref, first_ref, second_ref, grad_ref, grad_t_ref, psi_ref, weight_ref,
                 flags_ref, force_ref, face1_ref, face2_ref, disp_ref, vel_ref, mass_ref, live_ref,
                 power_ref, wdens_ref, g_ref, flux_ref, point_ref):
    even = is_even(flags_ref, 1, (BLOCK, 128))
    first, second = first_ref[...], second_ref[...]
    window = unpack(own_ref[...], jnp.where(even, second, first), jnp.where(even, first, second))
    disp, vel, energy = window[0:120], window[120:240], window[368:400]
    disp_ref[...] = disp
    vel_ref[...] = vel
    lane = lax.broadcasted_iota(jnp.int32, (1, 128), 1)
    live = jnp.where(lane < 9 * WINDOW, energy[27:28], 0.0)
    live_ref[...] = jnp.broadcast_to(live, (8, 128))
    table = grad_ref[...]
    g_ref[:, 0:384] = dot(table, stacked(to_local(disp)))
    g_ref[:, 384:768] = dot(table, stacked(to_local(vel)))
    point_ref[...] = dot(psi_ref[...], stacked(energy))
    alive = jnp.broadcast_to(live, (8, 128))
    for chunk in range(16):
        at = slice(8 * chunk, 8 * chunk + 8)
        j = plus_identity(gradients(g_ref, chunk))
        g = gradients(g_ref, chunk, 384)
        cof = cofactors(j)
        volume = j[0][0] * cof[0][0] + j[0][1] * cof[0][1] + j[0][2] * cof[0][2]
        volume = jnp.where(alive > 0.5, volume, 1.0)
        inverse = 1.0 / volume
        mass_density = window[240 + 8 * chunk : 248 + 8 * chunk]
        density = mass_density * inverse
        pressure = (5.0 / 3.0 - 1.0) * density * point_ref[at, :]
        spatial = [
            [
                (g[c][0] * cof[m][0] + g[c][1] * cof[m][1] + g[c][2] * cof[m][2]) * inverse
                for m in range(3)
            ]
            for c in range(3)
        ]
        drag = VISC * density
        stress = [[None] * 3 for _ in range(3)]
        for c in range(3):
            for m in range(c, 3):
                value = drag * (spatial[c][m] + spatial[m][c])
                stress[c][m] = stress[m][c] = value - pressure if c == m else value
        weight = weight_ref[at, :]
        live_weight = weight * alive
        for c in range(3):
            for m in range(3):
                flux_ref[128 * m + 8 * chunk : 128 * m + 8 * chunk + 8, 128 * c : 128 * c + 128] = (
                    -live_weight
                ) * (stress[c][0] * cof[0][m] + stress[c][1] * cof[1][m] + stress[c][2] * cof[2][m])
        power = stress[0][0] * spatial[0][0]
        for c in range(3):
            for m in range(3):
                if c + m > 0:
                    power = power + stress[c][m] * spatial[c][m]
        power_ref[at, :] = live_weight * volume * power
        wdens = weight * mass_density
        wdens_ref[at, :] = wdens
        mass_ref[at, :] = wdens * alive
    force = from_local(transposed_dot(grad_t_ref[...], flux_ref[...]))
    force_ref[...] = force
    send_faces(force, flags_ref, face1_ref, face2_ref)


def energy_kernel(power_ref, wdens_ref, psi_t_ref, take_ref, out_ref):
    table = psi_t_ref[...]
    lumped = transposed_dot(table, wdens_ref[...])
    lumped = jnp.where(lumped > 0.0, lumped, 1.0)
    rate = transposed_dot(table, power_ref[...]) / lumped
    out_ref[...] = exact_dot(rate, take_ref[...])[0:27]


def total_of(value):
    return jnp.sum(jnp.sum(value, axis=0, keepdims=True), axis=1, keepdims=True)


def mass_points(nodes, phi_ref):
    return dot(phi_ref[...], stacked(to_local(nodes)))


def point_energy(points, mass, own_element):
    square = (
        points[:, 0:128] * points[:, 0:128]
        + points[:, 128:256] * points[:, 128:256]
        + points[:, 256:384] * points[:, 256:384]
    )
    return total_of(jnp.sum(square * mass, axis=0, keepdims=True) * own_element)


def norm_of(nodes, own):
    return total_of(nodes * nodes * jnp.concatenate([own, own, own], axis=0))


def mass_kernel(part_ref, first_ref, second_ref, flags_ref, off_x_ref, off_z_ref, mass_ref, phi_ref,
                phi_t_ref, own_ref, own_element_ref, resid_ref, image_ref, face1_ref, face2_ref,
                sums_ref):
    resid = shared_sum(part_ref[...], flags_ref, first_ref, second_ref, off_x_ref, off_z_ref)
    resid_ref[...] = resid
    points = mass_points(resid, phi_ref)
    mass = mass_ref[...]
    image = from_local(
        transposed_dot(phi_t_ref[...], points * jnp.concatenate([mass, mass, mass], axis=1))
    )
    image_ref[...] = image
    send_faces(image, flags_ref, face1_ref, face2_ref)
    norm = norm_of(resid, own_ref[...])
    energy = point_energy(points, mass, own_element_ref[0:1])
    lane = lax.broadcasted_iota(jnp.int32, (8, 128), 1)
    sums_ref[...] = jnp.where(lane == 0, norm, jnp.where(lane == 1, energy, 0.0))


def moment_kernel(part_ref, first_ref, second_ref, flags_ref, off_x_ref, off_z_ref, mass_ref, phi_ref,
                  own_ref, own_element_ref, sums_ref, image_ref, out_ref):
    image = shared_sum(part_ref[...], flags_ref, first_ref, second_ref, off_x_ref, off_z_ref)
    image_ref[...] = image
    points = mass_points(image, phi_ref)
    norm = norm_of(image, own_ref[...])
    energy = point_energy(points, mass_ref[...], own_element_ref[0:1])
    lane = lax.broadcasted_iota(jnp.int32, (1, 128), 1)
    row = sums_ref[0:1] + jnp.where(lane == 2, norm, jnp.where(lane == 3, energy, 0.0))
    out_ref[...] = jnp.broadcast_to(row, out_ref.shape)


def shape_forces(u, live, grad_ref, grad_t_ref, weight_ref, g_ref, flux_ref):
    g_ref[...] = dot(grad_ref[...], stacked(to_local(u)))
    for chunk in range(16):
        at = slice(8 * chunk, 8 * chunk + 8)
        j = plus_identity(gradients(g_ref, chunk))
        cof = cofactors(j)
        volume = j[0][0] * cof[0][0] + j[0][1] * cof[0][1] + j[0][2] * cof[0][2]
        volume = jnp.where(live > 0.5, volume, 1.0)
        norm = j[0][0] * j[0][0]
        for c in range(3):
            for m in range(3):
                if c + m > 0:
                    norm = norm + j[c][m] * j[c][m]
        weight = weight_ref[at, :] * live * jnp.exp(jnp.log(volume) * (-2.0 / 3.0))
        first = weight * (2.0 / 3.0)
        second = weight * (-2.0 / 9.0) * (norm / volume)
        for c in range(3):
            for m in range(3):
                flux_ref[128 * m + 8 * chunk : 128 * m + 8 * chunk + 8, 128 * c : 128 * c + 128] = (
                    first * j[c][m] + second * cof[c][m]
                )
    return from_local(transposed_dot(grad_t_ref[...], flux_ref[...]))


def first_shape_kernel(moments_ref, disp_ref, vel_ref, resid_ref, image_ref, live_ref, flags_ref,
                       off_z_ref, grad_ref, grad_t_ref, weight_ref, newvel_ref, moved_ref, part_ref,
                       near_ref, far_ref, skip_ref, g_ref, flux_ref):
    moments = jnp.sum(moments_ref[...], axis=0, keepdims=True)
    mu0, mu1, mu2, mu3 = (moments[:, i : i + 1] for i in range(4))
    alpha = mu0 / mu1
    rest = alpha * alpha * mu2 - mu0
    beta = rest / mu0
    gain = 1.0 + beta
    second = rest / (gain * gain * mu1 - 2.0 * gain * alpha * mu2 + alpha * alpha * mu3)
    step = flag(flags_ref, 2)
    newvel = vel_ref[...] + step * (
        (alpha + second * gain) * resid_ref[...] - (alpha * second) * image_ref[...]
    )
    newvel_ref[...] = newvel
    moved = disp_ref[...] + step * newvel
    moved_ref[...] = moved
    live = live_ref[...]
    part = shape_forces(moved, live, grad_ref, grad_t_ref, weight_ref, g_ref, flux_ref)
    part_ref[...] = part
    next_u = moved - MESH_STEP * part * z_wall(flags_ref, off_z_ref)
    low = face_of(part, 0)
    skip_ref[...] = low
    down = jnp.concatenate([next_u, low, live], axis=0)
    up = jnp.concatenate(
        [jnp.zeros((120, 128), F32), face_of(part, 3), jnp.zeros((8, 128), F32)], axis=0
    )
    even = is_even(flags_ref, 0, (160, 128))
    near_ref[...] = jnp.where(even, up, down)
    far_ref[...] = jnp.where(even, down, up)


def write_nodes(nodes, back_ref, out_ref):
    wide = exact_dot(nodes, back_ref[...])
    plane = plane_index(450)
    masks = [node_mask() & (plane == a) for a in range(1, 4)]
    for comp in range(3):
        part = wide[ROWS * comp : ROWS * comp + ROWS]
        planes = [jnp.sum(jnp.where(mask, part, 0.0), axis=0, keepdims=True) for mask in masks]
        out_ref[comp : comp + 1, :] = jnp.concatenate(planes, axis=1)


def write_kernel(nodes_ref, back_ref, out_ref):
    write_nodes(nodes_ref[...], back_ref, out_ref)


def second_shape_kernel(part_ref, near_ref, far_ref, skip_ref, flags_ref, off_x_ref, off_z_ref,
                        newvel_ref, moved_ref, live_ref, grad_ref, grad_t_ref, weight_ref, back_ref,
                        out_ref, g_ref, flux_ref, next_g_ref, next_flux_ref):
    even = is_even(flags_ref, 0, (160, 128))
    near, far = near_ref[...], far_ref[...]
    upper, lower = jnp.where(even, near, far), jnp.where(even, far, near)
    wall = z_wall(flags_ref, off_z_ref)
    off_x = off_x_ref[...]
    x_wall = jnp.minimum(off_x + flag(flags_ref, 0), 1.0)
    total = add_faces(part_ref[...], lower[120:152], upper[120:152])
    gradient = total * wall * jnp.concatenate([x_wall, x_wall, x_wall], axis=0)
    u = moved_ref[...] - MESH_STEP * gradient
    zero = jnp.zeros((120, 128), F32)
    next_u = upper[0:120] * jnp.concatenate([off_x, off_x, off_x], axis=0)
    next_u = next_u + wall * add_faces(zero, face_of(u, 3), -MESH_STEP * skip_ref[...])
    part = shape_forces(u, live_ref[...], grad_ref, grad_t_ref, weight_ref, g_ref, flux_ref)
    next_part = shape_forces(
        next_u, upper[152:160], grad_ref, grad_t_ref, weight_ref, next_g_ref, next_flux_ref
    )
    second = add_faces(part, jnp.zeros((32, 128), F32), face_of(next_part, 0))
    nodes = newvel_ref[...] - (MESH_STEP / flag(flags_ref, 2)) * (gradient + second)
    write_nodes(nodes, back_ref, out_ref)


def copying(kernel, count):
    def run(*refs):
        sources, outs = refs[:count], refs[count : -count - 1]
        copies, sems = refs[-count - 1 : -1], refs[-1]
        moves = [
            pltpu.make_async_copy(source, target, sems.at[i])
            for i, (source, target) in enumerate(zip(sources, copies))
        ]
        for move in moves:
            move.start()
        for move in moves:
            move.wait()
        kernel(*copies, *outs)

    return run


def call(kernel, outs, scratch=(), flops=1_000_000, copied=False):
    spec = pl.BlockSpec(memory_space=pltpu.VMEM)

    def run(*args):
        given, body_of = spec, kernel
        extra = [pltpu.VMEM(shape, F32) for shape in scratch]
        if copied:
            given, body_of = pl.BlockSpec(memory_space=pltpu.HBM), copying(kernel, len(args))
            extra = [pltpu.VMEM(arg.shape, arg.dtype) for arg in args]
            extra.append(pltpu.SemaphoreType.DMA((len(args),)))
            args = [pltpu.with_memory_space_constraint(arg, pltpu.HBM) for arg in args]
        return pl.pallas_call(
            body_of,
            out_shape=[jax.ShapeDtypeStruct(shape, F32) for shape in outs],
            in_specs=[given] * len(args),
            out_specs=[spec] * len(outs),
            scratch_shapes=extra,
            compiler_params=pltpu.CompilerParams(vmem_limit_bytes=16 * 1024 * 1024),
            cost_estimate=pl.CostEstimate(flops=flops, bytes_accessed=400_000, transcendentals=0),
        )(*args)

    return run


NODES = (120, 128)
POINTS = (128, 128)
FACE = (32, 128)


def body(displacement, velocity, energy, mass_density, live_mask, time_step):
    table = {name: jnp.asarray(value) for name, value in constants().items()}
    n_dom, n_sub = lax.axis_size("dom"), lax.axis_size("sub")
    up = [(i, i + 1) for i in range(n_dom - 1)]

    def pairs(start, size):
        return [p for i in range(start, size - 1, 2) for p in ((i, i + 1), (i + 1, i))]

    walls = (table["off_x"], table["off_z"])

    (last,) = call(last_kernel, [(6, 450)], copied=True)(displacement, velocity)
    halo = lax.ppermute(last, "dom", up)
    packed, where = call(pack_kernel, [(400, 128), (8, 128)], copied=True)(
        displacement, velocity, mass_density.T, energy, live_mask.reshape(1, 48), table["pick"],
        table["place"],
    )
    row = lax.broadcasted_iota(jnp.int32, (8, 128), 0)
    own, z_first, z_second = call(
        halo_kernel, [(400, 128), (BLOCK, 128), (BLOCK, 128)]
    )(packed, halo, table["pick"], where)
    flags = jnp.where(row < 2, where, time_step)
    first = lax.ppermute(z_first, "sub", pairs(0, n_sub))
    second = lax.ppermute(z_second, "sub", pairs(1, n_sub))
    force, face1, face2, disp, vel, mass, live, power, wdens = call(
        force_kernel,
        [NODES, FACE, FACE, NODES, NODES, POINTS, (8, 128), POINTS, POINTS],
        [(384, 768), (384, 384), POINTS],
    )(own, first, second, table["grad"], table["grad_t"], table["psi"], table["weight"], flags)

    def swap(face1, face2):
        second = lax.ppermute(face2, "dom", pairs(1, n_dom))
        return lax.ppermute(face1, "dom", pairs(0, n_dom)), second

    first, second = swap(face1, face2)
    (energy_rate,) = call(energy_kernel, [(27, 48)])(power, wdens, table["psi_t"], table["take"])
    force, energy_rate = lax.optimization_barrier((force, energy_rate))
    resid, image_part, face1, face2, sums = call(
        mass_kernel, [NODES, NODES, FACE, FACE, (8, 128)]
    )(force, first, second, flags, *walls, mass, table["phi"], table["phi_t"], table["own"],
      table["own_element"])
    first, second = swap(face1, face2)
    image, local = call(moment_kernel, [NODES, (n_dom, 128)])(
        image_part, first, second, flags, *walls, mass, table["phi"], table["own"],
        table["own_element"], sums,
    )
    slab = jnp.sum(lax.all_to_all(local, "dom", 0, 0, tiled=True), axis=0, keepdims=True)
    moments = lax.all_to_all(jnp.broadcast_to(slab, (n_sub, 128)), "sub", 0, 0, tiled=True)
    newvel, moved, part, near, far, skip = call(
        first_shape_kernel, [NODES, NODES, NODES, (160, 128), (160, 128), FACE],
        [(384, 384), (384, 384)],
    )(moments, disp, vel, resid, image, live, flags, table["off_z"], table["grad"], table["grad_t"],
      table["weight"])
    near = lax.ppermute(near, "dom", pairs(0, n_dom))
    far = lax.ppermute(far, "dom", pairs(1, n_dom))
    skip = lax.ppermute(skip, "dom", [(i + 2, i) for i in range(n_dom - 2)])
    (new_velocity,) = call(write_kernel, [(3, 1350)])(newvel, table["back"])
    part, new_velocity = lax.optimization_barrier((part, new_velocity))
    (mesh_velocity,) = call(
        second_shape_kernel, [(3, 1350)], [(384, 384)] * 4
    )(part, near, far, skip, flags, *walls, newvel, moved, live, table["grad"], table["grad_t"],
      table["weight"], table["back"])
    return new_velocity, energy_rate, mesh_velocity


def solution(mesh):
    both = ("dom", "sub")

    return jax.shard_map(
        body,
        mesh=mesh,
        in_specs=(P(None, both), P(None, both), P(None, both), P(None, both), P(both), P()),
        out_specs=(P(None, both), P(None, both), P(None, both)),
        check_vma=False,
    )
```

```python
import functools
import math

import jax
import jax.numpy as jnp
import numpy as np
from jax import lax
from jax.experimental import pallas as pl
from jax.experimental.pallas import tpu as pltpu
from jax.sharding import PartitionSpec as P


EY = 8
EZ = 6
VISC = 0.3
MESH_STEP = 0.01
BF = jnp.bfloat16
F32 = jnp.float32
ROWS = 40
BELOW = 3
WINDOW = 13
LANE_OWN = 9 * BELOW
BLOCK = 136


def node_row(a, b, c):
    if b == 0 and c > 0:
        return 2 * a + c - 1
    if b > 0 and c == 0:
        return 8 + 2 * a + b - 1
    if b > 0:
        return 16 + 4 * a + 2 * (b - 1) + c - 1
    return 32 + a


def local_row(a, b, c):
    if b < 3 and c < 3:
        return node_row(a, b, c)
    if b == 3 and c < 3:
        return 48 + a if c == 0 else 40 + node_row(a, 0, c)
    if b < 3:
        return 64 + a if b == 0 else 56 + node_row(a, b, 0) - 8
    return 72 + a


def outer_triple(first, second, third):
    product = (
        first[:, None, None, :, None, None]
        * second[None, :, None, None, :, None]
        * third[None, None, :, None, None, :]
    )
    return product.reshape(
        first.shape[0] * second.shape[0] * third.shape[0],
        first.shape[1] * second.shape[1] * third.shape[1],
    )


def basis_tables():
    root_term = math.sqrt(10.0 / 7.0)
    outer = math.sqrt(5.0 + 2.0 * root_term) / 3.0
    inner = math.sqrt(5.0 - 2.0 * root_term) / 3.0
    gauss_roots = np.array([-outer, -inner, 0.0, inner, outer])
    outer_weight = (322.0 - 13.0 * math.sqrt(70.0)) / 900.0
    middle_weight = (322.0 + 13.0 * math.sqrt(70.0)) / 900.0
    weights = (
        np.array([outer_weight, middle_weight, 128.0 / 225.0, middle_weight, outer_weight]) / 2.0
    )
    points = (1.0 + gauss_roots) / 2.0
    lobatto = [0.0, (1.0 - 1.0 / math.sqrt(5.0)) / 2.0, (1.0 + 1.0 / math.sqrt(5.0)) / 2.0, 1.0]
    values = np.ones((5, 4))
    slopes = np.zeros((5, 4))
    for node in range(4):
        for other in range(4):
            if other != node:
                values[:, node] *= (points - lobatto[other]) / (lobatto[node] - lobatto[other])
        for other in range(4):
            if other != node:
                term = np.ones(5) / (lobatto[node] - lobatto[other])
                for third in range(4):
                    if third != node and third != other:
                        term = term * (points - lobatto[third]) / (lobatto[node] - lobatto[third])
                slopes[:, node] += term
    bernstein = np.stack([(1.0 - points) ** 2, 2.0 * points * (1.0 - points), points**2], axis=1)
    quad_weight = (
        weights[:, None, None] * weights[None, :, None] * weights[None, None, :]
    ).reshape(125)
    return (
        outer_triple(values, values, values),
        [
            outer_triple(slopes, values, values),
            outer_triple(values, slopes, values),
            outer_triple(values, values, slopes),
        ],
        outer_triple(bernstein, bernstein, bernstein),
        quad_weight,
    )


def split_table(table):
    high = table.astype(np.float32).astype(jnp.bfloat16)
    low = (table - high.astype(np.float64)).astype(np.float32).astype(jnp.bfloat16)
    return high, low


@functools.cache
def constants():
    vel_basis, grads, energy_basis, quad_weight = basis_tables()
    order = np.zeros(64, np.int64)
    for a in range(4):
        for b in range(4):
            for c in range(4):
                order[16 * a + 4 * b + c] = local_row(a, b, c)

    def spread_columns(table):
        wide = np.zeros((128, 80))
        wide[:125, order] = table
        return wide

    out = {}
    grad = np.concatenate([spread_columns(g) for g in grads], axis=0)
    high, low = split_table(grad)
    out["grad"] = np.concatenate([high, high, low], axis=1)
    high, low = split_table(grad.T)
    out["grad_t"] = np.concatenate([high, low], axis=0)
    phi = spread_columns(vel_basis)
    high, low = split_table(phi)
    out["phi"] = np.concatenate([high, high, low], axis=1)
    high, low = split_table(phi.T)
    out["phi_t"] = np.concatenate([high, low], axis=0)
    psi = np.zeros((128, 32))
    psi[:125, :27] = energy_basis
    high, low = split_table(psi)
    out["psi"] = np.concatenate([high, high, low], axis=1)
    high, low = split_table(psi.T)
    out["psi_t"] = np.concatenate([high, low], axis=0)
    weight = np.zeros((128, 128), np.float32)
    weight[:125] = quad_weight[:, None]
    out["weight"] = weight

    flat = np.arange(450)
    py, pz = flat // 18, flat % 18
    lane = 9 * ((pz + 1) // 3) + py // 3
    frame = lane - 9 * (pz % 3 == 2)
    own = np.zeros((ROWS, 128), np.float32)
    for a in range(4):
        for k in range(450):
            b, c = py[k] % 3, (pz[k] + 1) % 3
            row = node_row(a, b, c)
            if a > 0:
                own[row, lane[k] + LANE_OWN] = 1.0
    out["own"] = own
    pick = np.zeros((450, 128), np.float32)
    pick[flat, frame] = 1.0
    out["pick"] = pick.astype(jnp.bfloat16)
    back = np.zeros((128, 450), np.float32)
    back[lane + LANE_OWN, flat] = 1.0
    out["back"] = back.astype(jnp.bfloat16)
    off_x = np.ones((ROWS, 128), np.float32)
    off_z = np.ones((ROWS, 128), np.float32)
    for b in range(3):
        for c in range(3):
            for a in range(4):
                if a == 0:
                    off_x[node_row(a, b, c)] = 0.0
                off_z[node_row(a, b, c), 3 * (np.arange(128) // 9 - BELOW) + c <= 0] = 0.0
    out["off_x"] = off_x
    out["off_z"] = off_z
    element = np.arange(EY * EZ)
    elane = 9 * (element % EZ) + element // EZ
    place = np.zeros((48, 128), np.float32)
    place[element, elane] = 1.0
    out["place"] = place.astype(jnp.bfloat16)
    take = np.zeros((128, 48), np.float32)
    take[elane + LANE_OWN, element] = 1.0
    out["take"] = take.astype(jnp.bfloat16)
    own_element = np.zeros((8, 128), np.float32)
    own_element[:, elane + LANE_OWN] = 1.0
    out["own_element"] = own_element
    return out


def dot(left, right):
    return jnp.dot(left, right, preferred_element_type=F32)


def split2(value):
    high = value.astype(BF)
    return high, (value - high.astype(F32)).astype(BF)


def split3(value):
    high = value.astype(BF)
    rest = value - high.astype(F32)
    middle = rest.astype(BF)
    return high, middle, (rest - middle.astype(F32)).astype(BF)


def exact_dot(value, selection):
    high, middle, low = (part.astype(F32) for part in split3(value))
    rows = value.shape[0]
    wide = dot(jnp.concatenate([high, middle, low], axis=0).astype(BF), selection)
    return wide[:rows] + (wide[rows : 2 * rows] + wide[2 * rows :])


def stacked(value):
    high, low = split2(value)
    return jnp.concatenate([high, low, high], axis=0)


def rolled(value, by):
    return pltpu.roll(value, by % 128, 1)


def to_local(nodes):
    columns = []
    for comp in range(3):
        block = nodes[ROWS * comp : ROWS * comp + ROWS]
        corner = block[32:40]
        columns.append(
            jnp.concatenate(
                [
                    block,
                    rolled(block[0:8], -1),
                    rolled(corner, -1),
                    rolled(block[8:16], -9),
                    rolled(corner, -9),
                    rolled(corner, -10),
                ],
                axis=0,
            )
        )
    return jnp.concatenate(columns, axis=1)


def from_local(local):
    blocks = []
    for comp in range(3):
        part = local[:, 128 * comp : 128 * comp + 128]
        blocks += [
            part[0:8] + rolled(part[40:48], 1),
            part[8:16] + rolled(part[56:64], 9),
            part[16:32],
            part[32:40]
            + (rolled(part[48:56], 1) + rolled(part[64:72], 9) + rolled(part[72:80], 10)),
        ]
    return jnp.concatenate(blocks, axis=0)


def transposed_dot(table, value):
    high, low = split2(value)
    half = table.shape[0] // 2
    both = dot(table, high)
    return both[:half] + (both[half:] + dot(table[:half], low))


def turned(value, by):
    return value if by % 8 == 0 else pltpu.roll(value, by % 8, 0)


def row_index():
    return lax.broadcasted_iota(jnp.int32, (8, 128), 0)


def face_of(nodes, plane):
    row = row_index()
    by = (0, 2, 4) if plane == 0 else (2, 4, 0)
    inner = 16 if plane == 0 else 24
    blocks = []
    corners = jnp.zeros((8, 128), F32)
    for comp in range(3):
        at = ROWS * comp
        first = turned(nodes[at : at + 8], by[0])
        second = turned(nodes[at + 8 : at + 16], by[1])
        third = turned(nodes[at + inner : at + inner + 8], by[2])
        blocks.append(jnp.where(row < 2, first, jnp.where(row < 4, second, third)))
        corners = jnp.where(row == comp, turned(nodes[at + 32 : at + 40], comp - plane), corners)
    return jnp.concatenate(blocks + [corners], axis=0)


def add_faces(nodes, below, above):
    row = row_index()
    blocks = []
    for comp in range(3):
        at = ROWS * comp
        low, high = below[8 * comp : 8 * comp + 8], above[8 * comp : 8 * comp + 8]
        blocks.append(
            nodes[at : at + 8] + jnp.where(row < 2, low, jnp.where(row >= 6, turned(high, 6), 0.0))
        )
        blocks.append(
            nodes[at + 8 : at + 16]
            + jnp.where(row < 2, turned(low, 6), jnp.where(row >= 6, turned(high, 4), 0.0))
        )
        blocks.append(nodes[at + 16 : at + 24] + jnp.where(row < 4, turned(low, 4), 0.0))
        blocks.append(nodes[at + 24 : at + 32] + jnp.where(row >= 4, high, 0.0))
        low, high = turned(below[24:32], -comp), turned(above[24:32], 3 - comp)
        blocks.append(
            nodes[at + 32 : at + 40] + jnp.where(row == 0, low, jnp.where(row == 3, high, 0.0))
        )
    return jnp.concatenate(blocks, axis=0)


def flag(flags_ref, row):
    return flags_ref[row : row + 1, 0:1]


def is_even(flags_ref, row, shape):
    place = flag(flags_ref, row)
    rest = place - 2.0 * jnp.floor(place * 0.5)
    return jnp.broadcast_to(rest, shape) < 0.5


def z_wall(flags_ref, off_z_ref):
    wall = jnp.minimum(off_z_ref[...] + flag(flags_ref, 1), 1.0)
    return jnp.concatenate([wall, wall, wall], axis=0)


def cofactors(j):
    return [
        [
            j[(r + 1) % 3][(c + 1) % 3] * j[(r + 2) % 3][(c + 2) % 3]
            - j[(r + 1) % 3][(c + 2) % 3] * j[(r + 2) % 3][(c + 1) % 3]
            for c in range(3)
        ]
        for r in range(3)
    ]


def gradients(ref, chunk, base=0):
    return [
        [
            ref[128 * m + 8 * chunk : 128 * m + 8 * chunk + 8, base + 128 * c : base + 128 * c + 128]
            for m in range(3)
        ]
        for c in range(3)
    ]


def plus_identity(g):
    return [[g[c][m] + 1.0 if c == m else g[c][m] for m in range(3)] for c in range(3)]


def plane_index(width):
    row = lax.broadcasted_iota(jnp.int32, (ROWS, width), 0)
    return jnp.where(
        row < 8,
        row // 2,
        jnp.where(
            row < 16,
            (row - 8) // 2,
            jnp.where(row < 32, (row - 16) // 4, jnp.where(row < 36, row - 32, 9)),
        ),
    )


def node_mask():
    row = lax.broadcasted_iota(jnp.int32, (ROWS, 450), 0)
    odd = row & 1
    row_code = jnp.where(
        row < 8,
        odd + 1,
        jnp.where(
            row < 16,
            3 * odd + 3,
            jnp.where(row < 32, 3 * ((row >> 1) & 1) + odd + 4, jnp.where(row < 36, 0, 99)),
        ),
    )
    flat = lax.broadcasted_iota(jnp.int32, (ROWS, 450), 1)
    y = (flat * 3641) >> 16
    z = flat - 18 * y + 1
    code = 3 * (y - 3 * ((y * 86) >> 8)) + z - 3 * ((z * 86) >> 8)
    return row_code == code


def last_kernel(disp_ref, vel_ref, out_ref):
    out_ref[0:3, :] = disp_ref[:, 900:1350]
    out_ref[3:6, :] = vel_ref[:, 900:1350]


def pack_kernel(disp_ref, vel_ref, dens_ref, energy_ref, live_ref, pick_ref, place_ref, out_ref,
                where_ref):
    dom, sub = lax.axis_index("dom"), lax.axis_index("sub")
    where_ref[...] = jnp.where(row_index() == 0, dom.astype(F32), sub.astype(F32))
    plane = plane_index(450)
    mask = node_mask() & (plane >= 1)
    blocks = []
    for ref in (disp_ref, vel_ref):
        planes = [ref[:, 450 * x : 450 * x + 450] for x in range(3)]
        for comp in range(3):
            first, second, third = (jnp.broadcast_to(p[comp : comp + 1], (ROWS, 450)) for p in planes)
            blocks.append(
                jnp.where(
                    mask, jnp.where(plane == 1, first, jnp.where(plane == 2, second, third)), 0.0
                )
            )
    out_ref[0:240, :] = exact_dot(jnp.concatenate(blocks, axis=0), pick_ref[...])
    row = lax.broadcasted_iota(jnp.int32, (8, 48), 0)
    tail = jnp.pad(energy_ref[24:27], ((0, 5), (0, 0)))
    tail = jnp.where(row == 3, live_ref[...].astype(F32), tail)
    density = jnp.pad(dens_ref[...], ((0, 0), (0, 3))).T
    out_ref[240:400, :] = exact_dot(
        jnp.concatenate([density, energy_ref[0:24], tail], axis=0), place_ref[...]
    )


def send_columns(value, start):
    lane = lax.broadcasted_iota(jnp.int32, (BLOCK, 128), 1)
    value = jnp.concatenate([value, jnp.zeros((3 * BLOCK - 400, 128), F32)], axis=0)
    parts = [rolled(value[BLOCK * i : BLOCK * i + BLOCK], 36 * i - start) for i in range(3)]
    return jnp.where(lane < 36, parts[0], jnp.where(lane < 72, parts[1], parts[2]))


def halo_kernel(packed_ref, halo_ref, pick_ref, where_ref, own_ref, first_ref, second_ref):
    mask = node_mask() & (plane_index(450) == 0)
    blocks = [
        jnp.where(mask, jnp.broadcast_to(halo_ref[comp : comp + 1, :], (ROWS, 450)), 0.0)
        for comp in range(6)
    ]
    nodes = exact_dot(jnp.concatenate(blocks, axis=0), pick_ref[...])
    own = jnp.concatenate([packed_ref[0:240] + nodes, packed_ref[240:400]], axis=0)
    own_ref[...] = own
    up, down = send_columns(own, 18), send_columns(own, 0)
    even = is_even(where_ref, 1, (BLOCK, 128))
    first_ref[...] = jnp.where(even, up, down)
    second_ref[...] = jnp.where(even, down, up)


def unpack(own, below, above):
    lane = lax.broadcasted_iota(jnp.int32, (8, 128), 1)
    rows = []
    for at in range(0, 400, 8):
        block, inner = at // BLOCK, at % BLOCK
        on_vertex = 9 if at < 240 and at % ROWS in (8, 32) else 0
        base = 36 * block
        mine = rolled(own[at : at + 8], 27 + on_vertex)
        low = rolled(below[inner : inner + 8], on_vertex - 9 - base)
        high = rolled(above[inner : inner + 8], 81 + on_vertex - base)
        rows.append(
            jnp.where(
                lane < 27 + on_vertex, low, jnp.where(lane < 81 + on_vertex, mine, high)
            )
        )
    return jnp.concatenate(rows, axis=0)


def force_kernel(own_ref, first_ref, second_ref, grad_ref, grad_t_ref, psi_ref, weight_ref,
                 flags_ref, message_ref, low_ref, high_ref, disp_ref, vel_ref, live_ref,
                 power_ref, wdens_ref, g_ref, flux_ref, point_ref):
    even = is_even(flags_ref, 1, (BLOCK, 128))
    first, second = first_ref[...], second_ref[...]
    window = unpack(own_ref[...], jnp.where(even, second, first), jnp.where(even, first, second))
    disp, vel, energy = window[0:120], window[120:240], window[368:400]
    disp_ref[...] = disp
    vel_ref[...] = vel
    lane = lax.broadcasted_iota(jnp.int32, (1, 128), 1)
    live = jnp.where(lane < 9 * WINDOW, energy[27:28], 0.0)
    live_ref[...] = jnp.broadcast_to(live, (8, 128))
    table = grad_ref[...]
    g_ref[:, 0:384] = dot(table, stacked(to_local(disp)))
    g_ref[:, 384:768] = dot(table, stacked(to_local(vel)))
    point_ref[...] = dot(psi_ref[...], stacked(energy))
    alive = jnp.broadcast_to(live, (8, 128))
    for chunk in range(16):
        at = slice(8 * chunk, 8 * chunk + 8)
        j = plus_identity(gradients(g_ref, chunk))
        g = gradients(g_ref, chunk, 384)
        cof = cofactors(j)
        volume = j[0][0] * cof[0][0] + j[0][1] * cof[0][1] + j[0][2] * cof[0][2]
        volume = jnp.where(alive > 0.5, volume, 1.0)
        inverse = 1.0 / volume
        mass_density = window[240 + 8 * chunk : 248 + 8 * chunk]
        density = mass_density * inverse
        pressure = (5.0 / 3.0 - 1.0) * density * point_ref[at, :]
        spatial = [
            [
                (g[c][0] * cof[m][0] + g[c][1] * cof[m][1] + g[c][2] * cof[m][2]) * inverse
                for m in range(3)
            ]
            for c in range(3)
        ]
        drag = VISC * density
        stress = [[None] * 3 for _ in range(3)]
        for c in range(3):
            for m in range(c, 3):
                value = drag * (spatial[c][m] + spatial[m][c])
                stress[c][m] = stress[m][c] = value - pressure if c == m else value
        weight = weight_ref[at, :]
        live_weight = weight * alive
        for c in range(3):
            for m in range(3):
                flux_ref[128 * m + 8 * chunk : 128 * m + 8 * chunk + 8, 128 * c : 128 * c + 128] = (
                    -live_weight
                ) * (stress[c][0] * cof[0][m] + stress[c][1] * cof[1][m] + stress[c][2] * cof[2][m])
        power = stress[0][0] * spatial[0][0]
        for c in range(3):
            for m in range(3):
                if c + m > 0:
                    power = power + stress[c][m] * spatial[c][m]
        power_ref[at, :] = live_weight * volume * power
        wdens = weight * mass_density
        wdens_ref[at, :] = wdens
        message_ref[120 + 8 * chunk : 128 + 8 * chunk, :] = wdens * alive
    force = from_local(transposed_dot(grad_t_ref[...], flux_ref[...]))
    message_ref[0:120, :] = force
    low_ref[...] = face_of(force, 0)
    high_ref[...] = face_of(force, 3)


def energy_kernel(power_ref, wdens_ref, psi_t_ref, take_ref, out_ref):
    table = psi_t_ref[...]
    lumped = transposed_dot(table, wdens_ref[...])
    lumped = jnp.where(lumped > 0.0, lumped, 1.0)
    rate = transposed_dot(table, power_ref[...]) / lumped
    out_ref[...] = exact_dot(rate, take_ref[...])[0:27]


def total_of(value):
    return jnp.sum(jnp.sum(value, axis=0, keepdims=True), axis=1, keepdims=True)


def mass_points(nodes, phi_ref):
    return dot(phi_ref[...], stacked(to_local(nodes)))


def point_energy(points, mass, own_element):
    square = (
        points[:, 0:128] * points[:, 0:128]
        + points[:, 128:256] * points[:, 128:256]
        + points[:, 256:384] * points[:, 256:384]
    )
    return total_of(jnp.sum(square * mass, axis=0, keepdims=True) * own_element)


def norm_of(nodes, own):
    return total_of(nodes * nodes * jnp.concatenate([own, own, own], axis=0))


def mass_image(points, mass, phi_t_ref):
    return from_local(
        transposed_dot(phi_t_ref[...], points * jnp.concatenate([mass, mass, mass], axis=1))
    )


def krylov_kernel(message_ref, near_ref, far_ref, skip_up_ref, skip_down_ref, flags_ref, off_x_ref,
                  off_z_ref, phi_ref, phi_t_ref, own_ref, own_element_ref, resid_ref, image_ref,
                  out_ref):
    even = is_even(flags_ref, 0, (248, 128))
    near, far = near_ref[...], far_ref[...]
    upper, lower = jnp.where(even, near, far), jnp.where(even, far, near)
    force, mass = message_ref[0:120], message_ref[120:248]
    wall = z_wall(flags_ref, off_z_ref)
    dom = flag(flags_ref, 0)

    def walls(place):
        x_wall = jnp.minimum(off_x_ref[...] + jnp.maximum(place, 0.0), 1.0)
        return wall * jnp.concatenate([x_wall, x_wall, x_wall], axis=0)

    own_walls = walls(dom)
    resid = add_faces(force, face_of(lower, 3), face_of(upper, 0)) * own_walls
    resid_low = add_faces(lower[0:120], skip_up_ref[...], face_of(force, 0)) * walls(dom - 1.0)
    resid_up = add_faces(upper[0:120], face_of(force, 3), skip_down_ref[...]) * wall
    resid_ref[...] = resid
    points = mass_points(resid, phi_ref)
    part = mass_image(points, mass, phi_t_ref)
    part_low = mass_image(mass_points(resid_low, phi_ref), lower[120:248], phi_t_ref)
    part_up = mass_image(mass_points(resid_up, phi_ref), upper[120:248], phi_t_ref)
    image = add_faces(part, face_of(part_low, 3), face_of(part_up, 0)) * own_walls
    image_ref[...] = image
    own, own_element = own_ref[...], own_element_ref[0:1]
    moments = (
        norm_of(resid, own),
        point_energy(points, mass, own_element),
        norm_of(image, own),
        point_energy(mass_points(image, phi_ref), mass, own_element),
    )
    lane = lax.broadcasted_iota(jnp.int32, (1, 128), 1)
    row = jnp.zeros((1, 128), F32)
    for i, moment in enumerate(moments):
        row = jnp.where(lane == i, moment, row)
    out_ref[...] = jnp.broadcast_to(row, out_ref.shape)


def shape_forces(u, live, grad_ref, grad_t_ref, weight_ref, g_ref, flux_ref):
    g_ref[...] = dot(grad_ref[...], stacked(to_local(u)))
    for chunk in range(16):
        at = slice(8 * chunk, 8 * chunk + 8)
        j = plus_identity(gradients(g_ref, chunk))
        cof = cofactors(j)
        volume = j[0][0] * cof[0][0] + j[0][1] * cof[0][1] + j[0][2] * cof[0][2]
        volume = jnp.where(live > 0.5, volume, 1.0)
        norm = j[0][0] * j[0][0]
        for c in range(3):
            for m in range(3):
                if c + m > 0:
                    norm = norm + j[c][m] * j[c][m]
        weight = weight_ref[at, :] * live * jnp.exp(jnp.log(volume) * (-2.0 / 3.0))
        first = weight * (2.0 / 3.0)
        second = weight * (-2.0 / 9.0) * (norm / volume)
        for c in range(3):
            for m in range(3):
                flux_ref[128 * m + 8 * chunk : 128 * m + 8 * chunk + 8, 128 * c : 128 * c + 128] = (
                    first * j[c][m] + second * cof[c][m]
                )
    return from_local(transposed_dot(grad_t_ref[...], flux_ref[...]))


def first_shape_kernel(moments_ref, disp_ref, vel_ref, resid_ref, image_ref, live_ref, flags_ref,
                       off_z_ref, grad_ref, grad_t_ref, weight_ref, newvel_ref, moved_ref, part_ref,
                       near_ref, far_ref, skip_ref, g_ref, flux_ref):
    moments = jnp.sum(moments_ref[...], axis=0, keepdims=True)
    mu0, mu1, mu2, mu3 = (moments[:, i : i + 1] for i in range(4))
    alpha = mu0 / mu1
    rest = alpha * alpha * mu2 - mu0
    beta = rest / mu0
    gain = 1.0 + beta
    second = rest / (gain * gain * mu1 - 2.0 * gain * alpha * mu2 + alpha * alpha * mu3)
    step = flag(flags_ref, 2)
    newvel = vel_ref[...] + step * (
        (alpha + second * gain) * resid_ref[...] - (alpha * second) * image_ref[...]
    )
    newvel_ref[...] = newvel
    moved = disp_ref[...] + step * newvel
    moved_ref[...] = moved
    live = live_ref[...]
    part = shape_forces(moved, live, grad_ref, grad_t_ref, weight_ref, g_ref, flux_ref)
    part_ref[...] = part
    next_u = moved - MESH_STEP * part * z_wall(flags_ref, off_z_ref)
    low = face_of(part, 0)
    skip_ref[...] = low
    down = jnp.concatenate([next_u, low, live], axis=0)
    up = jnp.concatenate(
        [jnp.zeros((120, 128), F32), face_of(part, 3), jnp.zeros((8, 128), F32)], axis=0
    )
    even = is_even(flags_ref, 0, (160, 128))
    near_ref[...] = jnp.where(even, up, down)
    far_ref[...] = jnp.where(even, down, up)


def write_nodes(nodes, back_ref, out_ref):
    wide = exact_dot(nodes, back_ref[...])
    plane = plane_index(450)
    masks = [node_mask() & (plane == a) for a in range(1, 4)]
    for comp in range(3):
        part = wide[ROWS * comp : ROWS * comp + ROWS]
        planes = [jnp.sum(jnp.where(mask, part, 0.0), axis=0, keepdims=True) for mask in masks]
        out_ref[comp : comp + 1, :] = jnp.concatenate(planes, axis=1)


def write_kernel(nodes_ref, back_ref, out_ref):
    write_nodes(nodes_ref[...], back_ref, out_ref)


def second_shape_kernel(part_ref, near_ref, far_ref, skip_ref, flags_ref, off_x_ref, off_z_ref,
                        newvel_ref, moved_ref, live_ref, grad_ref, grad_t_ref, weight_ref, back_ref,
                        out_ref, g_ref, flux_ref, next_g_ref, next_flux_ref):
    even = is_even(flags_ref, 0, (160, 128))
    near, far = near_ref[...], far_ref[...]
    upper, lower = jnp.where(even, near, far), jnp.where(even, far, near)
    wall = z_wall(flags_ref, off_z_ref)
    off_x = off_x_ref[...]
    x_wall = jnp.minimum(off_x + flag(flags_ref, 0), 1.0)
    total = add_faces(part_ref[...], lower[120:152], upper[120:152])
    gradient = total * wall * jnp.concatenate([x_wall, x_wall, x_wall], axis=0)
    u = moved_ref[...] - MESH_STEP * gradient
    zero = jnp.zeros((120, 128), F32)
    next_u = upper[0:120] * jnp.concatenate([off_x, off_x, off_x], axis=0)
    next_u = next_u + wall * add_faces(zero, face_of(u, 3), -MESH_STEP * skip_ref[...])
    part = shape_forces(u, live_ref[...], grad_ref, grad_t_ref, weight_ref, g_ref, flux_ref)
    next_part = shape_forces(
        next_u, upper[152:160], grad_ref, grad_t_ref, weight_ref, next_g_ref, next_flux_ref
    )
    second = add_faces(part, jnp.zeros((32, 128), F32), face_of(next_part, 0))
    nodes = newvel_ref[...] - (MESH_STEP / flag(flags_ref, 2)) * (gradient + second)
    write_nodes(nodes, back_ref, out_ref)


def copying(kernel, count):
    def run(*refs):
        sources, outs = refs[:count], refs[count : -count - 1]
        copies, sems = refs[-count - 1 : -1], refs[-1]
        moves = [
            pltpu.make_async_copy(source, target, sems.at[i])
            for i, (source, target) in enumerate(zip(sources, copies))
        ]
        for move in moves:
            move.start()
        for move in moves:
            move.wait()
        kernel(*copies, *outs)

    return run


def call(kernel, outs, scratch=(), flops=1_000_000, copied=False):
    spec = pl.BlockSpec(memory_space=pltpu.VMEM)

    def run(*args):
        given, body_of = spec, kernel
        extra = [pltpu.VMEM(shape, F32) for shape in scratch]
        if copied:
            given, body_of = pl.BlockSpec(memory_space=pltpu.HBM), copying(kernel, len(args))
            extra = [pltpu.VMEM(arg.shape, arg.dtype) for arg in args]
            extra.append(pltpu.SemaphoreType.DMA((len(args),)))
            args = [pltpu.with_memory_space_constraint(arg, pltpu.HBM) for arg in args]
        return pl.pallas_call(
            body_of,
            out_shape=[jax.ShapeDtypeStruct(shape, F32) for shape in outs],
            in_specs=[given] * len(args),
            out_specs=[spec] * len(outs),
            scratch_shapes=extra,
            compiler_params=pltpu.CompilerParams(vmem_limit_bytes=16 * 1024 * 1024),
            cost_estimate=pl.CostEstimate(flops=flops, bytes_accessed=400_000, transcendentals=0),
        )(*args)

    return run


NODES = (120, 128)
POINTS = (128, 128)
FACE = (32, 128)


def body(displacement, velocity, energy, mass_density, live_mask, time_step):
    table = {name: jnp.asarray(value) for name, value in constants().items()}
    n_dom, n_sub = lax.axis_size("dom"), lax.axis_size("sub")
    up = [(i, i + 1) for i in range(n_dom - 1)]

    def pairs(start, size):
        return [p for i in range(start, size - 1, 2) for p in ((i, i + 1), (i + 1, i))]

    walls = (table["off_x"], table["off_z"])

    (last,) = call(last_kernel, [(6, 450)], copied=True)(displacement, velocity)
    halo = lax.ppermute(last, "dom", up)
    packed, where = call(pack_kernel, [(400, 128), (8, 128)], copied=True)(
        displacement, velocity, mass_density.T, energy, live_mask.reshape(1, 48), table["pick"],
        table["place"],
    )
    row = lax.broadcasted_iota(jnp.int32, (8, 128), 0)
    own, z_first, z_second = call(
        halo_kernel, [(400, 128), (BLOCK, 128), (BLOCK, 128)]
    )(packed, halo, table["pick"], where)
    flags = jnp.where(row < 2, where, time_step)
    first = lax.ppermute(z_first, "sub", pairs(0, n_sub))
    second = lax.ppermute(z_second, "sub", pairs(1, n_sub))
    message, low, high, disp, vel, live, power, wdens = call(
        force_kernel,
        [(248, 128), FACE, FACE, NODES, NODES, (8, 128), POINTS, POINTS],
        [(384, 768), (384, 384), POINTS],
    )(own, first, second, table["grad"], table["grad_t"], table["psi"], table["weight"], flags)
    far = lax.ppermute(message, "dom", pairs(1, n_dom))
    skip_up = lax.ppermute(high, "dom", [(i, i + 2) for i in range(n_dom - 2)])
    skip_down = lax.ppermute(low, "dom", [(i + 2, i) for i in range(n_dom - 2)])
    near = lax.ppermute(message, "dom", pairs(0, n_dom))
    (energy_rate,) = call(energy_kernel, [(27, 48)])(power, wdens, table["psi_t"], table["take"])
    message, energy_rate = lax.optimization_barrier((message, energy_rate))
    resid, image, local = call(krylov_kernel, [NODES, NODES, (n_dom, 128)])(
        message, near, far, skip_up, skip_down, flags, *walls, table["phi"], table["phi_t"],
        table["own"], table["own_element"],
    )
    slab = jnp.sum(lax.all_to_all(local, "dom", 0, 0, tiled=True), axis=0, keepdims=True)
    moments = lax.all_to_all(jnp.broadcast_to(slab, (n_sub, 128)), "sub", 0, 0, tiled=True)
    newvel, moved, part, near, far, skip = call(
        first_shape_kernel, [NODES, NODES, NODES, (160, 128), (160, 128), FACE],
        [(384, 384), (384, 384)],
    )(moments, disp, vel, resid, image, live, flags, table["off_z"], table["grad"], table["grad_t"],
      table["weight"])
    near = lax.ppermute(near, "dom", pairs(0, n_dom))
    far = lax.ppermute(far, "dom", pairs(1, n_dom))
    skip = lax.ppermute(skip, "dom", [(i + 2, i) for i in range(n_dom - 2)])
    (new_velocity,) = call(write_kernel, [(3, 1350)])(newvel, table["back"])
    part, new_velocity = lax.optimization_barrier((part, new_velocity))
    (mesh_velocity,) = call(
        second_shape_kernel, [(3, 1350)], [(384, 384)] * 4
    )(part, near, far, skip, flags, *walls, newvel, moved, live, table["grad"], table["grad_t"],
      table["weight"], table["back"])
    return new_velocity, energy_rate, mesh_velocity


def solution(mesh):
    both = ("dom", "sub")

    return jax.shard_map(
        body,
        mesh=mesh,
        in_specs=(P(None, both), P(None, both), P(None, both), P(None, both), P(both), P()),
        out_specs=(P(None, both), P(None, both), P(None, both)),
        check_vma=False,
    )
```

```python
import functools
import math

import jax
import jax.numpy as jnp
import numpy as np
from jax import lax
from jax.experimental import pallas as pl
from jax.experimental.pallas import tpu as pltpu
from jax.sharding import PartitionSpec as P


EY = 8
EZ = 6
VISC = 0.3
MESH_STEP = 0.01
BF = jnp.bfloat16
F32 = jnp.float32
ROWS = 40
BELOW = 3
WINDOW = 13
LANE_OWN = 9 * BELOW
BLOCK = 136


def node_row(a, b, c):
    if b == 0 and c > 0:
        return 2 * a + c - 1
    if b > 0 and c == 0:
        return 8 + 2 * a + b - 1
    if b > 0:
        return 16 + 4 * a + 2 * (b - 1) + c - 1
    return 32 + a


def local_row(a, b, c):
    if b < 3 and c < 3:
        return node_row(a, b, c)
    if b == 3 and c < 3:
        return 48 + a if c == 0 else 40 + node_row(a, 0, c)
    if b < 3:
        return 64 + a if b == 0 else 56 + node_row(a, b, 0) - 8
    return 72 + a


def outer_triple(first, second, third):
    product = (
        first[:, None, None, :, None, None]
        * second[None, :, None, None, :, None]
        * third[None, None, :, None, None, :]
    )
    return product.reshape(
        first.shape[0] * second.shape[0] * third.shape[0],
        first.shape[1] * second.shape[1] * third.shape[1],
    )


def basis_tables():
    root_term = math.sqrt(10.0 / 7.0)
    outer = math.sqrt(5.0 + 2.0 * root_term) / 3.0
    inner = math.sqrt(5.0 - 2.0 * root_term) / 3.0
    gauss_roots = np.array([-outer, -inner, 0.0, inner, outer])
    outer_weight = (322.0 - 13.0 * math.sqrt(70.0)) / 900.0
    middle_weight = (322.0 + 13.0 * math.sqrt(70.0)) / 900.0
    weights = (
        np.array([outer_weight, middle_weight, 128.0 / 225.0, middle_weight, outer_weight]) / 2.0
    )
    points = (1.0 + gauss_roots) / 2.0
    lobatto = [0.0, (1.0 - 1.0 / math.sqrt(5.0)) / 2.0, (1.0 + 1.0 / math.sqrt(5.0)) / 2.0, 1.0]
    values = np.ones((5, 4))
    slopes = np.zeros((5, 4))
    for node in range(4):
        for other in range(4):
            if other != node:
                values[:, node] *= (points - lobatto[other]) / (lobatto[node] - lobatto[other])
        for other in range(4):
            if other != node:
                term = np.ones(5) / (lobatto[node] - lobatto[other])
                for third in range(4):
                    if third != node and third != other:
                        term = term * (points - lobatto[third]) / (lobatto[node] - lobatto[third])
                slopes[:, node] += term
    bernstein = np.stack([(1.0 - points) ** 2, 2.0 * points * (1.0 - points), points**2], axis=1)
    quad_weight = (
        weights[:, None, None] * weights[None, :, None] * weights[None, None, :]
    ).reshape(125)
    return (
        outer_triple(values, values, values),
        [
            outer_triple(slopes, values, values),
            outer_triple(values, slopes, values),
            outer_triple(values, values, slopes),
        ],
        outer_triple(bernstein, bernstein, bernstein),
        quad_weight,
    )


def split_table(table):
    high = table.astype(np.float32).astype(jnp.bfloat16)
    low = (table - high.astype(np.float64)).astype(np.float32).astype(jnp.bfloat16)
    return high, low


@functools.cache
def constants():
    vel_basis, grads, energy_basis, quad_weight = basis_tables()
    order = np.zeros(64, np.int64)
    for a in range(4):
        for b in range(4):
            for c in range(4):
                order[16 * a + 4 * b + c] = local_row(a, b, c)

    def spread_columns(table):
        wide = np.zeros((128, 80))
        wide[:125, order] = table
        return wide

    out = {}
    grad = np.concatenate([spread_columns(g) for g in grads], axis=0)
    high, low = split_table(grad)
    out["grad"] = np.concatenate([high, high, low], axis=1)
    high, low = split_table(grad.T)
    out["grad_t"] = np.concatenate([high, low], axis=0)
    phi = spread_columns(vel_basis)
    high, low = split_table(phi)
    out["phi"] = np.concatenate([high, high, low], axis=1)
    high, low = split_table(phi.T)
    out["phi_t"] = np.concatenate([high, low], axis=0)
    psi = np.zeros((128, 32))
    psi[:125, :27] = energy_basis
    high, low = split_table(psi)
    out["psi"] = np.concatenate([high, high, low], axis=1)
    high, low = split_table(psi.T)
    out["psi_t"] = np.concatenate([high, low], axis=0)
    weight = np.zeros((128, 128), np.float32)
    weight[:125] = quad_weight[:, None]
    out["weight"] = weight

    flat = np.arange(450)
    py, pz = flat // 18, flat % 18
    lane = 9 * ((pz + 1) // 3) + py // 3
    frame = lane - 9 * (pz % 3 == 2)
    own = np.zeros((ROWS, 128), np.float32)
    for a in range(4):
        for k in range(450):
            b, c = py[k] % 3, (pz[k] + 1) % 3
            row = node_row(a, b, c)
            if a > 0:
                own[row, lane[k] + LANE_OWN] = 1.0
    out["own"] = own
    pick = np.zeros((450, 128), np.float32)
    pick[flat, frame] = 1.0
    out["pick"] = pick.astype(jnp.bfloat16)
    back = np.zeros((128, 450), np.float32)
    back[lane + LANE_OWN, flat] = 1.0
    out["back"] = back.astype(jnp.bfloat16)
    off_x = np.ones((ROWS, 128), np.float32)
    off_z = np.ones((ROWS, 128), np.float32)
    for b in range(3):
        for c in range(3):
            for a in range(4):
                if a == 0:
                    off_x[node_row(a, b, c)] = 0.0
                off_z[node_row(a, b, c), 3 * (np.arange(128) // 9 - BELOW) + c <= 0] = 0.0
    out["off_x"] = off_x
    out["off_z"] = off_z
    element = np.arange(EY * EZ)
    elane = 9 * (element % EZ) + element // EZ
    place = np.zeros((48, 128), np.float32)
    place[element, elane] = 1.0
    out["place"] = place.astype(jnp.bfloat16)
    take = np.zeros((128, 48), np.float32)
    take[elane + LANE_OWN, element] = 1.0
    out["take"] = take.astype(jnp.bfloat16)
    own_element = np.zeros((8, 128), np.float32)
    own_element[:, elane + LANE_OWN] = 1.0
    out["own_element"] = own_element
    return out


def dot(left, right):
    return jnp.dot(left, right, preferred_element_type=F32)


def split2(value):
    high = value.astype(BF)
    return high, (value - high.astype(F32)).astype(BF)


def split3(value):
    high = value.astype(BF)
    rest = value - high.astype(F32)
    middle = rest.astype(BF)
    return high, middle, (rest - middle.astype(F32)).astype(BF)


def exact_dot(value, selection):
    high, middle, low = (part.astype(F32) for part in split3(value))
    rows = value.shape[0]
    wide = dot(jnp.concatenate([high, middle, low], axis=0).astype(BF), selection)
    return wide[:rows] + (wide[rows : 2 * rows] + wide[2 * rows :])


def stacked(value):
    high, low = split2(value)
    return jnp.concatenate([high, low, high], axis=0)


def rolled(value, by):
    return pltpu.roll(value, by % 128, 1)


def to_local(nodes):
    columns = []
    for comp in range(3):
        block = nodes[ROWS * comp : ROWS * comp + ROWS]
        corner = block[32:40]
        columns.append(
            jnp.concatenate(
                [
                    block,
                    rolled(block[0:8], -1),
                    rolled(corner, -1),
                    rolled(block[8:16], -9),
                    rolled(corner, -9),
                    rolled(corner, -10),
                ],
                axis=0,
            )
        )
    return jnp.concatenate(columns, axis=1)


def from_local(local):
    blocks = []
    for comp in range(3):
        part = local[:, 128 * comp : 128 * comp + 128]
        blocks += [
            part[0:8] + rolled(part[40:48], 1),
            part[8:16] + rolled(part[56:64], 9),
            part[16:32],
            part[32:40]
            + (rolled(part[48:56], 1) + rolled(part[64:72], 9) + rolled(part[72:80], 10)),
        ]
    return jnp.concatenate(blocks, axis=0)


def transposed_dot(table, value):
    high, low = split2(value)
    half = table.shape[0] // 2
    both = dot(table, high)
    return both[:half] + (both[half:] + dot(table[:half], low))


def turned(value, by):
    return value if by % 8 == 0 else pltpu.roll(value, by % 8, 0)


def row_index():
    return lax.broadcasted_iota(jnp.int32, (8, 128), 0)


def face_of(nodes, plane):
    row = row_index()
    by = (0, 2, 4) if plane == 0 else (2, 4, 0)
    inner = 16 if plane == 0 else 24
    blocks = []
    corners = jnp.zeros((8, 128), F32)
    for comp in range(3):
        at = ROWS * comp
        first = turned(nodes[at : at + 8], by[0])
        second = turned(nodes[at + 8 : at + 16], by[1])
        third = turned(nodes[at + inner : at + inner + 8], by[2])
        blocks.append(jnp.where(row < 2, first, jnp.where(row < 4, second, third)))
        corners = jnp.where(row == comp, turned(nodes[at + 32 : at + 40], comp - plane), corners)
    return jnp.concatenate(blocks + [corners], axis=0)


def add_faces(nodes, below, above):
    row = row_index()
    blocks = []
    for comp in range(3):
        at = ROWS * comp
        low, high = below[8 * comp : 8 * comp + 8], above[8 * comp : 8 * comp + 8]
        blocks.append(
            nodes[at : at + 8] + jnp.where(row < 2, low, jnp.where(row >= 6, turned(high, 6), 0.0))
        )
        blocks.append(
            nodes[at + 8 : at + 16]
            + jnp.where(row < 2, turned(low, 6), jnp.where(row >= 6, turned(high, 4), 0.0))
        )
        blocks.append(nodes[at + 16 : at + 24] + jnp.where(row < 4, turned(low, 4), 0.0))
        blocks.append(nodes[at + 24 : at + 32] + jnp.where(row >= 4, high, 0.0))
        low, high = turned(below[24:32], -comp), turned(above[24:32], 3 - comp)
        blocks.append(
            nodes[at + 32 : at + 40] + jnp.where(row == 0, low, jnp.where(row == 3, high, 0.0))
        )
    return jnp.concatenate(blocks, axis=0)


def flag(flags_ref, row):
    return flags_ref[row : row + 1, 0:1]


def is_even(flags_ref, row, shape):
    place = flag(flags_ref, row)
    rest = place - 2.0 * jnp.floor(place * 0.5)
    return jnp.broadcast_to(rest, shape) < 0.5


def leads_pair(flags_ref):
    place = flag(flags_ref, 0)
    rest = place - 4.0 * jnp.floor(place * 0.25)
    return jnp.broadcast_to(rest, (32, 128)) < 1.5


def z_wall(flags_ref, off_z_ref):
    wall = jnp.minimum(off_z_ref[...] + flag(flags_ref, 1), 1.0)
    return jnp.concatenate([wall, wall, wall], axis=0)


def cofactors(j):
    return [
        [
            j[(r + 1) % 3][(c + 1) % 3] * j[(r + 2) % 3][(c + 2) % 3]
            - j[(r + 1) % 3][(c + 2) % 3] * j[(r + 2) % 3][(c + 1) % 3]
            for c in range(3)
        ]
        for r in range(3)
    ]


def gradients(ref, chunk, base=0):
    return [
        [
            ref[128 * m + 8 * chunk : 128 * m + 8 * chunk + 8, base + 128 * c : base + 128 * c + 128]
            for m in range(3)
        ]
        for c in range(3)
    ]


def plus_identity(g):
    return [[g[c][m] + 1.0 if c == m else g[c][m] for m in range(3)] for c in range(3)]


def plane_index(width):
    row = lax.broadcasted_iota(jnp.int32, (ROWS, width), 0)
    return jnp.where(
        row < 8,
        row // 2,
        jnp.where(
            row < 16,
            (row - 8) // 2,
            jnp.where(row < 32, (row - 16) // 4, jnp.where(row < 36, row - 32, 9)),
        ),
    )


def node_mask():
    row = lax.broadcasted_iota(jnp.int32, (ROWS, 450), 0)
    odd = row & 1
    row_code = jnp.where(
        row < 8,
        odd + 1,
        jnp.where(
            row < 16,
            3 * odd + 3,
            jnp.where(row < 32, 3 * ((row >> 1) & 1) + odd + 4, jnp.where(row < 36, 0, 99)),
        ),
    )
    flat = lax.broadcasted_iota(jnp.int32, (ROWS, 450), 1)
    y = (flat * 3641) >> 16
    z = flat - 18 * y + 1
    code = 3 * (y - 3 * ((y * 86) >> 8)) + z - 3 * ((z * 86) >> 8)
    return row_code == code


def last_kernel(disp_ref, vel_ref, out_ref):
    out_ref[0:3, :] = disp_ref[:, 900:1350]
    out_ref[3:6, :] = vel_ref[:, 900:1350]


def pack_kernel(disp_ref, vel_ref, dens_ref, energy_ref, live_ref, pick_ref, place_ref, out_ref,
                where_ref):
    dom, sub = lax.axis_index("dom"), lax.axis_index("sub")
    where_ref[...] = jnp.where(row_index() == 0, dom.astype(F32), sub.astype(F32))
    plane = plane_index(450)
    mask = node_mask() & (plane >= 1)
    blocks = []
    for ref in (disp_ref, vel_ref):
        planes = [ref[:, 450 * x : 450 * x + 450] for x in range(3)]
        for comp in range(3):
            first, second, third = (jnp.broadcast_to(p[comp : comp + 1], (ROWS, 450)) for p in planes)
            blocks.append(
                jnp.where(
                    mask, jnp.where(plane == 1, first, jnp.where(plane == 2, second, third)), 0.0
                )
            )
    out_ref[0:240, :] = exact_dot(jnp.concatenate(blocks, axis=0), pick_ref[...])
    row = lax.broadcasted_iota(jnp.int32, (8, 48), 0)
    tail = jnp.pad(energy_ref[24:27], ((0, 5), (0, 0)))
    tail = jnp.where(row == 3, live_ref[...].astype(F32), tail)
    density = jnp.pad(dens_ref[...], ((0, 0), (0, 3))).T
    out_ref[240:400, :] = exact_dot(
        jnp.concatenate([density, energy_ref[0:24], tail], axis=0), place_ref[...]
    )


def send_columns(value, start):
    lane = lax.broadcasted_iota(jnp.int32, (BLOCK, 128), 1)
    value = jnp.concatenate([value, jnp.zeros((3 * BLOCK - 400, 128), F32)], axis=0)
    parts = [rolled(value[BLOCK * i : BLOCK * i + BLOCK], 36 * i - start) for i in range(3)]
    return jnp.where(lane < 36, parts[0], jnp.where(lane < 72, parts[1], parts[2]))


def halo_kernel(packed_ref, halo_ref, pick_ref, where_ref, own_ref, first_ref, second_ref):
    mask = node_mask() & (plane_index(450) == 0)
    blocks = [
        jnp.where(mask, jnp.broadcast_to(halo_ref[comp : comp + 1, :], (ROWS, 450)), 0.0)
        for comp in range(6)
    ]
    nodes = exact_dot(jnp.concatenate(blocks, axis=0), pick_ref[...])
    own = jnp.concatenate([packed_ref[0:240] + nodes, packed_ref[240:400]], axis=0)
    own_ref[...] = own
    up, down = send_columns(own, 18), send_columns(own, 0)
    even = is_even(where_ref, 1, (BLOCK, 128))
    first_ref[...] = jnp.where(even, up, down)
    second_ref[...] = jnp.where(even, down, up)


def unpack(own, below, above):
    lane = lax.broadcasted_iota(jnp.int32, (8, 128), 1)
    rows = []
    for at in range(0, 400, 8):
        block, inner = at // BLOCK, at % BLOCK
        on_vertex = 9 if at < 240 and at % ROWS in (8, 32) else 0
        base = 36 * block
        mine = rolled(own[at : at + 8], 27 + on_vertex)
        low = rolled(below[inner : inner + 8], on_vertex - 9 - base)
        high = rolled(above[inner : inner + 8], 81 + on_vertex - base)
        rows.append(
            jnp.where(
                lane < 27 + on_vertex, low, jnp.where(lane < 81 + on_vertex, mine, high)
            )
        )
    return jnp.concatenate(rows, axis=0)


def force_kernel(own_ref, first_ref, second_ref, grad_ref, grad_t_ref, psi_ref, weight_ref,
                 flags_ref, message_ref, skip1_ref, skip2_ref, disp_ref, vel_ref, live_ref,
                 power_ref, wdens_ref, g_ref, flux_ref, point_ref):
    even = is_even(flags_ref, 1, (BLOCK, 128))
    first, second = first_ref[...], second_ref[...]
    window = unpack(own_ref[...], jnp.where(even, second, first), jnp.where(even, first, second))
    disp, vel, energy = window[0:120], window[120:240], window[368:400]
    disp_ref[...] = disp
    vel_ref[...] = vel
    lane = lax.broadcasted_iota(jnp.int32, (1, 128), 1)
    live = jnp.where(lane < 9 * WINDOW, energy[27:28], 0.0)
    live_ref[...] = jnp.broadcast_to(live, (8, 128))
    table = grad_ref[...]
    g_ref[:, 0:384] = dot(table, stacked(to_local(disp)))
    g_ref[:, 384:768] = dot(table, stacked(to_local(vel)))
    point_ref[...] = dot(psi_ref[...], stacked(energy))
    alive = jnp.broadcast_to(live, (8, 128))
    for chunk in range(16):
        at = slice(8 * chunk, 8 * chunk + 8)
        j = plus_identity(gradients(g_ref, chunk))
        g = gradients(g_ref, chunk, 384)
        cof = cofactors(j)
        volume = j[0][0] * cof[0][0] + j[0][1] * cof[0][1] + j[0][2] * cof[0][2]
        volume = jnp.where(alive > 0.5, volume, 1.0)
        inverse = 1.0 / volume
        mass_density = window[240 + 8 * chunk : 248 + 8 * chunk]
        density = mass_density * inverse
        pressure = (5.0 / 3.0 - 1.0) * density * point_ref[at, :]
        spatial = [
            [
                (g[c][0] * cof[m][0] + g[c][1] * cof[m][1] + g[c][2] * cof[m][2]) * inverse
                for m in range(3)
            ]
            for c in range(3)
        ]
        drag = VISC * density
        stress = [[None] * 3 for _ in range(3)]
        for c in range(3):
            for m in range(c, 3):
                value = drag * (spatial[c][m] + spatial[m][c])
                stress[c][m] = stress[m][c] = value - pressure if c == m else value
        weight = weight_ref[at, :]
        live_weight = weight * alive
        for c in range(3):
            for m in range(3):
                flux_ref[128 * m + 8 * chunk : 128 * m + 8 * chunk + 8, 128 * c : 128 * c + 128] = (
                    -live_weight
                ) * (stress[c][0] * cof[0][m] + stress[c][1] * cof[1][m] + stress[c][2] * cof[2][m])
        power = stress[0][0] * spatial[0][0]
        for c in range(3):
            for m in range(3):
                if c + m > 0:
                    power = power + stress[c][m] * spatial[c][m]
        power_ref[at, :] = live_weight * volume * power
        wdens = weight * mass_density
        wdens_ref[at, :] = wdens
        message_ref[120 + 8 * chunk : 128 + 8 * chunk, :] = wdens * alive
    force = from_local(transposed_dot(grad_t_ref[...], flux_ref[...]))
    message_ref[0:120, :] = force
    low, high = face_of(force, 0), face_of(force, 3)
    leads = leads_pair(flags_ref)
    skip1_ref[...] = jnp.where(leads, high, low)
    skip2_ref[...] = jnp.where(leads, low, high)


def energy_kernel(power_ref, wdens_ref, psi_t_ref, take_ref, out_ref):
    table = psi_t_ref[...]
    lumped = transposed_dot(table, wdens_ref[...])
    lumped = jnp.where(lumped > 0.0, lumped, 1.0)
    rate = transposed_dot(table, power_ref[...]) / lumped
    out_ref[...] = exact_dot(rate, take_ref[...])[0:27]


def total_of(value):
    return jnp.sum(jnp.sum(value, axis=0, keepdims=True), axis=1, keepdims=True)


def mass_points(nodes, phi_ref):
    return dot(phi_ref[...], stacked(to_local(nodes)))


def point_energy(points, mass, own_element):
    square = (
        points[:, 0:128] * points[:, 0:128]
        + points[:, 128:256] * points[:, 128:256]
        + points[:, 256:384] * points[:, 256:384]
    )
    return total_of(jnp.sum(square * mass, axis=0, keepdims=True) * own_element)


def norm_of(nodes, own):
    return total_of(nodes * nodes * jnp.concatenate([own, own, own], axis=0))


def mass_image(points, mass, phi_t_ref):
    return from_local(
        transposed_dot(phi_t_ref[...], points * jnp.concatenate([mass, mass, mass], axis=1))
    )


def krylov_kernel(message_ref, near_ref, far_ref, skip1_ref, skip2_ref, flags_ref, off_x_ref,
                  off_z_ref, phi_ref, phi_t_ref, own_ref, own_element_ref, resid_ref, image_ref,
                  out_ref):
    even = is_even(flags_ref, 0, (248, 128))
    near, far = near_ref[...], far_ref[...]
    upper, lower = jnp.where(even, near, far), jnp.where(even, far, near)
    force, mass = message_ref[0:120], message_ref[120:248]
    leads = leads_pair(flags_ref)
    skip_down = jnp.where(leads, skip1_ref[...], skip2_ref[...])
    skip_up = jnp.where(leads, skip2_ref[...], skip1_ref[...])
    wall = z_wall(flags_ref, off_z_ref)
    dom = flag(flags_ref, 0)

    def walls(place):
        x_wall = jnp.minimum(off_x_ref[...] + jnp.maximum(place, 0.0), 1.0)
        return wall * jnp.concatenate([x_wall, x_wall, x_wall], axis=0)

    own_walls = walls(dom)
    resid = add_faces(force, face_of(lower, 3), face_of(upper, 0)) * own_walls
    resid_low = add_faces(lower[0:120], skip_up, face_of(force, 0)) * walls(dom - 1.0)
    resid_up = add_faces(upper[0:120], face_of(force, 3), skip_down) * wall
    resid_ref[...] = resid
    points = mass_points(resid, phi_ref)
    part = mass_image(points, mass, phi_t_ref)
    part_low = mass_image(mass_points(resid_low, phi_ref), lower[120:248], phi_t_ref)
    part_up = mass_image(mass_points(resid_up, phi_ref), upper[120:248], phi_t_ref)
    image = add_faces(part, face_of(part_low, 3), face_of(part_up, 0)) * own_walls
    image_ref[...] = image
    own, own_element = own_ref[...], own_element_ref[0:1]
    moments = (
        norm_of(resid, own),
        point_energy(points, mass, own_element),
        norm_of(image, own),
        point_energy(mass_points(image, phi_ref), mass, own_element),
    )
    lane = lax.broadcasted_iota(jnp.int32, (1, 128), 1)
    row = jnp.zeros((1, 128), F32)
    for i, moment in enumerate(moments):
        row = jnp.where(lane == i, moment, row)
    out_ref[...] = jnp.broadcast_to(row, out_ref.shape)


def shape_forces(u, live, grad_ref, grad_t_ref, weight_ref, g_ref, flux_ref):
    g_ref[...] = dot(grad_ref[...], stacked(to_local(u)))
    for chunk in range(16):
        at = slice(8 * chunk, 8 * chunk + 8)
        j = plus_identity(gradients(g_ref, chunk))
        cof = cofactors(j)
        volume = j[0][0] * cof[0][0] + j[0][1] * cof[0][1] + j[0][2] * cof[0][2]
        volume = jnp.where(live > 0.5, volume, 1.0)
        norm = j[0][0] * j[0][0]
        for c in range(3):
            for m in range(3):
                if c + m > 0:
                    norm = norm + j[c][m] * j[c][m]
        weight = weight_ref[at, :] * live * jnp.exp(jnp.log(volume) * (-2.0 / 3.0))
        first = weight * (2.0 / 3.0)
        second = weight * (-2.0 / 9.0) * (norm / volume)
        for c in range(3):
            for m in range(3):
                flux_ref[128 * m + 8 * chunk : 128 * m + 8 * chunk + 8, 128 * c : 128 * c + 128] = (
                    first * j[c][m] + second * cof[c][m]
                )
    return from_local(transposed_dot(grad_t_ref[...], flux_ref[...]))


def first_shape_kernel(moments_ref, disp_ref, vel_ref, resid_ref, image_ref, live_ref, flags_ref,
                       off_z_ref, grad_ref, grad_t_ref, weight_ref, newvel_ref, moved_ref, part_ref,
                       near_ref, far_ref, skip_ref, g_ref, flux_ref):
    moments = jnp.sum(moments_ref[...], axis=0, keepdims=True)
    mu0, mu1, mu2, mu3 = (moments[:, i : i + 1] for i in range(4))
    alpha = mu0 / mu1
    rest = alpha * alpha * mu2 - mu0
    beta = rest / mu0
    gain = 1.0 + beta
    second = rest / (gain * gain * mu1 - 2.0 * gain * alpha * mu2 + alpha * alpha * mu3)
    step = flag(flags_ref, 2)
    newvel = vel_ref[...] + step * (
        (alpha + second * gain) * resid_ref[...] - (alpha * second) * image_ref[...]
    )
    newvel_ref[...] = newvel
    moved = disp_ref[...] + step * newvel
    moved_ref[...] = moved
    live = live_ref[...]
    part = shape_forces(moved, live, grad_ref, grad_t_ref, weight_ref, g_ref, flux_ref)
    part_ref[...] = part
    next_u = moved - MESH_STEP * part * z_wall(flags_ref, off_z_ref)
    low = face_of(part, 0)
    skip_ref[...] = low
    down = jnp.concatenate([next_u, low, live], axis=0)
    up = jnp.concatenate(
        [jnp.zeros((120, 128), F32), face_of(part, 3), jnp.zeros((8, 128), F32)], axis=0
    )
    even = is_even(flags_ref, 0, (160, 128))
    near_ref[...] = jnp.where(even, up, down)
    far_ref[...] = jnp.where(even, down, up)


def write_nodes(nodes, back_ref, out_ref):
    wide = exact_dot(nodes, back_ref[...])
    plane = plane_index(450)
    masks = [node_mask() & (plane == a) for a in range(1, 4)]
    for comp in range(3):
        part = wide[ROWS * comp : ROWS * comp + ROWS]
        planes = [jnp.sum(jnp.where(mask, part, 0.0), axis=0, keepdims=True) for mask in masks]
        out_ref[comp : comp + 1, :] = jnp.concatenate(planes, axis=1)


def write_kernel(nodes_ref, back_ref, out_ref):
    write_nodes(nodes_ref[...], back_ref, out_ref)


def second_shape_kernel(part_ref, near_ref, far_ref, skip_ref, flags_ref, off_x_ref, off_z_ref,
                        newvel_ref, moved_ref, live_ref, grad_ref, grad_t_ref, weight_ref, back_ref,
                        out_ref, g_ref, flux_ref, next_g_ref, next_flux_ref):
    even = is_even(flags_ref, 0, (160, 128))
    near, far = near_ref[...], far_ref[...]
    upper, lower = jnp.where(even, near, far), jnp.where(even, far, near)
    wall = z_wall(flags_ref, off_z_ref)
    off_x = off_x_ref[...]
    x_wall = jnp.minimum(off_x + flag(flags_ref, 0), 1.0)
    total = add_faces(part_ref[...], lower[120:152], upper[120:152])
    gradient = total * wall * jnp.concatenate([x_wall, x_wall, x_wall], axis=0)
    u = moved_ref[...] - MESH_STEP * gradient
    zero = jnp.zeros((120, 128), F32)
    next_u = upper[0:120] * jnp.concatenate([off_x, off_x, off_x], axis=0)
    next_u = next_u + wall * add_faces(zero, face_of(u, 3), -MESH_STEP * skip_ref[...])
    part = shape_forces(u, live_ref[...], grad_ref, grad_t_ref, weight_ref, g_ref, flux_ref)
    next_part = shape_forces(
        next_u, upper[152:160], grad_ref, grad_t_ref, weight_ref, next_g_ref, next_flux_ref
    )
    second = add_faces(part, jnp.zeros((32, 128), F32), face_of(next_part, 0))
    nodes = newvel_ref[...] - (MESH_STEP / flag(flags_ref, 2)) * (gradient + second)
    write_nodes(nodes, back_ref, out_ref)


def copying(kernel, count):
    def run(*refs):
        sources, outs = refs[:count], refs[count : -count - 1]
        copies, sems = refs[-count - 1 : -1], refs[-1]
        moves = [
            pltpu.make_async_copy(source, target, sems.at[i])
            for i, (source, target) in enumerate(zip(sources, copies))
        ]
        for move in moves:
            move.start()
        for move in moves:
            move.wait()
        kernel(*copies, *outs)

    return run


def call(kernel, outs, scratch=(), flops=1_000_000, copied=False):
    spec = pl.BlockSpec(memory_space=pltpu.VMEM)

    def run(*args):
        given, body_of = spec, kernel
        extra = [pltpu.VMEM(shape, F32) for shape in scratch]
        if copied:
            given, body_of = pl.BlockSpec(memory_space=pltpu.HBM), copying(kernel, len(args))
            extra = [pltpu.VMEM(arg.shape, arg.dtype) for arg in args]
            extra.append(pltpu.SemaphoreType.DMA((len(args),)))
            args = [pltpu.with_memory_space_constraint(arg, pltpu.HBM) for arg in args]
        return pl.pallas_call(
            body_of,
            out_shape=[jax.ShapeDtypeStruct(shape, F32) for shape in outs],
            in_specs=[given] * len(args),
            out_specs=[spec] * len(outs),
            scratch_shapes=extra,
            compiler_params=pltpu.CompilerParams(vmem_limit_bytes=16 * 1024 * 1024),
            cost_estimate=pl.CostEstimate(flops=flops, bytes_accessed=400_000, transcendentals=0),
        )(*args)

    return run


NODES = (120, 128)
POINTS = (128, 128)
FACE = (32, 128)


def body(displacement, velocity, energy, mass_density, live_mask, time_step):
    table = {name: jnp.asarray(value) for name, value in constants().items()}
    n_dom, n_sub = lax.axis_size("dom"), lax.axis_size("sub")
    up = [(i, i + 1) for i in range(n_dom - 1)]

    def pairs(start, size):
        return [p for i in range(start, size - 1, 2) for p in ((i, i + 1), (i + 1, i))]

    walls = (table["off_x"], table["off_z"])

    (last,) = call(last_kernel, [(6, 450)], copied=True)(displacement, velocity)
    halo = lax.ppermute(last, "dom", up)
    packed, where = call(pack_kernel, [(400, 128), (8, 128)], copied=True)(
        displacement, velocity, mass_density.T, energy, live_mask.reshape(1, 48), table["pick"],
        table["place"],
    )
    row = lax.broadcasted_iota(jnp.int32, (8, 128), 0)
    own, z_first, z_second = call(
        halo_kernel, [(400, 128), (BLOCK, 128), (BLOCK, 128)]
    )(packed, halo, table["pick"], where)
    flags = jnp.where(row < 2, where, time_step)
    first = lax.ppermute(z_first, "sub", pairs(0, n_sub))
    second = lax.ppermute(z_second, "sub", pairs(1, n_sub))
    message, skip1, skip2, disp, vel, live, power, wdens = call(
        force_kernel,
        [(248, 128), FACE, FACE, NODES, NODES, (8, 128), POINTS, POINTS],
        [(384, 768), (384, 384), POINTS],
    )(own, first, second, table["grad"], table["grad_t"], table["psi"], table["weight"], flags)
    far = lax.ppermute(message, "dom", pairs(1, n_dom))

    def two_apart(phase):
        starts = [i for i in range(n_dom - 2) if (i % 4) // 2 == phase]
        return [p for i in starts for p in ((i, i + 2), (i + 2, i))]

    skip2 = lax.ppermute(skip2, "dom", two_apart(1))
    skip1 = lax.ppermute(skip1, "dom", two_apart(0))
    near = lax.ppermute(message, "dom", pairs(0, n_dom))
    (energy_rate,) = call(energy_kernel, [(27, 48)])(power, wdens, table["psi_t"], table["take"])
    message, energy_rate = lax.optimization_barrier((message, energy_rate))
    resid, image, local = call(krylov_kernel, [NODES, NODES, (n_dom, 128)])(
        message, near, far, skip1, skip2, flags, *walls, table["phi"], table["phi_t"],
        table["own"], table["own_element"],
    )
    slab = jnp.sum(lax.all_to_all(local, "dom", 0, 0, tiled=True), axis=0, keepdims=True)
    moments = lax.all_to_all(jnp.broadcast_to(slab, (n_sub, 128)), "sub", 0, 0, tiled=True)
    newvel, moved, part, near, far, skip = call(
        first_shape_kernel, [NODES, NODES, NODES, (160, 128), (160, 128), FACE],
        [(384, 384), (384, 384)],
    )(moments, disp, vel, resid, image, live, flags, table["off_z"], table["grad"], table["grad_t"],
      table["weight"])
    near = lax.ppermute(near, "dom", pairs(0, n_dom))
    far = lax.ppermute(far, "dom", pairs(1, n_dom))
    skip = lax.ppermute(skip, "dom", [(i + 2, i) for i in range(n_dom - 2)])
    (new_velocity,) = call(write_kernel, [(3, 1350)])(newvel, table["back"])
    part, new_velocity = lax.optimization_barrier((part, new_velocity))
    (mesh_velocity,) = call(
        second_shape_kernel, [(3, 1350)], [(384, 384)] * 4
    )(part, near, far, skip, flags, *walls, newvel, moved, live, table["grad"], table["grad_t"],
      table["weight"], table["back"])
    return new_velocity, energy_rate, mesh_velocity


def solution(mesh):
    both = ("dom", "sub")

    return jax.shard_map(
        body,
        mesh=mesh,
        in_specs=(P(None, both), P(None, both), P(None, both), P(None, both), P(both), P()),
        out_specs=(P(None, both), P(None, both), P(None, both)),
        check_vma=False,
    )
```

```python
import functools
import math

import jax
import jax.numpy as jnp
import numpy as np
from jax import lax
from jax.experimental import pallas as pl
from jax.experimental.pallas import tpu as pltpu
from jax.sharding import PartitionSpec as P


EY = 8
EZ = 6
VISC = 0.3
MESH_STEP = 0.01
BF = jnp.bfloat16
F32 = jnp.float32
ROWS = 40
BELOW = 3
WINDOW = 13
LANE_OWN = 9 * BELOW
BLOCK = 136


def node_row(a, b, c):
    if b == 0 and c > 0:
        return 2 * a + c - 1
    if b > 0 and c == 0:
        return 8 + 2 * a + b - 1
    if b > 0:
        return 16 + 4 * a + 2 * (b - 1) + c - 1
    return 32 + a


def local_row(a, b, c):
    if b < 3 and c < 3:
        return node_row(a, b, c)
    if b == 3 and c < 3:
        return 48 + a if c == 0 else 40 + node_row(a, 0, c)
    if b < 3:
        return 64 + a if b == 0 else 56 + node_row(a, b, 0) - 8
    return 72 + a


def outer_triple(first, second, third):
    product = (
        first[:, None, None, :, None, None]
        * second[None, :, None, None, :, None]
        * third[None, None, :, None, None, :]
    )
    return product.reshape(
        first.shape[0] * second.shape[0] * third.shape[0],
        first.shape[1] * second.shape[1] * third.shape[1],
    )


def basis_tables():
    root_term = math.sqrt(10.0 / 7.0)
    outer = math.sqrt(5.0 + 2.0 * root_term) / 3.0
    inner = math.sqrt(5.0 - 2.0 * root_term) / 3.0
    gauss_roots = np.array([-outer, -inner, 0.0, inner, outer])
    outer_weight = (322.0 - 13.0 * math.sqrt(70.0)) / 900.0
    middle_weight = (322.0 + 13.0 * math.sqrt(70.0)) / 900.0
    weights = (
        np.array([outer_weight, middle_weight, 128.0 / 225.0, middle_weight, outer_weight]) / 2.0
    )
    points = (1.0 + gauss_roots) / 2.0
    lobatto = [0.0, (1.0 - 1.0 / math.sqrt(5.0)) / 2.0, (1.0 + 1.0 / math.sqrt(5.0)) / 2.0, 1.0]
    values = np.ones((5, 4))
    slopes = np.zeros((5, 4))
    for node in range(4):
        for other in range(4):
            if other != node:
                values[:, node] *= (points - lobatto[other]) / (lobatto[node] - lobatto[other])
        for other in range(4):
            if other != node:
                term = np.ones(5) / (lobatto[node] - lobatto[other])
                for third in range(4):
                    if third != node and third != other:
                        term = term * (points - lobatto[third]) / (lobatto[node] - lobatto[third])
                slopes[:, node] += term
    bernstein = np.stack([(1.0 - points) ** 2, 2.0 * points * (1.0 - points), points**2], axis=1)
    quad_weight = (
        weights[:, None, None] * weights[None, :, None] * weights[None, None, :]
    ).reshape(125)
    return (
        outer_triple(values, values, values),
        [
            outer_triple(slopes, values, values),
            outer_triple(values, slopes, values),
            outer_triple(values, values, slopes),
        ],
        outer_triple(bernstein, bernstein, bernstein),
        quad_weight,
    )


def split_table(table):
    high = table.astype(np.float32).astype(jnp.bfloat16)
    low = (table - high.astype(np.float64)).astype(np.float32).astype(jnp.bfloat16)
    return high, low


@functools.cache
def constants():
    vel_basis, grads, energy_basis, quad_weight = basis_tables()
    order = np.zeros(64, np.int64)
    for a in range(4):
        for b in range(4):
            for c in range(4):
                order[16 * a + 4 * b + c] = local_row(a, b, c)

    def spread_columns(table):
        wide = np.zeros((128, 80))
        wide[:125, order] = table
        return wide

    out = {}
    grad = np.concatenate([spread_columns(g) for g in grads], axis=0)
    high, low = split_table(grad)
    out["grad"] = np.concatenate([high, high, low], axis=1)
    high, low = split_table(grad.T)
    out["grad_t"] = np.concatenate([high, low], axis=0)
    phi = spread_columns(vel_basis)
    high, low = split_table(phi)
    out["phi"] = np.concatenate([high, high, low], axis=1)
    high, low = split_table(phi.T)
    out["phi_t"] = np.concatenate([high, low], axis=0)
    psi = np.zeros((128, 32))
    psi[:125, :27] = energy_basis
    high, low = split_table(psi)
    out["psi"] = np.concatenate([high, high, low], axis=1)
    high, low = split_table(psi.T)
    out["psi_t"] = np.concatenate([high, low], axis=0)
    weight = np.zeros((128, 128), np.float32)
    weight[:125] = quad_weight[:, None]
    out["weight"] = weight

    flat = np.arange(450)
    py, pz = flat // 18, flat % 18
    lane = 9 * ((pz + 1) // 3) + py // 3
    frame = lane - 9 * (pz % 3 == 2)
    own = np.zeros((ROWS, 128), np.float32)
    for a in range(4):
        for k in range(450):
            b, c = py[k] % 3, (pz[k] + 1) % 3
            row = node_row(a, b, c)
            if a > 0:
                own[row, lane[k] + LANE_OWN] = 1.0
    out["own"] = own
    pick = np.zeros((450, 128), np.float32)
    pick[flat, frame] = 1.0
    out["pick"] = pick.astype(jnp.bfloat16)
    back = np.zeros((128, 450), np.float32)
    back[lane + LANE_OWN, flat] = 1.0
    out["back"] = back.astype(jnp.bfloat16)
    off_x = np.ones((ROWS, 128), np.float32)
    off_z = np.ones((ROWS, 128), np.float32)
    for b in range(3):
        for c in range(3):
            for a in range(4):
                if a == 0:
                    off_x[node_row(a, b, c)] = 0.0
                off_z[node_row(a, b, c), 3 * (np.arange(128) // 9 - BELOW) + c <= 0] = 0.0
    out["off_x"] = off_x
    out["off_z"] = off_z
    element = np.arange(EY * EZ)
    elane = 9 * (element % EZ) + element // EZ
    place = np.zeros((48, 128), np.float32)
    place[element, elane] = 1.0
    out["place"] = place.astype(jnp.bfloat16)
    take = np.zeros((128, 48), np.float32)
    take[elane + LANE_OWN, element] = 1.0
    out["take"] = take.astype(jnp.bfloat16)
    own_element = np.zeros((8, 128), np.float32)
    own_element[:, elane + LANE_OWN] = 1.0
    out["own_element"] = own_element
    return out


def dot(left, right):
    return jnp.dot(left, right, preferred_element_type=F32)


def split2(value):
    high = value.astype(BF)
    return high, (value - high.astype(F32)).astype(BF)


def split3(value):
    high = value.astype(BF)
    rest = value - high.astype(F32)
    middle = rest.astype(BF)
    return high, middle, (rest - middle.astype(F32)).astype(BF)


def exact_dot(value, selection):
    high, middle, low = (part.astype(F32) for part in split3(value))
    rows = value.shape[0]
    wide = dot(jnp.concatenate([high, middle, low], axis=0).astype(BF), selection)
    return wide[:rows] + (wide[rows : 2 * rows] + wide[2 * rows :])


def stacked(value):
    high, low = split2(value)
    return jnp.concatenate([high, low, high], axis=0)


def rolled(value, by):
    return pltpu.roll(value, by % 128, 1)


def to_local(nodes):
    columns = []
    for comp in range(3):
        block = nodes[ROWS * comp : ROWS * comp + ROWS]
        corner = block[32:40]
        columns.append(
            jnp.concatenate(
                [
                    block,
                    rolled(block[0:8], -1),
                    rolled(corner, -1),
                    rolled(block[8:16], -9),
                    rolled(corner, -9),
                    rolled(corner, -10),
                ],
                axis=0,
            )
        )
    return jnp.concatenate(columns, axis=1)


def from_local(local):
    blocks = []
    for comp in range(3):
        part = local[:, 128 * comp : 128 * comp + 128]
        blocks += [
            part[0:8] + rolled(part[40:48], 1),
            part[8:16] + rolled(part[56:64], 9),
            part[16:32],
            part[32:40]
            + (rolled(part[48:56], 1) + rolled(part[64:72], 9) + rolled(part[72:80], 10)),
        ]
    return jnp.concatenate(blocks, axis=0)


def transposed_dot(table, value):
    high, low = split2(value)
    half = table.shape[0] // 2
    both = dot(table, high)
    return both[:half] + (both[half:] + dot(table[:half], low))


def turned(value, by):
    return value if by % 8 == 0 else pltpu.roll(value, by % 8, 0)


def row_index():
    return lax.broadcasted_iota(jnp.int32, (8, 128), 0)


def face_of(nodes, plane):
    row = row_index()
    by = (0, 2, 4) if plane == 0 else (2, 4, 0)
    inner = 16 if plane == 0 else 24
    blocks = []
    corners = jnp.zeros((8, 128), F32)
    for comp in range(3):
        at = ROWS * comp
        first = turned(nodes[at : at + 8], by[0])
        second = turned(nodes[at + 8 : at + 16], by[1])
        third = turned(nodes[at + inner : at + inner + 8], by[2])
        blocks.append(jnp.where(row < 2, first, jnp.where(row < 4, second, third)))
        corners = jnp.where(row == comp, turned(nodes[at + 32 : at + 40], comp - plane), corners)
    return jnp.concatenate(blocks + [corners], axis=0)


def add_faces(nodes, below, above):
    row = row_index()
    blocks = []
    for comp in range(3):
        at = ROWS * comp
        low, high = below[8 * comp : 8 * comp + 8], above[8 * comp : 8 * comp + 8]
        blocks.append(
            nodes[at : at + 8] + jnp.where(row < 2, low, jnp.where(row >= 6, turned(high, 6), 0.0))
        )
        blocks.append(
            nodes[at + 8 : at + 16]
            + jnp.where(row < 2, turned(low, 6), jnp.where(row >= 6, turned(high, 4), 0.0))
        )
        blocks.append(nodes[at + 16 : at + 24] + jnp.where(row < 4, turned(low, 4), 0.0))
        blocks.append(nodes[at + 24 : at + 32] + jnp.where(row >= 4, high, 0.0))
        low, high = turned(below[24:32], -comp), turned(above[24:32], 3 - comp)
        blocks.append(
            nodes[at + 32 : at + 40] + jnp.where(row == 0, low, jnp.where(row == 3, high, 0.0))
        )
    return jnp.concatenate(blocks, axis=0)


def flag(flags_ref, row):
    return flags_ref[row : row + 1, 0:1]


def is_even(flags_ref, row, shape):
    place = flag(flags_ref, row)
    rest = place - 2.0 * jnp.floor(place * 0.5)
    return jnp.broadcast_to(rest, shape) < 0.5


def leads_pair(flags_ref):
    place = flag(flags_ref, 0)
    rest = place - 4.0 * jnp.floor(place * 0.25)
    return jnp.broadcast_to(rest, (32, 128)) < 1.5


def z_wall(flags_ref, off_z_ref):
    wall = jnp.minimum(off_z_ref[...] + flag(flags_ref, 1), 1.0)
    return jnp.concatenate([wall, wall, wall], axis=0)


def cofactors(j):
    return [
        [
            j[(r + 1) % 3][(c + 1) % 3] * j[(r + 2) % 3][(c + 2) % 3]
            - j[(r + 1) % 3][(c + 2) % 3] * j[(r + 2) % 3][(c + 1) % 3]
            for c in range(3)
        ]
        for r in range(3)
    ]


def gradients(ref, chunk, base=0):
    return [
        [
            ref[128 * m + 8 * chunk : 128 * m + 8 * chunk + 8, base + 128 * c : base + 128 * c + 128]
            for m in range(3)
        ]
        for c in range(3)
    ]


def plus_identity(g):
    return [[g[c][m] + 1.0 if c == m else g[c][m] for m in range(3)] for c in range(3)]


def plane_index(width):
    row = lax.broadcasted_iota(jnp.int32, (ROWS, width), 0)
    return jnp.where(
        row < 8,
        row // 2,
        jnp.where(
            row < 16,
            (row - 8) // 2,
            jnp.where(row < 32, (row - 16) // 4, jnp.where(row < 36, row - 32, 9)),
        ),
    )


def node_mask():
    row = lax.broadcasted_iota(jnp.int32, (ROWS, 450), 0)
    odd = row & 1
    row_code = jnp.where(
        row < 8,
        odd + 1,
        jnp.where(
            row < 16,
            3 * odd + 3,
            jnp.where(row < 32, 3 * ((row >> 1) & 1) + odd + 4, jnp.where(row < 36, 0, 99)),
        ),
    )
    flat = lax.broadcasted_iota(jnp.int32, (ROWS, 450), 1)
    y = (flat * 3641) >> 16
    z = flat - 18 * y + 1
    code = 3 * (y - 3 * ((y * 86) >> 8)) + z - 3 * ((z * 86) >> 8)
    return row_code == code


def last_kernel(disp_ref, vel_ref, out_ref):
    out_ref[0:3, :] = disp_ref[:, 900:1350]
    out_ref[3:6, :] = vel_ref[:, 900:1350]


def pack_kernel(disp_ref, vel_ref, dens_ref, energy_ref, live_ref, pick_ref, place_ref, out_ref,
                where_ref):
    dom, sub = lax.axis_index("dom"), lax.axis_index("sub")
    where_ref[...] = jnp.where(row_index() == 0, dom.astype(F32), sub.astype(F32))
    plane = plane_index(450)
    mask = node_mask() & (plane >= 1)
    blocks = []
    for ref in (disp_ref, vel_ref):
        planes = [ref[:, 450 * x : 450 * x + 450] for x in range(3)]
        for comp in range(3):
            first, second, third = (jnp.broadcast_to(p[comp : comp + 1], (ROWS, 450)) for p in planes)
            blocks.append(
                jnp.where(
                    mask, jnp.where(plane == 1, first, jnp.where(plane == 2, second, third)), 0.0
                )
            )
    out_ref[0:240, :] = exact_dot(jnp.concatenate(blocks, axis=0), pick_ref[...])
    row = lax.broadcasted_iota(jnp.int32, (8, 48), 0)
    tail = jnp.pad(energy_ref[24:27], ((0, 5), (0, 0)))
    tail = jnp.where(row == 3, live_ref[...].astype(F32), tail)
    density = jnp.pad(dens_ref[...], ((0, 0), (0, 3))).T
    out_ref[240:400, :] = exact_dot(
        jnp.concatenate([density, energy_ref[0:24], tail], axis=0), place_ref[...]
    )


def send_columns(value, start):
    lane = lax.broadcasted_iota(jnp.int32, (BLOCK, 128), 1)
    value = jnp.concatenate([value, jnp.zeros((3 * BLOCK - 400, 128), F32)], axis=0)
    parts = [rolled(value[BLOCK * i : BLOCK * i + BLOCK], 36 * i - start) for i in range(3)]
    return jnp.where(lane < 36, parts[0], jnp.where(lane < 72, parts[1], parts[2]))


def halo_kernel(packed_ref, halo_ref, pick_ref, where_ref, own_ref, first_ref, second_ref):
    mask = node_mask() & (plane_index(450) == 0)
    blocks = [
        jnp.where(mask, jnp.broadcast_to(halo_ref[comp : comp + 1, :], (ROWS, 450)), 0.0)
        for comp in range(6)
    ]
    nodes = exact_dot(jnp.concatenate(blocks, axis=0), pick_ref[...])
    own = jnp.concatenate([packed_ref[0:240] + nodes, packed_ref[240:400]], axis=0)
    own_ref[...] = own
    up, down = send_columns(own, 18), send_columns(own, 0)
    even = is_even(where_ref, 1, (BLOCK, 128))
    first_ref[...] = jnp.where(even, up, down)
    second_ref[...] = jnp.where(even, down, up)


def unpack(own, below, above):
    lane = lax.broadcasted_iota(jnp.int32, (8, 128), 1)
    rows = []
    for at in range(0, 400, 8):
        block, inner = at // BLOCK, at % BLOCK
        on_vertex = 9 if at < 240 and at % ROWS in (8, 32) else 0
        base = 36 * block
        mine = rolled(own[at : at + 8], 27 + on_vertex)
        low = rolled(below[inner : inner + 8], on_vertex - 9 - base)
        high = rolled(above[inner : inner + 8], 81 + on_vertex - base)
        rows.append(
            jnp.where(
                lane < 27 + on_vertex, low, jnp.where(lane < 81 + on_vertex, mine, high)
            )
        )
    return jnp.concatenate(rows, axis=0)


def force_kernel(own_ref, first_ref, second_ref, grad_ref, grad_t_ref, psi_ref, weight_ref,
                 flags_ref, message_ref, skip1_ref, skip2_ref, disp_ref, vel_ref, live_ref,
                 power_ref, wdens_ref, g_ref, flux_ref, point_ref):
    even = is_even(flags_ref, 1, (BLOCK, 128))
    first, second = first_ref[...], second_ref[...]
    window = unpack(own_ref[...], jnp.where(even, second, first), jnp.where(even, first, second))
    disp, vel, energy = window[0:120], window[120:240], window[368:400]
    disp_ref[...] = disp
    vel_ref[...] = vel
    lane = lax.broadcasted_iota(jnp.int32, (1, 128), 1)
    live = jnp.where(lane < 9 * WINDOW, energy[27:28], 0.0)
    live_ref[...] = jnp.broadcast_to(live, (8, 128))
    table = grad_ref[...]
    g_ref[:, 0:384] = dot(table, stacked(to_local(disp)))
    g_ref[:, 384:768] = dot(table, stacked(to_local(vel)))
    point_ref[...] = dot(psi_ref[...], stacked(energy))
    alive = jnp.broadcast_to(live, (8, 128))
    for chunk in range(16):
        at = slice(8 * chunk, 8 * chunk + 8)
        j = plus_identity(gradients(g_ref, chunk))
        g = gradients(g_ref, chunk, 384)
        cof = cofactors(j)
        volume = j[0][0] * cof[0][0] + j[0][1] * cof[0][1] + j[0][2] * cof[0][2]
        volume = jnp.where(alive > 0.5, volume, 1.0)
        inverse = 1.0 / volume
        mass_density = window[240 + 8 * chunk : 248 + 8 * chunk]
        density = mass_density * inverse
        pressure = (5.0 / 3.0 - 1.0) * density * point_ref[at, :]
        spatial = [
            [
                (g[c][0] * cof[m][0] + g[c][1] * cof[m][1] + g[c][2] * cof[m][2]) * inverse
                for m in range(3)
            ]
            for c in range(3)
        ]
        drag = VISC * density
        stress = [[None] * 3 for _ in range(3)]
        for c in range(3):
            for m in range(c, 3):
                value = drag * (spatial[c][m] + spatial[m][c])
                stress[c][m] = stress[m][c] = value - pressure if c == m else value
        weight = weight_ref[at, :]
        live_weight = weight * alive
        for c in range(3):
            for m in range(3):
                flux_ref[128 * m + 8 * chunk : 128 * m + 8 * chunk + 8, 128 * c : 128 * c + 128] = (
                    -live_weight
                ) * (stress[c][0] * cof[0][m] + stress[c][1] * cof[1][m] + stress[c][2] * cof[2][m])
        power = stress[0][0] * spatial[0][0]
        for c in range(3):
            for m in range(3):
                if c + m > 0:
                    power = power + stress[c][m] * spatial[c][m]
        power_ref[at, :] = live_weight * volume * power
        wdens = weight * mass_density
        wdens_ref[at, :] = wdens
        message_ref[120 + 8 * chunk : 128 + 8 * chunk, :] = wdens * alive
    force = from_local(transposed_dot(grad_t_ref[...], flux_ref[...]))
    message_ref[0:120, :] = force
    low, high = face_of(force, 0), face_of(force, 3)
    leads = leads_pair(flags_ref)
    skip1_ref[...] = jnp.where(leads, high, low)
    skip2_ref[...] = jnp.where(leads, low, high)


def energy_kernel(power_ref, wdens_ref, psi_t_ref, take_ref, out_ref):
    table = psi_t_ref[...]
    lumped = transposed_dot(table, wdens_ref[...])
    lumped = jnp.where(lumped > 0.0, lumped, 1.0)
    rate = transposed_dot(table, power_ref[...]) / lumped
    out_ref[...] = exact_dot(rate, take_ref[...])[0:27]


def total_of(value):
    return jnp.sum(jnp.sum(value, axis=0, keepdims=True), axis=1, keepdims=True)


def mass_points(nodes, phi_ref):
    return dot(phi_ref[...], stacked(to_local(nodes)))


def point_energy(points, mass, own_element):
    square = (
        points[:, 0:128] * points[:, 0:128]
        + points[:, 128:256] * points[:, 128:256]
        + points[:, 256:384] * points[:, 256:384]
    )
    return total_of(jnp.sum(square * mass, axis=0, keepdims=True) * own_element)


def norm_of(nodes, own):
    return total_of(nodes * nodes * jnp.concatenate([own, own, own], axis=0))


def mass_image(points, mass, phi_t_ref):
    return from_local(
        transposed_dot(phi_t_ref[...], points * jnp.concatenate([mass, mass, mass], axis=1))
    )


def krylov_kernel(message_ref, near_ref, far_ref, skip1_ref, skip2_ref, flags_ref, off_x_ref,
                  off_z_ref, phi_ref, phi_t_ref, own_ref, own_element_ref, resid_ref, image_ref,
                  out_ref):
    even = is_even(flags_ref, 0, (248, 128))
    near, far = near_ref[...], far_ref[...]
    upper, lower = jnp.where(even, near, far), jnp.where(even, far, near)
    force, mass = message_ref[0:120], message_ref[120:248]
    leads = leads_pair(flags_ref)
    skip_down = jnp.where(leads, skip1_ref[...], skip2_ref[...])
    skip_up = jnp.where(leads, skip2_ref[...], skip1_ref[...])
    wall = z_wall(flags_ref, off_z_ref)
    dom = flag(flags_ref, 0)

    def walls(place):
        x_wall = jnp.minimum(off_x_ref[...] + jnp.maximum(place, 0.0), 1.0)
        return wall * jnp.concatenate([x_wall, x_wall, x_wall], axis=0)

    own_walls = walls(dom)
    resid = add_faces(force, face_of(lower, 3), face_of(upper, 0)) * own_walls
    resid_low = add_faces(lower[0:120], skip_up, face_of(force, 0)) * walls(dom - 1.0)
    resid_up = add_faces(upper[0:120], face_of(force, 3), skip_down) * wall
    resid_ref[...] = resid
    points = mass_points(resid, phi_ref)
    part = mass_image(points, mass, phi_t_ref)
    part_low = mass_image(mass_points(resid_low, phi_ref), lower[120:248], phi_t_ref)
    part_up = mass_image(mass_points(resid_up, phi_ref), upper[120:248], phi_t_ref)
    image = add_faces(part, face_of(part_low, 3), face_of(part_up, 0)) * own_walls
    image_ref[...] = image
    own, own_element = own_ref[...], own_element_ref[0:1]
    moments = (
        norm_of(resid, own),
        point_energy(points, mass, own_element),
        norm_of(image, own),
        point_energy(mass_points(image, phi_ref), mass, own_element),
    )
    lane = lax.broadcasted_iota(jnp.int32, (1, 128), 1)
    row = jnp.zeros((1, 128), F32)
    for i, moment in enumerate(moments):
        row = jnp.where(lane == i, moment, row)
    out_ref[...] = jnp.broadcast_to(row, out_ref.shape)


def shape_forces(u, live, grad_ref, grad_t_ref, weight_ref, g_ref, flux_ref):
    g_ref[...] = dot(grad_ref[...], stacked(to_local(u)))
    for chunk in range(16):
        at = slice(8 * chunk, 8 * chunk + 8)
        j = plus_identity(gradients(g_ref, chunk))
        cof = cofactors(j)
        volume = j[0][0] * cof[0][0] + j[0][1] * cof[0][1] + j[0][2] * cof[0][2]
        volume = jnp.where(live > 0.5, volume, 1.0)
        norm = j[0][0] * j[0][0]
        for c in range(3):
            for m in range(3):
                if c + m > 0:
                    norm = norm + j[c][m] * j[c][m]
        weight = weight_ref[at, :] * live * jnp.exp(jnp.log(volume) * (-2.0 / 3.0))
        first = weight * (2.0 / 3.0)
        second = weight * (-2.0 / 9.0) * (norm / volume)
        for c in range(3):
            for m in range(3):
                flux_ref[128 * m + 8 * chunk : 128 * m + 8 * chunk + 8, 128 * c : 128 * c + 128] = (
                    first * j[c][m] + second * cof[c][m]
                )
    return from_local(transposed_dot(grad_t_ref[...], flux_ref[...]))


def first_shape_kernel(moments_ref, disp_ref, vel_ref, resid_ref, image_ref, live_ref, flags_ref,
                       off_z_ref, grad_ref, grad_t_ref, weight_ref, newvel_ref, moved_ref, part_ref,
                       near_ref, far_ref, skip_ref, g_ref, flux_ref):
    moments = jnp.sum(moments_ref[...], axis=0, keepdims=True)
    mu0, mu1, mu2, mu3 = (moments[:, i : i + 1] for i in range(4))
    alpha = mu0 / mu1
    rest = alpha * alpha * mu2 - mu0
    beta = rest / mu0
    gain = 1.0 + beta
    second = rest / (gain * gain * mu1 - 2.0 * gain * alpha * mu2 + alpha * alpha * mu3)
    step = flag(flags_ref, 2)
    newvel = vel_ref[...] + step * (
        (alpha + second * gain) * resid_ref[...] - (alpha * second) * image_ref[...]
    )
    newvel_ref[...] = newvel
    moved = disp_ref[...] + step * newvel
    moved_ref[...] = moved
    live = live_ref[...]
    part = shape_forces(moved, live, grad_ref, grad_t_ref, weight_ref, g_ref, flux_ref)
    part_ref[...] = part
    next_u = moved - MESH_STEP * part * z_wall(flags_ref, off_z_ref)
    low = face_of(part, 0)
    skip_ref[...] = low
    down = jnp.concatenate([next_u, low, live], axis=0)
    up = jnp.concatenate(
        [jnp.zeros((120, 128), F32), face_of(part, 3), jnp.zeros((8, 128), F32)], axis=0
    )
    even = is_even(flags_ref, 0, (160, 128))
    near_ref[...] = jnp.where(even, up, down)
    far_ref[...] = jnp.where(even, down, up)


def write_nodes(nodes, back_ref, out_ref):
    wide = exact_dot(nodes, back_ref[...])
    plane = plane_index(450)
    masks = [node_mask() & (plane == a) for a in range(1, 4)]
    for comp in range(3):
        part = wide[ROWS * comp : ROWS * comp + ROWS]
        planes = [jnp.sum(jnp.where(mask, part, 0.0), axis=0, keepdims=True) for mask in masks]
        out_ref[comp : comp + 1, :] = jnp.concatenate(planes, axis=1)


def write_kernel(nodes_ref, back_ref, out_ref):
    write_nodes(nodes_ref[...], back_ref, out_ref)


def second_shape_kernel(part_ref, near_ref, far_ref, skip_ref, flags_ref, off_x_ref, off_z_ref,
                        newvel_ref, moved_ref, live_ref, grad_ref, grad_t_ref, weight_ref, back_ref,
                        out_ref, g_ref, flux_ref, next_g_ref, next_flux_ref):
    even = is_even(flags_ref, 0, (160, 128))
    near, far = near_ref[...], far_ref[...]
    upper, lower = jnp.where(even, near, far), jnp.where(even, far, near)
    wall = z_wall(flags_ref, off_z_ref)
    off_x = off_x_ref[...]
    x_wall = jnp.minimum(off_x + flag(flags_ref, 0), 1.0)
    total = add_faces(part_ref[...], lower[120:152], upper[120:152])
    gradient = total * wall * jnp.concatenate([x_wall, x_wall, x_wall], axis=0)
    u = moved_ref[...] - MESH_STEP * gradient
    zero = jnp.zeros((120, 128), F32)
    next_u = upper[0:120] * jnp.concatenate([off_x, off_x, off_x], axis=0)
    next_u = next_u + wall * add_faces(zero, face_of(u, 3), -MESH_STEP * skip_ref[...])
    part = shape_forces(u, live_ref[...], grad_ref, grad_t_ref, weight_ref, g_ref, flux_ref)
    next_part = shape_forces(
        next_u, upper[152:160], grad_ref, grad_t_ref, weight_ref, next_g_ref, next_flux_ref
    )
    second = add_faces(part, jnp.zeros((32, 128), F32), face_of(next_part, 0))
    nodes = newvel_ref[...] - (MESH_STEP / flag(flags_ref, 2)) * (gradient + second)
    write_nodes(nodes, back_ref, out_ref)


def copying(kernel, count):
    def run(*refs):
        sources, outs = refs[:count], refs[count : -count - 1]
        copies, sems = refs[-count - 1 : -1], refs[-1]
        moves = [
            pltpu.make_async_copy(source, target, sems.at[i])
            for i, (source, target) in enumerate(zip(sources, copies))
        ]
        for move in moves:
            move.start()
        for move in moves:
            move.wait()
        kernel(*copies, *outs)

    return run


def call(kernel, outs, scratch=(), flops=1_000_000, copied=False):
    spec = pl.BlockSpec(memory_space=pltpu.VMEM)

    def run(*args):
        given, body_of = spec, kernel
        extra = [pltpu.VMEM(shape, F32) for shape in scratch]
        if copied:
            given, body_of = pl.BlockSpec(memory_space=pltpu.HBM), copying(kernel, len(args))
            extra = [pltpu.VMEM(arg.shape, arg.dtype) for arg in args]
            extra.append(pltpu.SemaphoreType.DMA((len(args),)))
            args = [pltpu.with_memory_space_constraint(arg, pltpu.HBM) for arg in args]
        return pl.pallas_call(
            body_of,
            out_shape=[jax.ShapeDtypeStruct(shape, F32) for shape in outs],
            in_specs=[given] * len(args),
            out_specs=[spec] * len(outs),
            scratch_shapes=extra,
            compiler_params=pltpu.CompilerParams(vmem_limit_bytes=16 * 1024 * 1024),
            cost_estimate=pl.CostEstimate(flops=flops, bytes_accessed=400_000, transcendentals=0),
        )(*args)

    return run


NODES = (120, 128)
POINTS = (128, 128)
FACE = (32, 128)


def body(displacement, velocity, energy, mass_density, live_mask, time_step):
    table = {name: jnp.asarray(value) for name, value in constants().items()}
    n_dom, n_sub = lax.axis_size("dom"), lax.axis_size("sub")
    up = [(i, i + 1) for i in range(n_dom - 1)]

    def pairs(start, size):
        return [p for i in range(start, size - 1, 2) for p in ((i, i + 1), (i + 1, i))]

    walls = (table["off_x"], table["off_z"])

    (last,) = call(last_kernel, [(6, 450)], copied=True)(displacement, velocity)
    halo = lax.ppermute(last, "dom", up)
    packed, where = call(pack_kernel, [(400, 128), (8, 128)], copied=True)(
        displacement, velocity, mass_density.T, energy, live_mask.reshape(1, 48), table["pick"],
        table["place"],
    )
    row = lax.broadcasted_iota(jnp.int32, (8, 128), 0)
    own, z_first, z_second = call(
        halo_kernel, [(400, 128), (BLOCK, 128), (BLOCK, 128)]
    )(packed, halo, table["pick"], where)
    flags = jnp.where(row < 2, where, time_step)
    first = lax.ppermute(z_first, "sub", pairs(0, n_sub))
    second = lax.ppermute(z_second, "sub", pairs(1, n_sub))
    message, skip1, skip2, disp, vel, live, power, wdens = call(
        force_kernel,
        [(248, 128), FACE, FACE, NODES, NODES, (8, 128), POINTS, POINTS],
        [(384, 768), (384, 384), POINTS],
    )(own, first, second, table["grad"], table["grad_t"], table["psi"], table["weight"], flags)
    far = lax.ppermute(message, "dom", pairs(1, n_dom))

    def two_apart(phase):
        starts = [i for i in range(n_dom - 2) if (i % 4) // 2 == phase]
        return [p for i in starts for p in ((i, i + 2), (i + 2, i))]

    skip2 = lax.ppermute(skip2, "dom", two_apart(1))
    skip1 = lax.ppermute(skip1, "dom", two_apart(0))
    near = lax.ppermute(message, "dom", pairs(0, n_dom))
    (energy_rate,) = call(energy_kernel, [(27, 48)])(power, wdens, table["psi_t"], table["take"])
    message, energy_rate = lax.optimization_barrier((message, energy_rate))
    resid, image, local = call(krylov_kernel, [NODES, NODES, (n_sub, 128)])(
        message, near, far, skip1, skip2, flags, *walls, table["phi"], table["phi_t"],
        table["own"], table["own_element"],
    )
    column = jnp.sum(lax.all_to_all(local, "sub", 0, 0, tiled=True), axis=0, keepdims=True)
    moments = lax.all_to_all(jnp.broadcast_to(column, (n_dom, 128)), "dom", 0, 0, tiled=True)
    newvel, moved, part, near, far, skip = call(
        first_shape_kernel, [NODES, NODES, NODES, (160, 128), (160, 128), FACE],
        [(384, 384), (384, 384)],
    )(moments, disp, vel, resid, image, live, flags, table["off_z"], table["grad"], table["grad_t"],
      table["weight"])
    near = lax.ppermute(near, "dom", pairs(0, n_dom))
    far = lax.ppermute(far, "dom", pairs(1, n_dom))
    skip = lax.ppermute(skip, "dom", [(i + 2, i) for i in range(n_dom - 2)])
    (new_velocity,) = call(write_kernel, [(3, 1350)])(newvel, table["back"])
    part, new_velocity = lax.optimization_barrier((part, new_velocity))
    (mesh_velocity,) = call(
        second_shape_kernel, [(3, 1350)], [(384, 384)] * 4
    )(part, near, far, skip, flags, *walls, newvel, moved, live, table["grad"], table["grad_t"],
      table["weight"], table["back"])
    return new_velocity, energy_rate, mesh_velocity


def solution(mesh):
    both = ("dom", "sub")

    return jax.shard_map(
        body,
        mesh=mesh,
        in_specs=(P(None, both), P(None, both), P(None, both), P(None, both), P(both), P()),
        out_specs=(P(None, both), P(None, both), P(None, both)),
        check_vma=False,
    )
```
